32 devices in a mesh: rep: 2 (over z, core), dp: 16 (over x, y).
Axes of the slice: x: 4, y: 4, z: 1, core: 2. Of those that a mesh axis runs over, the one named last changes fastest.
The devices are a block of a 4x4x8 slice.
Arguments:
- g_w_gate: bfloat16 [32, 2, 1536, 4224], P(('rep', 'dp')), parts along dimension 0
- g_w_up: bfloat16 [32, 2, 1536, 4224], P(('rep', 'dp')), parts along dimension 0
- g_w_down: bfloat16 [32, 2, 4224, 1536], P(('rep', 'dp')), parts along dimension 0
- w_gate: bfloat16 [2, 1536, 4224], replicated
- w_up: bfloat16 [2, 1536, 4224], replicated
- w_down: bfloat16 [2, 4224, 1536], replicated
- m_w_gate: float32 [2, 1536, 4224], P(None, 'dp')
- m_w_up: float32 [2, 1536, 4224], P(None, 'dp')
- m_w_down: float32 [2, 4224, 1536], P(None, 'dp')
- v_w_gate: float32 [2, 1536, 4224], P(None, 'dp')
- v_w_up: float32 [2, 1536, 4224], P(None, 'dp')
- v_w_down: float32 [2, 4224, 1536], P(None, 'dp')
Outputs:
- output 1: bfloat16 [4, 1536, 4224], P('rep'), parts along dimension 0
- output 2: bfloat16 [4, 1536, 4224], P('rep'), parts along dimension 0
- output 3: bfloat16 [4, 4224, 1536], P('rep'), parts along dimension 0
- output 4: float32 [4, 1536, 4224], P('rep', 'dp'), parts along dimension 0
- output 5: float32 [4, 1536, 4224], P('rep', 'dp'), parts along dimension 0
- output 6: float32 [4, 4224, 1536], P('rep', 'dp'), parts along dimension 0
- output 7: float32 [4, 1536, 4224], P('rep', 'dp'), parts along dimension 0
- output 8: float32 [4, 1536, 4224], P('rep', 'dp'), parts along dimension 0
- output 9: float32 [4, 4224, 1536], P('rep', 'dp'), parts along dimension 0
There are 2 independent parts. The reference program is written for one: setup_inputs(seed, part) draws one part's arguments, and reference() takes and returns one part's arrays. A program takes and returns all parts, laid end to end along the dimension named above; an argument that names none is the same for every part.
All inputs are finite; a program needn't handle non-finite values.
Results may differ from the reference program's by a relative error of at most 0.022.
Values are sent between devices in bfloat16 or wider.
A program may use at most 768 MiB of HBM per device.

```python
import jax
import jax.numpy as jnp
from jax import lax

DEVICES = 16
D = 1536
FF = 4224
LAYERS = 2
NAMES = ("w_gate", "w_up", "w_down")
SHAPES = {"w_gate": (LAYERS, D, FF), "w_up": (LAYERS, D, FF), "w_down": (LAYERS, FF, D)}


def setup_inputs(seed: int = 0, part: int = 0) -> dict:
    kz, *keys = jax.random.split(jax.random.key(seed), 1 + 5 * len(NAMES))
    loud = 2.0 ** jax.random.uniform(kz, (), jnp.float32, -1.0, 1.0)
    drawn = {}
    for name, key, both in zip(NAMES, keys[:3], keys[3:6], strict=True):
        own = jax.random.normal(jax.random.fold_in(key, part), (DEVICES, *SHAPES[name]), jnp.float32)
        shared = jax.random.normal(jax.random.fold_in(both, part), SHAPES[name], jnp.float32)
        drawn["g_" + name] = (loud * (0.7 * shared / DEVICES + 0.7 * own * DEVICES**-0.5)).astype(jnp.bfloat16)
    for name, key in zip(NAMES, keys[6:9], strict=True):
        drawn[name] = (jax.random.normal(key, SHAPES[name], jnp.float32) * SHAPES[name][1] ** -0.5).astype(jnp.bfloat16)
    for name, key in zip(NAMES, keys[9:12], strict=True):
        drawn["m_" + name] = loud * 0.5 * jax.random.normal(key, SHAPES[name], jnp.float32)
    for name, key in zip(NAMES, keys[12:15], strict=True):
        drawn["v_" + name] = loud * loud * jax.random.uniform(key, SHAPES[name], jnp.float32, 0.5, 1.5)
    return drawn


def adamw(w, m, v, g):
    m = 0.9 * m + 0.1 * g
    v = 0.95 * v + 0.05 * g * g
    step = m * lax.rsqrt(v + 1e-8) + 0.1 * w
    return (w - 0.02 * step).astype(jnp.bfloat16), m, v


def clipped(gradients, sum_of_squares, count):
    factor = jnp.minimum(1.0, 0.5 * lax.rsqrt(sum_of_squares / count + 1e-30))
    return [g * factor for g in gradients]


def reference(g_w_gate, g_w_up, g_w_down, w_gate, w_up, w_down, m_w_gate, m_w_up, m_w_down, v_w_gate, v_w_up, v_w_down):
    def total(terms):
        return lax.scan(lambda so_far, term: (so_far + term.astype(jnp.float32), None), jnp.zeros(terms.shape[1:], jnp.float32), terms)[0]

    gradients = [total(terms).astype(jnp.bfloat16).astype(jnp.float32) for terms in (g_w_gate, g_w_up, g_w_down)]
    gradients = clipped(gradients, sum(jnp.sum(g * g) for g in gradients), sum(g.size for g in gradients))
    new = [
        adamw(w.astype(jnp.float32), m, v, g)
        for w, m, v, g in zip((w_gate, w_up, w_down), (m_w_gate, m_w_up, m_w_down), (v_w_gate, v_w_up, v_w_down), gradients, strict=True)
    ]
    return tuple(one[which] for which in range(3) for one in new)
```

```python
import functools
import math

import jax
import jax.numpy as jnp
from jax import lax
from jax.experimental import pallas as pl
from jax.experimental.pallas import tpu as pltpu
from jax.sharding import PartitionSpec as P

MESH = pl.DeviceIdType.MESH
F32, BF16 = jnp.float32, jnp.bfloat16
COLOURS = range(4)
PIECES = 4


def divisor(whole, unit, most):
    return max(d for d in range(unit, most + 1, unit) if whole % d == 0)


def moments(m, v, g):
    m = 0.9 * m + 0.1 * g
    v = 0.95 * v + 0.05 * g * g
    return m, v


def new_weight(w, m, v):
    step = m * lax.rsqrt(v + 1e-8) + 0.1 * w
    return (w - 0.02 * step).astype(BF16)


def kernel(n, side, count,
           g_gate, g_up, g_down, w_gate, w_up, w_down, m_gate, m_up, m_down, v_gate, v_up, v_down,
           o_gate, o_up, o_down, og_gate, og_up, og_down, factor_ref,
           bufr, bufc, ownr, ownc, mr, mc, vr, vc, acc, sq,
           ss, rs, own_sem, mv_sem, cred1, cred2, sq_ss, sq_rs, loc_sem, ags_a, agr_a, ags_b, agr_b, agr_own, ags_own):
    layers = g_gate.shape[0]
    r, wide = bufr.shape[-2:]
    tall, quarter = bufc.shape[-2:]
    cstep = divisor(wide, 128, 384)
    rstep = divisor(tall, 8, 24)
    kinds = PIECES + layers

    me = lax.axis_index("dp")
    x, y = me // side, lax.rem(me, side)

    def around(v):
        return lax.rem(v + 4 * side, side)

    def ab(c):
        return (x, y) if c < 2 else (y, x)

    def sign(c):
        return 1 if c % 2 == 0 else -1

    def dev(c, a, b):
        return a * side + b if c < 2 else b * side + a

    def to(device):
        return {"dp": device}

    def along_a(c, k):
        a, b = ab(c)
        return dev(c, around(a + k * sign(c)), b)

    def along_b(c, k):
        a, b = ab(c)
        return dev(c, a, around(b + k * sign(c)))

    def block(c, back_a, back_b):
        a, b = ab(c)
        return dev(c, around(a - back_a * sign(c)), around(b - back_b * sign(c)))

    gates = (g_gate, g_up), (w_gate, w_up), (m_gate, m_up), (v_gate, v_up), (o_gate, o_up), (og_gate, og_up)

    def pick(which, c):
        return gates[which][c // layers], c % layers

    def cols(c):
        return pl.ds(c * quarter, quarter)

    def source(which, down, c, j, i):
        if i < PIECES:
            ref, layer = pick(which, c)
            return ref.at[layer, j, i]
        return down.at[i - PIECES, j, :, cols(c)]

    def part(r_ref, c_ref, lead, i):
        return r_ref.at[(*lead, i)] if i < PIECES else c_ref.at[(*lead, i - PIECES)]

    def buf(par, c, q, i):
        return part(bufr, bufc, (par, c, q), i)

    def own(par, c, i):
        return part(ownr, ownc, (par, c), i)

    def copy(src, dst, send, recv, device):
        return pltpu.make_async_remote_copy(src, dst, send, recv, device_id=to(device), device_id_type=MESH)

    def got(ref, sem):
        pltpu.make_async_copy(ref, ref, sem).wait()

    barrier = pltpu.get_barrier_semaphore()
    for k in range(1, n):
        pl.semaphore_signal(barrier, inc=1, device_id=to(lax.rem(me + k, n)), device_id_type=MESH)
    pl.semaphore_wait(barrier, n - 1)

    @pl.loop(0, side)
    def _(q):
        for i in range(kinds):
            for c in COLOURS:
                copy(source(0, g_down, c, block(c, 1, q + 1), i), buf(0, c, q, i), ss.at[0, c, q, i], rs.at[0, c, q, i], along_a(c, 1)).start()

    def own_load(step, which, down, c, i):
        stage, q = 1 + step // side, lax.rem(step, side)
        j = block(c, stage + 1, q + 1)
        par = lax.rem(step, 2)
        return pltpu.make_async_copy(source(which, down, c, j, i), own(par, c, i), own_sem.at[par, c, i])

    def start_own(step):
        for i in range(kinds):
            for c in COLOURS:
                own_load(step, 0, g_down, c, i).start()

    def mv_load(c, i):
        if i < PIECES:
            (m, layer), (v, _) = pick(2, c), pick(3, c)
            srcs = m.at[layer, i], v.at[layer, i]
        else:
            srcs = m_down.at[i - PIECES, :, cols(c)], v_down.at[i - PIECES, :, cols(c)]
        dsts = part(mr, mc, (c,), i), part(vr, vc, (c,), i)
        if i < PIECES:
            dsts = mr.at[c, i % 2], vr.at[c, i % 2]
        return [pltpu.make_async_copy(s, d, mv_sem.at[k, c, i]) for k, (s, d) in enumerate(zip(srcs, dsts, strict=True))]

    start_own(0)
    for i in (0, 1, *range(PIECES, kinds)):
        for c in COLOURS:
            for cp in mv_load(c, i):
                cp.start()

    def tiles(i, body):
        if i < PIECES:
            @pl.loop(0, wide // cstep)
            def _(k):
                body((slice(None), pl.ds(pl.multiple_of(k * cstep, 128), cstep)))
        else:
            @pl.loop(0, tall // rstep)
            def _(k):
                body((pl.ds(pl.multiple_of(k * rstep, 8), rstep), slice(None)))

    def add(i, dst, *more):
        def body(at):
            total = dst[at].astype(F32)
            for one in more:
                total += one[at].astype(F32)
            dst[at] = total.astype(BF16)

        tiles(i, body)

    @pl.loop(0, 2 * side)
    def _(step):
        par, q = step // side, lax.rem(step, side)
        start_own(step + 1)
        for i in range(kinds):
            for c in COLOURS:
                got(buf(par, c, q, i), rs.at[par, c, q, i])
                got(buf(par, c, q, i), ss.at[par, c, q, i])

                @pl.when(par == 1)
                def _():
                    pl.semaphore_signal(cred1.at[c], inc=1, device_id=to(along_a(c, -1)), device_id_type=MESH)

                own_load(step, 0, g_down, c, i).wait()
                add(i, buf(par, c, q, i), own(lax.rem(step, 2), c, i))
            for c in COLOURS:
                @pl.when(par == 1)
                def _():
                    pl.semaphore_wait(cred1.at[c], 1)

                copy(buf(par, c, q, i), buf(1 - par, c, q, i), ss.at[1 - par, c, q, i], rs.at[1 - par, c, q, i], along_a(c, 1)).start()

    acc[...] = jnp.zeros_like(acc)
    for q in range(side):
        step = 2 * side + q
        if q < side - 1:
            start_own(step + 1)
        else:
            for i in range(kinds):
                for c in COLOURS:
                    own_load(step + 1, 1, w_down, c, i).start() if False else None
                    pltpu.make_async_copy(source(1, w_down, c, me, i), own((step + 1) % 2, c, i), own_sem.at[(step + 1) % 2, c, i]).start()
        for i in range(kinds):
            for c in COLOURS:
                here = buf(0, c, q, i)
                got(here, rs.at[0, c, q, i])
                got(here, ss.at[0, c, q, i])
                if q < side - 1:
                    pl.semaphore_signal(cred2.at[c], inc=1, device_id=to(along_b(c, -1)), device_id_type=MESH)
                own_load(step, 0, g_down, c, i).wait()
                more = [own(step % 2, c, i)]
                if q:
                    got(here, rs.at[1, c, q - 1, i])
                    got(here, ss.at[1, c, q - 1, i])
                    more.append(buf(1, c, q - 1, i))
                if q < side - 1:
                    add(i, here, *more)
                    continue

                def last(at, here=here, more=more):
                    total = here[at].astype(F32)
                    for one in more:
                        total += one[at].astype(F32)
                    total = total.astype(BF16)
                    here[at] = total
                    square = total.astype(F32)
                    square = square * square
                    rows, columns = square.shape
                    acc[...] += sum(square[a : a + 8, b : b + 128] for a in range(0, rows, 8) for b in range(0, columns, 128))

                tiles(i, last)
            if q < side - 1:
                for c in COLOURS:
                    pl.semaphore_wait(cred2.at[c], 1)
                    copy(buf(0, c, q, i), buf(1, c, q, i), ss.at[1, c, q, i], rs.at[1, c, q, i], along_b(c, 1)).start()

    sq[me] = acc[...]

    def sq_copy(k):
        return copy(sq.at[me], sq.at[me], sq_ss.at[k], sq_rs.at[k], lax.rem(me + k, n))

    for k in range(1, n):
        sq_copy(k).start()
    for k in range(1, n):
        sq_copy(k).wait()
    total = sum(sq[k] for k in range(n))
    total = jnp.sum(total, axis=(0, 1), keepdims=True)
    factor = jnp.minimum(1.0, 0.5 * lax.rsqrt(total / count + 1e-30))
    factor_ref[...] = jnp.broadcast_to(factor, factor_ref.shape)

    last_own = (3 * side) % 2

    def out(c, j, rows):
        if rows:
            ref, layer = pick(4, c)
            return ref.at[layer, j]
        return o_down.at[:, j, :, cols(c)]

    for i in range(kinds):
        for c in COLOURS:
            rows = i < PIECES
            pltpu.make_async_copy(source(1, w_down, c, me, i), own(last_own, c, i), own_sem.at[last_own, c, i]).wait()
            for cp in mv_load(c, i):
                cp.wait()
            w_ref, g_ref = own(last_own, c, i), buf(0, c, side - 1, i)
            m_ref = mr.at[c, i % 2] if rows else mc.at[c, i - PIECES]
            v_ref = vr.at[c, i % 2] if rows else vc.at[c, i - PIECES]

            def body(at, w_ref=w_ref, g_ref=g_ref, m_ref=m_ref, v_ref=v_ref):
                g = g_ref[at].astype(F32) * factor
                m, v = moments(m_ref[at], v_ref[at], g)
                w_ref[at] = new_weight(w_ref[at].astype(F32), m, v)

            tiles(i, body)
            if i + 2 < PIECES:
                for cp in mv_load(c, i + 2):
                    cp.start()
            kind = 0 if rows else 1
            there = source(4, o_down, c, me, i)
            copy(w_ref, there, ags_own.at[0, c, i], agr_own.at[0, c, i], along_b(c, 1)).start()
            copy(w_ref, there, ags_own.at[1, c, i], agr_own.at[1, c, i], along_a(c, 1)).start()
            pltpu.make_async_copy(w_ref, there, loc_sem.at[0, c, i]).start()
            og = pick(5, c)[0].at[pick(5, c)[1], i] if rows else og_down.at[i - PIECES, :, cols(c)]
            pltpu.make_async_copy(g_ref, og, loc_sem.at[1, c, i]).start()

    for hop in range(1, side):
        for rows in (True, False):
            kind = 0 if rows else 1
            for c in COLOURS:
                here = out(c, block(c, 0, hop), rows)
                if hop == 1:
                    for i in range(kinds):
                        if (i < PIECES) == rows:
                            got(own(last_own, c, i), agr_own.at[0, c, i])
                else:
                    got(here, agr_a.at[hop, c, kind])
                if hop < side - 1:
                    copy(here, here, ags_a.at[hop + 1, c, kind], agr_a.at[hop + 1, c, kind], along_b(c, 1)).start()
                copy(here, here, ags_b.at[0, c, hop, kind], agr_b.at[0, c, hop, kind], along_a(c, 1)).start()
    for hop in range(1, side):
        for q in range(side):
            for rows in (True, False):
                kind = 0 if rows else 1
                for c in COLOURS:
                    here = out(c, block(c, hop, q), rows)
                    if hop == 1 and q == 0:
                        for i in range(kinds):
                            if (i < PIECES) == rows:
                                got(own(last_own, c, i), agr_own.at[1, c, i])
                    else:
                        got(here, agr_b.at[hop - 1, c, q, kind])
                    if hop < side - 1:
                        copy(here, here, ags_b.at[hop, c, q, kind], agr_b.at[hop, c, q, kind], along_a(c, 1)).start()

    for c in COLOURS:
        for i in range(kinds):
            for k in range(2):
                got(own(last_own, c, i), ags_own.at[k, c, i])
                got(own(last_own, c, i), loc_sem.at[k, c, i])
        for rows in (True, False):
            kind = 0 if rows else 1
            here = out(c, me, rows)
            for hop in range(2, side):
                got(here, ags_a.at[hop, c, kind])
            for hop in range(side - 1):
                for q in range(side):
                    if (hop, q) != (0, 0):
                        got(here, ags_b.at[hop, c, q, kind])


def solution(mesh):
    n = mesh.shape["dp"]
    side = math.isqrt(n)

    def step(*arrays):
        terms, weights, m, v = (arrays[i : i + 3] for i in (0, 3, 6, 9))
        layers, rows, wide = m[0].shape
        tall, narrow = m[2].shape[1:]
        assert side * side == n and layers * 2 == len(COLOURS), (n, layers)
        r, quarter = rows // PIECES, narrow // len(COLOURS)
        kinds = PIECES + layers

        def cut(whole):
            a, b, c = (w.reshape(layers, n, *shape) for w, shape in zip(whole, ((PIECES, r, wide),) * 2 + ((tall, narrow),), strict=True))
            return a, b, c

        def cut_own(blocks):
            return (*(one.reshape(layers, PIECES, r, wide) for one in blocks[:2]), blocks[2])

        args = (*cut([t[0] for t in terms]), *cut(weights), *cut_own(m), *cut_own(v))
        whole_shapes = [jax.ShapeDtypeStruct((layers, n, PIECES, r, wide), BF16)] * 2 + [jax.ShapeDtypeStruct((layers, n, tall, narrow), BF16)]
        own_shapes = [jax.ShapeDtypeStruct((layers, PIECES, r, wide), BF16)] * 2 + [jax.ShapeDtypeStruct((layers, tall, narrow), BF16)]
        count = float(n * sum(one.size for one in m))
        dma = pltpu.SemaphoreType.DMA
        anywhere = pl.BlockSpec(memory_space=pl.ANY)
        results = pl.pallas_call(
            functools.partial(kernel, n, side, count),
            name="sum_step_gather",
            out_shape=(*whole_shapes, *own_shapes, jax.ShapeDtypeStruct((8, 128), F32)),
            in_specs=[anywhere] * 12,
            out_specs=[anywhere] * 6 + [pl.BlockSpec(memory_space=pltpu.VMEM)],
            scratch_shapes=[
                pltpu.VMEM((2, 4, side, PIECES, r, wide), BF16),
                pltpu.VMEM((2, 4, side, layers, tall, quarter), BF16),
                pltpu.VMEM((2, 4, PIECES, r, wide), BF16),
                pltpu.VMEM((2, 4, layers, tall, quarter), BF16),
                pltpu.VMEM((4, 2, r, wide), F32),
                pltpu.VMEM((4, layers, tall, quarter), F32),
                pltpu.VMEM((4, 2, r, wide), F32),
                pltpu.VMEM((4, layers, tall, quarter), F32),
                pltpu.VMEM((8, 128), F32),
                pltpu.VMEM((n, 8, 128), F32),
                dma((2, 4, side, kinds)),
                dma((2, 4, side, kinds)),
                dma((2, 4, kinds)),
                dma((2, 4, kinds)),
                pltpu.SemaphoreType.REGULAR((4,)),
                pltpu.SemaphoreType.REGULAR((4,)),
                dma((n,)),
                dma((n,)),
                dma((2, 4, kinds)),
                dma((side, 4, 2)),
                dma((side, 4, 2)),
                dma((side, 4, side, 2)),
                dma((side, 4, side, 2)),
                dma((2, 4, kinds)),
                dma((2, 4, kinds)),
            ],
            compiler_params=pltpu.CompilerParams(collective_id=0, has_side_effects=True, vmem_limit_bytes=66_000_000),
        )(*args)
        new_w = [one.reshape(w.shape) for one, w in zip(results[:3], weights, strict=True)]
        g = [one.reshape(old.shape).astype(F32) * results[6][0, 0] for one, old in zip(results[3:6], m, strict=True)]
        new = [moments(*one) for one in zip(m, v, g, strict=True)]
        return (*new_w, *(one[0] for one in new), *(one[1] for one in new))

    all_of, part = P(None, None, None), P(None, "dp", None)
    return jax.shard_map(
        step,
        mesh=mesh,
        in_specs=(P(("rep", "dp"), None, None, None),) * 3 + (all_of,) * 3 + (part,) * 6,
        out_specs=(P("rep", None, None),) * 3 + (P("rep", "dp", None),) * 6,
        check_vma=False,
    )
```

```python
import functools
import math

import jax
import jax.numpy as jnp
from jax import lax
from jax.experimental import pallas as pl
from jax.experimental.pallas import tpu as pltpu
from jax.sharding import PartitionSpec as P

MESH = pl.DeviceIdType.MESH
F32, BF16 = jnp.float32, jnp.bfloat16
COLOURS = range(4)
PIECES = 4
SPLIT = (3, 1)
ROWS, COLS = 0, 1


def divisor(whole, unit, most):
    return max(d for d in range(unit, most + 1, unit) if whole % d == 0)


def moments(m, v, g):
    m = 0.9 * m + 0.1 * g
    v = 0.95 * v + 0.05 * g * g
    return m, v


def new_weight(w, m, v):
    step = m * lax.rsqrt(v + 1e-8) + 0.1 * w
    return (w - 0.02 * step).astype(BF16)


class Torus:
    def __init__(self, side):
        self.side = side
        self.me = lax.axis_index("dp")
        self.x, self.y = self.me // side, lax.rem(self.me, side)

    def around(self, v):
        return lax.rem(v + 4 * self.side, self.side)

    def ab(self, c):
        return (self.x, self.y) if c < 2 else (self.y, self.x)

    def dev(self, c, a, b):
        return a * self.side + b if c < 2 else b * self.side + a

    def along_a(self, c, k):
        a, b = self.ab(c)
        return self.dev(c, self.around(a + k * sign(c)), b)

    def along_b(self, c, k):
        a, b = self.ab(c)
        return self.dev(c, a, self.around(b + k * sign(c)))

    def back(self, c, back_a, back_b):
        a, b = self.ab(c)
        return self.around(a - back_a * sign(c)), self.around(b - back_b * sign(c))

    def block(self, c, back_a, back_b):
        return self.dev(c, *self.back(c, back_a, back_b))


def sign(c):
    return 1 if c % 2 == 0 else -1


def remote(src, dst, send, recv, device):
    return pltpu.make_async_remote_copy(src, dst, send, recv, device_id={"dp": device}, device_id_type=MESH)


def local(src, dst, sem):
    return pltpu.make_async_copy(src, dst, sem)


def got(ref, sem):
    pltpu.make_async_copy(ref, ref, sem).wait()


def tell(sem, device):
    pl.semaphore_signal(sem, inc=1, device_id={"dp": device}, device_id_type=MESH)


def main_kernel(n, side, count,
                g_gate, g_up, g_down, w_gate, w_up, w_down, m_gate, m_up, m_down, v_gate, v_up, v_down,
                o_gate, o_up, o_down, og_gate, og_up, og_down, factor_ref, *rest):
    stay, rest = rest[: len(SPLIT) * 4], rest[len(SPLIT) * 4 :]
    bufr, bufc, ownr, ownc, mr, mc, vr, vc, acc, sq, rs, ss, p2r, p2s, own_sem, mv_sem, cred1, cred2, sq_sem, loc = rest
    layers = g_gate.shape[0]
    wide = bufr.shape[-1]
    tall, quarter = bufc.shape[-2:]
    cstep, rstep = divisor(wide, 128, 384), divisor(tall, 8, 24)
    kinds = PIECES + layers
    t = Torus(side)
    me = t.me

    gates = (g_gate, g_up), (w_gate, w_up), (m_gate, m_up), (v_gate, v_up), (o_gate, o_up), (og_gate, og_up)
    downs = g_down, w_down, m_down, v_down, o_down, og_down
    TERM, WEIGHT, M, V, OUT, SUM = range(6)

    def pick(which, c):
        return gates[which][c // layers], c % layers

    def cols(c):
        return pl.ds(c * quarter, quarter)

    def group(which, c, kind, j):
        if kind == ROWS:
            ref, layer = pick(which, c)
            return ref.at[layer, j]
        return downs[which].at[:, j, :, cols(c)]

    def piece(which, c, i, j):
        if i < PIECES:
            ref, layer = pick(which, c)
            return ref.at[layer, j, i]
        return downs[which].at[i - PIECES, j, :, cols(c)]

    def own_group(which, c, kind):
        if kind == ROWS:
            ref, layer = pick(which, c)
            return ref.at[layer]
        return downs[which].at[:, :, cols(c)]

    def own_piece(which, c, i):
        if i < PIECES:
            ref, layer = pick(which, c)
            return ref.at[layer, i]
        return downs[which].at[i - PIECES, :, cols(c)]

    def buf(kind, *lead):
        return (bufr, bufc)[kind].at[lead]

    def own(kind, *lead):
        return (ownr, ownc)[kind].at[lead]

    def part(ref, kind, i):
        return ref.at[i if kind == ROWS else i - PIECES]

    def kind_of(i):
        return ROWS if i < PIECES else COLS

    def pieces(kind):
        return range(PIECES) if kind == ROWS else range(PIECES, kinds)

    def tiles(kind, body):
        if kind == ROWS:
            @pl.loop(0, wide // cstep)
            def _(k):
                body((slice(None), pl.ds(pl.multiple_of(k * cstep, 128), cstep)))
        else:
            @pl.loop(0, tall // rstep)
            def _(k):
                body((pl.ds(pl.multiple_of(k * rstep, 8), rstep), slice(None)))

    def add(kind, dst, *more):
        def body(at):
            total = dst[at].astype(F32)
            for one in more:
                total += one[at].astype(F32)
            dst[at] = total.astype(BF16)

        tiles(kind, body)

    barrier = pltpu.get_barrier_semaphore()
    for k in range(1, n):
        tell(barrier, lax.rem(me + k, n))
    pl.semaphore_wait(barrier, n - 1)

    @pl.loop(0, side)
    def _(q):
        for kind in (ROWS, COLS):
            for c in COLOURS:
                remote(group(TERM, c, kind, t.block(c, 1, q + 1)), buf(kind, 0, c, q), ss.at[0, c, q, kind], rs.at[0, c, q, kind], t.along_a(c, 1)).start()

    def own_load(step, c, kind):
        stage, q = 1 + step // side, lax.rem(step, side)
        par = lax.rem(step, 2)
        return local(group(TERM, c, kind, t.block(c, stage + 1, q + 1)), own(kind, par, c), own_sem.at[par, c, kind])

    def start_own(step):
        for kind in (ROWS, COLS):
            for c in COLOURS:
                own_load(step, c, kind).start()

    def mv_load(c, i):
        kind = kind_of(i)
        if kind == ROWS:
            return [
                local(own_piece(which, c, i), ref.at[c, i % 2], mv_sem.at[k, c, i % 2]) for k, (which, ref) in enumerate(((M, mr), (V, vr)))
            ]
        return [local(own_group(which, c, COLS), ref.at[c], mv_sem.at[k, c, 2]) for k, (which, ref) in enumerate(((M, mc), (V, vc)))]

    start_own(0)
    for i in (0, 1, PIECES):
        for c in COLOURS:
            for copy in mv_load(c, i):
                copy.start()

    @pl.loop(0, 2 * side)
    def _(step):
        par, q = step // side, lax.rem(step, side)
        start_own(step + 1)
        for kind in (ROWS, COLS):
            for c in COLOURS:
                here = buf(kind, par, c, q)
                got(here, rs.at[par, c, q, kind])
                got(here, ss.at[par, c, q, kind])

                @pl.when(par == 1)
                def _():
                    tell(cred1.at[c], t.along_a(c, -1))

                own_load(step, c, kind).wait()
                mine = own(kind, lax.rem(step, 2), c)
                for i in pieces(kind):
                    add(kind, part(here, kind, i), part(mine, kind, i))
            for c in COLOURS:
                @pl.when(par == 1)
                def _():
                    pl.semaphore_wait(cred1.at[c], 1)

                remote(buf(kind, par, c, q), buf(kind, 1 - par, c, q), ss.at[1 - par, c, q, kind], rs.at[1 - par, c, q, kind], t.along_a(c, 1)).start()

    acc[...] = jnp.zeros_like(acc)
    last_own = (3 * side) % 2
    for q in range(side):
        step = 2 * side + q
        if q < side - 1:
            start_own(step + 1)
        else:
            for kind in (ROWS, COLS):
                for c in COLOURS:
                    local(group(WEIGHT, c, kind, me), own(kind, last_own, c), own_sem.at[last_own, c, kind]).start()
        for i in range(kinds):
            kind = kind_of(i)
            first = i == pieces(kind)[0]
            for c in COLOURS:
                whole, mine = buf(kind, 0, c, q), own(kind, step % 2, c)
                here = part(whole, kind, i)
                if first:
                    got(whole, rs.at[0, c, q, kind])
                    got(whole, ss.at[0, c, q, kind])
                    own_load(step, c, kind).wait()
                more = [part(mine, kind, i)]
                if q:
                    got(here, p2r.at[c, i])
                    got(here, p2s.at[c, i])
                    more.append(part(buf(kind, 1, c, q - 1), kind, i))
                if q < side - 1:
                    tell(cred2.at[c], t.along_b(c, -1))
                    add(kind, here, *more)
                    continue

                def last(at, here=here, more=more):
                    total = here[at].astype(F32)
                    for one in more:
                        total += one[at].astype(F32)
                    total = total.astype(BF16)
                    here[at] = total
                    square = total.astype(F32)
                    square = square * square
                    rows, columns = square.shape
                    acc[...] += sum(square[a : a + 8, b : b + 128] for a in range(0, rows, 8) for b in range(0, columns, 128))

                tiles(kind, last)
            if q < side - 1:
                for c in COLOURS:
                    pl.semaphore_wait(cred2.at[c], 1)
                    remote(part(buf(kind, 0, c, q), kind, i), part(buf(kind, 1, c, q), kind, i), p2s.at[c, i], p2r.at[c, i], t.along_b(c, 1)).start()

    sq[me] = acc[...]
    for k in range(1, n):
        remote(sq.at[me], sq.at[me], sq_sem.at[0], sq_sem.at[1], lax.rem(me + k, n)).start()
    got(sq.at[pl.ds(0, n - 1)], sq_sem.at[1])
    total = sum(sq[k] for k in range(n))
    total = jnp.sum(total, axis=(0, 1), keepdims=True)
    factor = jnp.minimum(1.0, 0.5 * lax.rsqrt(total / count + 1e-30))
    factor_ref[...] = jnp.broadcast_to(factor, factor_ref.shape)

    def arrived_b(c, hop, kind):
        return p2r.at[c, 2 * (hop - 1) + kind]

    def arrived_a(c, hop, q, kind):
        return rs.at[hop - 1, c, q, kind]

    def sent(c, kind):
        return p2s.at[c, kind]

    for i in range(kinds):
        kind = kind_of(i)
        for c in COLOURS:
            if i == pieces(kind)[0]:
                local(group(WEIGHT, c, kind, me), own(kind, last_own, c), own_sem.at[last_own, c, kind]).wait()
            if i <= PIECES:
                for copy in mv_load(c, i):
                    copy.wait()
            w_ref, g_ref = (part(ref, kind, i) for ref in (own(kind, last_own, c), buf(kind, 0, c, side - 1)))
            m_ref, v_ref = (rows.at[c, i % 2] if kind == ROWS else columns.at[c, i - PIECES] for rows, columns in ((mr, mc), (vr, vc)))

            def body(at, w_ref=w_ref, g_ref=g_ref, m_ref=m_ref, v_ref=v_ref):
                g = g_ref[at].astype(F32) * factor
                m, v = moments(m_ref[at], v_ref[at], g)
                w_ref[at] = new_weight(w_ref[at].astype(F32), m, v)

            tiles(kind, body)
            if i + 2 < PIECES:
                for copy in mv_load(c, i + 2):
                    copy.start()
            there = piece(OUT, c, i, me)
            remote(w_ref, there, sent(c, kind), arrived_b(c, 1, kind), t.along_b(c, 1)).start()
            remote(w_ref, there, sent(c, kind), arrived_a(c, 1, 0, kind), t.along_a(c, 1)).start()
            local(w_ref, there, loc.at[0, c, kind]).start()
            local(g_ref, own_piece(SUM, c, i), loc.at[1, c, kind]).start()

    for hop in range(1, side):
        for kind in (ROWS, COLS):
            for c in COLOURS:
                here = group(OUT, c, kind, t.block(c, 0, hop))
                got(here, arrived_b(c, hop, kind))
                if hop < side - 1:
                    remote(here, here, sent(c, kind), arrived_b(c, hop + 1, kind), t.along_b(c, 1)).start()
                remote(here, here, sent(c, kind), arrived_a(c, 1, hop, kind), t.along_a(c, 1)).start()

    def staying(c, k, b):
        return stay[c * len(SPLIT) + k].at[b]

    starts = [sum(SPLIT[:k]) for k in range(len(SPLIT))]
    final = own_sem.at[0]
    for hop in range(1, side - 1):
        for q in range(side):
            for kind in (ROWS, COLS):
                for c in COLOURS:
                    a, b = t.back(c, hop, q)
                    here = group(OUT, c, kind, t.dev(c, a, b))
                    got(here, arrived_a(c, hop, q, kind))
                    next_hop = functools.partial(remote, send=sent(c, kind), device=t.along_a(c, 1))
                    if hop < side - 2 and (kind == COLS or hop < side - 3):
                        next_hop(here, here, recv=arrived_a(c, hop + 1, q, kind)).start()
                    elif hop == side - 3:
                        for k, size in enumerate(SPLIT):
                            next_hop(here.at[pl.ds(starts[k], size)], staying(c, k, b), recv=arrived_a(c, hop + 1, q, kind)).start()
                    elif kind == COLS:
                        next_hop(here, here, recv=final.at[c, COLS]).start()
    for c in COLOURS:
        got(o_down.at[:, pl.ds(0, side), :, cols(c)], final.at[c, COLS])

    got(sq.at[pl.ds(0, n - 1)], sq_sem.at[0])
    for c in COLOURS:
        for kind in (ROWS, COLS):
            for k in range(2):
                got(own(kind, last_own, c), loc.at[k, c, kind])
        ref, layer = pick(OUT, c)
        got(ref.at[layer, pl.ds(0, n - 1 - side)], sent(c, ROWS))
        got(o_down.at[:, pl.ds(0, n - 1), :, cols(c)], sent(c, COLS))


def copy_kernel(side, t_gate, t_up, t_down, g_gate, g_up, g_down, factor_ref, m_gate, m_up, m_down, v_gate, v_up, v_down, *rest):
    stay, rest = rest[: 4 * len(SPLIT)], rest[4 * len(SPLIT) :]
    o_gate, o_up, o_down, nm_gate, nm_up, nm_down, nv_gate, nv_up, nv_down, rowbuf, colbuf, gr, gc, mr, mc, vr, vc, load_sem, store_sem = rest
    layers = o_down.shape[0]
    wide = gr.shape[-1]
    tall, narrow = gc.shape[-2:]
    t = Torus(side)
    factor = factor_ref[0:1, 0:1]

    def at_a(ref, layer, c, a, pieces=None):
        ref = ref.at[layer, a] if c < 2 else ref.at[layer, :, a]
        return ref if pieces is None else ref.at[:, pl.ds(*pieces)]

    jobs = []
    slots = {"rows": (rowbuf, 0), "cols": (colbuf, 1)}
    made = {"rows": 0, "cols": 0, "mr": 0, "mc": 0}
    depth = {"rows": rowbuf.shape[0], "cols": colbuf.shape[0], "mr": gr.shape[0], "mc": gc.shape[0]}
    base = {"rows": 0, "cols": depth["rows"], "mr": depth["rows"] + depth["cols"], "mc": depth["rows"] + depth["cols"] + depth["mr"]}

    def job(what, loads, stores, work=None):
        slot = made[what] % depth[what]
        made[what] += 1
        jobs.append((what, slot, [f(slot) for f in loads], [f(slot) for f in stores], work and functools.partial(work, slot)))

    def copy_job(what, src, dst):
        ref = slots[what][0]
        job(what, [lambda slot: (src, ref.at[slot])], [lambda slot: (ref.at[slot], dst)])

    def step(gs, ms, vs, parts, where, slot):
        @pl.loop(0, parts)
        def _(k):
            at = (slot, *where(k))
            g = gs[at].astype(F32) * factor
            ms[at], vs[at] = moments(ms[at], vs[at], g)

    def moment_job(what, g, m, v, nm, nv):
        gs, ms, vs = (gr, mr, vr) if what == "mr" else (gc, mc, vc)
        if what == "mr":
            size = divisor(wide, 128, 384)
            parts = gs.shape[1] * (wide // size)
            each = wide // size
            where = lambda k: (k // each, slice(None), pl.ds(pl.multiple_of(lax.rem(k, each) * size, 128), size))
        else:
            size = divisor(tall, 8, 24)
            parts = tall // size
            where = lambda k: (pl.ds(pl.multiple_of(k * size, 8), size), slice(None))
        job(
            what,
            [lambda slot: (g, gs.at[slot]), lambda slot: (m, ms.at[slot]), lambda slot: (v, vs.at[slot])],
            [lambda slot: (ms.at[slot], nm), lambda slot: (vs.at[slot], nv)],
            functools.partial(step, gs, ms, vs, parts, where),
        )

    big = ((t_gate, o_gate), (t_up, o_up))
    small = ((g_gate, m_gate, v_gate, nm_gate, nv_gate), (g_up, m_up, v_up, nm_up, nv_up), (g_down, m_down, v_down, nm_down, nv_down))
    for c in COLOURS:
        layer = c % layers
        src, dst = big[c // layers]
        for back in range(side - 2):
            a, _ = t.back(c, back, 0)
            copy_job("rows", at_a(src, layer, c, a), at_a(dst, layer, c, a))
        moment_job("mr", *(one.at[layer] for one in small[c // layers]))
        a, _ = t.back(c, side - 2, 0)
        ref = rowbuf
        first = 0
        parts = []
        for k, size in enumerate(SPLIT):
            parts.append((stay[c * len(SPLIT) + k], first, size))
            first += size
        job(
            "rows",
            [lambda slot, s=s, f=f, z=z: (s, ref.at[slot, :, pl.ds(f, z)]) for s, f, z in parts],
            [lambda slot, layer=layer, c=c, a=a, dst=dst: (ref.at[slot], at_a(dst, layer, c, a))],
        )
        for k in range(2):
            copy_job("cols", t_down.at[layer, 2 * (c // layers) + k], o_down.at[layer, 2 * (c // layers) + k])
        if c // layers == 1:
            moment_job("mc", *(one.at[layer] for one in small[2]))

    def copies(k, which):
        what, slot = jobs[k][:2]
        sem = (load_sem, store_sem)[which]
        return [local(src, dst, sem.at[base[what] + slot, z]) for z, (src, dst) in enumerate(jobs[k][2 + which])]

    ahead, stored = 4, [False] * len(jobs)

    def start_loads(k):
        for one in range(k):
            if jobs[one][:2] == jobs[k][:2] and not stored[one]:
                for copy in copies(one, 1):
                    copy.wait()
                stored[one] = True
        for copy in copies(k, 0):
            copy.start()

    for k in range(ahead):
        start_loads(k)
    for k, (*_, work) in enumerate(jobs):
        for copy in copies(k, 0):
            copy.wait()
        if work is not None:
            work()
        for copy in copies(k, 1):
            copy.start()
        if k + ahead < len(jobs):
            start_loads(k + ahead)
    for k in range(len(jobs)):
        if not stored[k]:
            for copy in copies(k, 1):
                copy.wait()


def place_kernel(side, first, size, in_gate, in_up, r0, r1, r2, r3, o_gate, o_up, sem):
    del in_gate, in_up
    t = Torus(side)
    layers = o_gate.shape[0]
    moves = []
    for c, src in enumerate((r0, r1, r2, r3)):
        a, _ = t.back(c, side - 1, 0)
        dst = (o_gate, o_up)[c // layers]
        dst = dst.at[c % layers, a] if c < 2 else dst.at[c % layers, :, a]
        moves.append(local(src, dst.at[:, pl.ds(first, size)], sem.at[c]))
    for move in moves:
        move.start()
    for move in moves:
        move.wait()


def solution(mesh):
    n = mesh.shape["dp"]
    side = math.isqrt(n)
    dma = pltpu.SemaphoreType.DMA
    anywhere, in_vmem = pl.BlockSpec(memory_space=pl.ANY), pl.BlockSpec(memory_space=pltpu.VMEM)

    def shape(*dims, dtype=BF16):
        return jax.ShapeDtypeStruct(dims, dtype)

    def in_hbm(*some):
        return [pltpu.with_memory_space_constraint(one, pltpu.HBM) for one in some]

    def permutation(c):
        moved = []
        for i in range(n):
            a, b = (i // side, i % side) if c < 2 else (i % side, i // side)
            a = (a + sign(c)) % side
            moved.append((i, a * side + b if c < 2 else b * side + a))
        return moved

    def step(*arrays):
        terms, weights, m, v = (arrays[i : i + 3] for i in (0, 3, 6, 9))
        layers, rows, wide = m[0].shape
        tall, narrow = m[2].shape[1:]
        assert side == 4 and side * side == n and layers * 2 == len(COLOURS), (n, layers)
        r, quarter = rows // PIECES, narrow // len(COLOURS)
        kinds = PIECES + layers
        block, low_block = (PIECES, r, wide), (tall, narrow)

        def cut(whole, *lead):
            return [one.reshape(layers, *lead, *dims) for one, dims in zip(whole, (block, block, low_block), strict=True)]

        m, v = cut(m), cut(v)
        stays = [shape(side, size, r, wide) for _ in COLOURS for size in SPLIT]
        out = pl.pallas_call(
            functools.partial(main_kernel, n, side, float(n * sum(one.size for one in m))),
            name="sum_step_gather",
            out_shape=(
                *(shape(layers, n, *block),) * 2, shape(layers, n, *low_block),
                *(shape(layers, *block),) * 2, shape(layers, *low_block),
                shape(8, 128, dtype=F32), *stays,
            ),
            in_specs=[anywhere] * 12,
            out_specs=[anywhere] * 6 + [in_vmem] + [anywhere] * len(stays),
            scratch_shapes=[
                pltpu.VMEM((2, 4, side, *block), BF16),
                pltpu.VMEM((2, 4, side, layers, tall, quarter), BF16),
                pltpu.VMEM((2, 4, *block), BF16),
                pltpu.VMEM((2, 4, layers, tall, quarter), BF16),
                pltpu.VMEM((4, 2, r, wide), F32),
                pltpu.VMEM((4, layers, tall, quarter), F32),
                pltpu.VMEM((4, 2, r, wide), F32),
                pltpu.VMEM((4, layers, tall, quarter), F32),
                pltpu.VMEM((8, 128), F32),
                pltpu.VMEM((n, 8, 128), F32),
                dma((2, 4, side, 2)),
                dma((2, 4, side, 2)),
                dma((4, kinds)),
                dma((4, kinds)),
                dma((2, 4, 2)),
                dma((2, 4, 3)),
                pltpu.SemaphoreType.REGULAR((4,)),
                pltpu.SemaphoreType.REGULAR((4,)),
                dma((2,)),
                dma((2, 4, 2)),
            ],
            compiler_params=pltpu.CompilerParams(collective_id=0, has_side_effects=True, vmem_limit_bytes=66_000_000),
        )(*cut([one[0] for one in terms], n), *cut(weights, n), *m, *v)
        gathered, g, factor, stay = out[:3], out[3:6], out[6], out[7:]

        moved = [lax.ppermute(one, "dp", permutation(i // len(SPLIT))) for i, one in enumerate(stay)]

        square = (layers, side, side)
        copied = pl.pallas_call(
            functools.partial(copy_kernel, side),
            name="copy_and_moments",
            out_shape=(
                *(shape(*square, *block),) * 2, shape(*square, *low_block),
                *((shape(layers, *block, dtype=F32),) * 2 + (shape(layers, *low_block, dtype=F32),)) * 2,
            ),
            in_specs=[anywhere] * 6 + [in_vmem] + [anywhere] * (6 + len(stay)),
            out_specs=[anywhere] * 9,
            scratch_shapes=[
                pltpu.VMEM((3, side, *block), BF16),
                pltpu.VMEM((3, side, *low_block), BF16),
                pltpu.VMEM((1, *block), BF16),
                pltpu.VMEM((1, *low_block), BF16),
                pltpu.VMEM((1, *block), F32),
                pltpu.VMEM((1, *low_block), F32),
                pltpu.VMEM((1, *block), F32),
                pltpu.VMEM((1, *low_block), F32),
                dma((8, 3)),
                dma((8, 2)),
            ],
            cost_estimate=pl.CostEstimate(flops=10**9, bytes_accessed=200_000_000, transcendentals=0),
            compiler_params=pltpu.CompilerParams(vmem_limit_bytes=32_000_000),
        )(*in_hbm(*(one.reshape(*square, *one.shape[2:]) for one in gathered), *g), factor, *in_hbm(*m, *v, *stay))
        new_w, new_m, new_v = list(copied[:3]), copied[3:6], copied[6:]

        first = 0
        for k, size in enumerate(SPLIT):
            new_w[:2] = pl.pallas_call(
                functools.partial(place_kernel, side, first, size),
                name=f"place_{k}",
                out_shape=(shape(*square, *block),) * 2,
                in_specs=[anywhere] * 2 + [in_vmem] * 4,
                out_specs=[anywhere] * 2,
                scratch_shapes=[dma((4,))],
                input_output_aliases={0: 0, 1: 1},
                compiler_params=pltpu.CompilerParams(vmem_limit_bytes=16_000_000),
            )(*new_w[:2], *moved[k :: len(SPLIT)])
            first += size
        return tuple(one.reshape(old.shape) for one, old in zip((*new_w, *new_m, *new_v), (*weights, *arrays[6:]), strict=True))

    all_of, part = P(None, None, None), P(None, "dp", None)
    return jax.shard_map(
        step,
        mesh=mesh,
        in_specs=(P(("rep", "dp"), None, None, None),) * 3 + (all_of,) * 3 + (part,) * 6,
        out_specs=(P("rep", None, None),) * 3 + (P("rep", "dp", None),) * 6,
        check_vma=False,
    )
```

```python
import functools
import math

import jax
import jax.numpy as jnp
from jax import lax
from jax.experimental import pallas as pl
from jax.experimental.pallas import tpu as pltpu
from jax.sharding import PartitionSpec as P

MESH = pl.DeviceIdType.MESH
F32, BF16 = jnp.float32, jnp.bfloat16
COLOURS = range(4)
PIECES = 4
SPLIT = (3, 1)
ROWS, COLS = 0, 1


def divisor(whole, unit, most):
    return max(d for d in range(unit, most + 1, unit) if whole % d == 0)


def moments(m, v, g):
    m = 0.9 * m + 0.1 * g
    v = 0.95 * v + 0.05 * g * g
    return m, v


def new_weight(w, m, v):
    step = m * lax.rsqrt(v + 1e-8) + 0.1 * w
    return (w - 0.02 * step).astype(BF16)


class Torus:
    def __init__(self, side):
        self.side = side
        self.me = lax.axis_index("dp")
        self.x, self.y = self.me // side, lax.rem(self.me, side)

    def around(self, v):
        return lax.rem(v + 4 * self.side, self.side)

    def ab(self, c):
        return (self.x, self.y) if c < 2 else (self.y, self.x)

    def dev(self, c, a, b):
        return a * self.side + b if c < 2 else b * self.side + a

    def along_a(self, c, k):
        a, b = self.ab(c)
        return self.dev(c, self.around(a + k * sign(c)), b)

    def along_b(self, c, k):
        a, b = self.ab(c)
        return self.dev(c, a, self.around(b + k * sign(c)))

    def back(self, c, back_a, back_b):
        a, b = self.ab(c)
        return self.around(a - back_a * sign(c)), self.around(b - back_b * sign(c))

    def block(self, c, back_a, back_b):
        return self.dev(c, *self.back(c, back_a, back_b))


def sign(c):
    return 1 if c % 2 == 0 else -1


def remote(src, dst, send, recv, device):
    return pltpu.make_async_remote_copy(src, dst, send, recv, device_id={"dp": device}, device_id_type=MESH)


def local(src, dst, sem):
    return pltpu.make_async_copy(src, dst, sem)


def got(ref, sem):
    pltpu.make_async_copy(ref, ref, sem).wait()


def tell(sem, device):
    pl.semaphore_signal(sem, inc=1, device_id={"dp": device}, device_id_type=MESH)


def main_kernel(n, side, count,
                g_gate, g_up, g_down, w_gate, w_up, w_down, m_gate, m_up, m_down, v_gate, v_up, v_down,
                o_gate, o_up, o_down, og_gate, og_up, og_down, factor_ref, *rest):
    stay, low_stay, rest = rest[: len(SPLIT) * 4], rest[len(SPLIT) * 4 : len(SPLIT) * 4 + 4], rest[len(SPLIT) * 4 + 4 :]
    bufr, bufc, ownr, ownc, mr, mc, vr, vc, acc, sq, rs, ss, p2r, p2s, own_sem, mv_sem, cred1, cred2, sq_sem, loc = rest
    layers = g_gate.shape[0]
    wide = bufr.shape[-1]
    tall, quarter = bufc.shape[-2:]
    cstep, rstep = divisor(wide, 128, 384), divisor(tall, 8, 24)
    kinds = PIECES + layers
    t = Torus(side)
    me = t.me

    gates = (g_gate, g_up), (w_gate, w_up), (m_gate, m_up), (v_gate, v_up), (o_gate, o_up), (og_gate, og_up)
    downs = g_down, w_down, m_down, v_down, o_down, og_down
    TERM, WEIGHT, M, V, OUT, SUM = range(6)

    def pick(which, c):
        return gates[which][c // layers], c % layers

    def cols(c):
        return pl.ds(c * quarter, quarter)

    def group(which, c, kind, j):
        if kind == ROWS:
            ref, layer = pick(which, c)
            return ref.at[layer, j]
        return downs[which].at[:, j, :, cols(c)]

    def piece(which, c, i, j):
        if i < PIECES:
            ref, layer = pick(which, c)
            return ref.at[layer, j, i]
        return downs[which].at[i - PIECES, j, :, cols(c)]

    def own_group(which, c, kind):
        if kind == ROWS:
            ref, layer = pick(which, c)
            return ref.at[layer]
        return downs[which].at[:, :, cols(c)]

    def own_piece(which, c, i):
        if i < PIECES:
            ref, layer = pick(which, c)
            return ref.at[layer, i]
        return downs[which].at[i - PIECES, :, cols(c)]

    def buf(kind, *lead):
        return (bufr, bufc)[kind].at[lead]

    def own(kind, *lead):
        return (ownr, ownc)[kind].at[lead]

    def part(ref, kind, i):
        return ref.at[i if kind == ROWS else i - PIECES]

    def kind_of(i):
        return ROWS if i < PIECES else COLS

    def pieces(kind):
        return range(PIECES) if kind == ROWS else range(PIECES, kinds)

    def tiles(kind, body):
        if kind == ROWS:
            @pl.loop(0, wide // cstep)
            def _(k):
                body((slice(None), pl.ds(pl.multiple_of(k * cstep, 128), cstep)))
        else:
            @pl.loop(0, tall // rstep)
            def _(k):
                body((pl.ds(pl.multiple_of(k * rstep, 8), rstep), slice(None)))

    def add(kind, dst, *more):
        def body(at):
            total = dst[at].astype(F32)
            for one in more:
                total += one[at].astype(F32)
            dst[at] = total.astype(BF16)

        tiles(kind, body)

    def six(sem):
        got(bufr.at[0, 0, pl.ds(0, kinds // 3), pl.ds(0, 3)], sem)

    barrier = pltpu.get_barrier_semaphore()
    for c in COLOURS:
        tell(barrier, t.along_a(c, 1))
    pl.semaphore_wait(barrier, len(COLOURS))

    @pl.loop(0, side)
    def _(q):
        for kind in (ROWS, COLS):
            for c in COLOURS:
                remote(group(TERM, c, kind, t.block(c, 1, q + 1)), buf(kind, 0, c, q), ss.at[0, c, q], rs.at[0, c, q], t.along_a(c, 1)).start()

    def own_load(step, c, kind):
        stage, q = 1 + step // side, lax.rem(step, side)
        par = lax.rem(step, 2)
        return local(group(TERM, c, kind, t.block(c, stage + 1, q + 1)), own(kind, par, c), own_sem.at[par, c])

    def start_own(step):
        for kind in (ROWS, COLS):
            for c in COLOURS:
                own_load(step, c, kind).start()

    def mv_load(c, i):
        kind = kind_of(i)
        if kind == ROWS:
            return [local(own_piece(which, c, i), ref.at[c, i % 2], mv_sem.at[c, i % 2]) for which, ref in ((M, mr), (V, vr))]
        return [local(own_group(which, c, COLS), ref.at[c], mv_sem.at[c, 2]) for which, ref in ((M, mc), (V, vc))]

    def mv_wait(c, i):
        if kind_of(i) == ROWS:
            got(mr.at[c], mv_sem.at[c, i % 2])
        else:
            got(mc.at[pl.ds(0, 2)], mv_sem.at[c, 2])

    start_own(0)
    for i in (0, 1, PIECES):
        for c in COLOURS:
            for copy in mv_load(c, i):
                copy.start()

    @pl.loop(0, 2 * side)
    def _(step):
        par, q = step // side, lax.rem(step, side)
        start_own(step + 1)
        for c in COLOURS:
            six(rs.at[par, c, q])
            six(ss.at[par, c, q])

            @pl.when(par == 1)
            def _():
                tell(cred1.at[c], t.along_a(c, -1))

            six(own_sem.at[lax.rem(step, 2), c])
            for kind in (ROWS, COLS):
                here, mine = buf(kind, par, c, q), own(kind, lax.rem(step, 2), c)
                for i in pieces(kind):
                    add(kind, part(here, kind, i), part(mine, kind, i))
        for c in COLOURS:
            @pl.when(par == 1)
            def _():
                pl.semaphore_wait(cred1.at[c], 1)

            for kind in (ROWS, COLS):
                remote(buf(kind, par, c, q), buf(kind, 1 - par, c, q), ss.at[1 - par, c, q], rs.at[1 - par, c, q], t.along_a(c, 1)).start()

    acc[...] = jnp.zeros_like(acc)
    last_own = (3 * side) % 2
    for q in range(side):
        step = 2 * side + q
        if q < side - 1:
            start_own(step + 1)
        else:
            for kind in (ROWS, COLS):
                for c in COLOURS:
                    local(group(WEIGHT, c, kind, me), own(kind, last_own, c), own_sem.at[last_own, c]).start()
        for i in range(kinds):
            kind = kind_of(i)
            for c in COLOURS:
                whole, mine = buf(kind, 0, c, q), own(kind, step % 2, c)
                here = part(whole, kind, i)
                if i == 0:
                    six(rs.at[0, c, q])
                    six(ss.at[0, c, q])
                    six(own_sem.at[step % 2, c])
                more = [part(mine, kind, i)]
                if q:
                    got(here, p2r.at[c, i])
                    more.append(part(buf(kind, 1, c, q - 1), kind, i))
                if q < side - 1:
                    tell(cred2.at[c], t.along_b(c, -1))
                    add(kind, here, *more)
                    continue

                def last(at, here=here, more=more):
                    total = here[at].astype(F32)
                    for one in more:
                        total += one[at].astype(F32)
                    total = total.astype(BF16)
                    here[at] = total
                    square = total.astype(F32)
                    square = square * square
                    rows, columns = square.shape
                    acc[...] += sum(square[a : a + 8, b : b + 128] for a in range(0, rows, 8) for b in range(0, columns, 128))

                tiles(kind, last)
            if q < side - 1:
                for c in COLOURS:
                    pl.semaphore_wait(cred2.at[c], 1)
                    remote(part(buf(kind, 0, c, q), kind, i), part(buf(kind, 1, c, q), kind, i), p2s.at[c, kind], p2r.at[c, i], t.along_b(c, 1)).start()

    sq[me] = acc[...]
    for k in range(1, n):
        remote(sq.at[me], sq.at[me], sq_sem.at[0], sq_sem.at[1], lax.rem(me + k, n)).start()
    for c in COLOURS:
        for kind in (ROWS, COLS):
            got((bufr, bufc)[kind].at[0, c, pl.ds(0, side - 1)], p2s.at[c, kind])
    got(sq.at[pl.ds(0, n - 1)], sq_sem.at[1])
    total = sum(sq[k] for k in range(n))
    total = jnp.sum(total, axis=(0, 1), keepdims=True)
    factor = jnp.minimum(1.0, 0.5 * lax.rsqrt(total / count + 1e-30))
    factor_ref[...] = jnp.broadcast_to(factor, factor_ref.shape)

    def arrived_b(c, hop):
        return p2r.at[c, hop - 1]

    def arrived_a(c, hop, q):
        return rs.at[hop - 1, c, q]

    def sent(c, kind):
        return p2s.at[c, kind]

    for i in range(kinds):
        kind = kind_of(i)
        for c in COLOURS:
            if i == 0:
                six(own_sem.at[last_own, c])
            if i <= PIECES:
                mv_wait(c, i)
            w_ref, g_ref = (part(ref, kind, i) for ref in (own(kind, last_own, c), buf(kind, 0, c, side - 1)))
            m_ref, v_ref = (rows.at[c, i % 2] if kind == ROWS else columns.at[c, i - PIECES] for rows, columns in ((mr, mc), (vr, vc)))

            def body(at, w_ref=w_ref, g_ref=g_ref, m_ref=m_ref, v_ref=v_ref):
                g = g_ref[at].astype(F32) * factor
                m, v = moments(m_ref[at], v_ref[at], g)
                w_ref[at] = new_weight(w_ref[at].astype(F32), m, v)

            tiles(kind, body)
            if i + 2 < PIECES:
                for copy in mv_load(c, i + 2):
                    copy.start()
            there = piece(OUT, c, i, me)
            remote(w_ref, there, sent(c, kind), arrived_b(c, 1), t.along_b(c, 1)).start()
            remote(w_ref, there, sent(c, kind), arrived_a(c, 1, 0), t.along_a(c, 1)).start()
            local(w_ref, there, loc.at[0, kind]).start()
            local(g_ref, own_piece(SUM, c, i), loc.at[1, kind]).start()

    for hop in range(1, side):
        for c in COLOURS:
            six(arrived_b(c, hop))
            for kind in (ROWS, COLS):
                here = group(OUT, c, kind, t.block(c, 0, hop))
                if hop < side - 1:
                    remote(here, here, sent(c, kind), arrived_b(c, hop + 1), t.along_b(c, 1)).start()
                remote(here, here, sent(c, kind), arrived_a(c, 1, hop), t.along_a(c, 1)).start()

    starts = [sum(SPLIT[:k]) for k in range(len(SPLIT))]
    for hop in range(1, side - 2):
        for q in range(side):
            for c in COLOURS:
                six(arrived_a(c, hop, q))
                a, b = t.back(c, hop, q)
                next_hop = functools.partial(remote, recv=arrived_a(c, hop + 1, q), device=t.along_a(c, 1))
                rows, columns = (group(OUT, c, kind, t.dev(c, a, b)) for kind in (ROWS, COLS))
                if hop < side - 3:
                    next_hop(rows, rows, send=sent(c, ROWS)).start()
                    next_hop(columns, columns, send=sent(c, COLS)).start()
                    continue
                for k, size in enumerate(SPLIT):
                    next_hop(rows.at[pl.ds(starts[k], size)], stay[c * len(SPLIT) + k].at[b], send=sent(c, ROWS)).start()
                next_hop(columns, low_stay[c].at[:, b], send=sent(c, COLS)).start()
    for q in range(side):
        for c in COLOURS:
            six(arrived_a(c, side - 2, q))

    got(sq.at[pl.ds(0, n - 1)], sq_sem.at[0])
    for kind in (ROWS, COLS):
        for k in range(2):
            got((ownr, ownc)[kind].at[last_own], loc.at[k, kind])
    for c in COLOURS:
        ref, layer = pick(OUT, c)
        got(ref.at[layer, pl.ds(0, n - 1 - side)], sent(c, ROWS))
        got(o_down.at[:, pl.ds(0, n - 1 - side), :, cols(c)], sent(c, COLS))


def copy_kernel(side, t_gate, t_up, t_down, g_gate, g_up, g_down, factor_ref, m_gate, m_up, m_down, v_gate, v_up, v_down, *rest):
    stay, low_stay, rest = rest[: 4 * len(SPLIT)], rest[4 * len(SPLIT) : 4 * len(SPLIT) + 4], rest[4 * len(SPLIT) + 4 :]
    o_gate, o_up, o_down, nm_gate, nm_up, nm_down, nv_gate, nv_up, nv_down, rowbuf, colbuf, gr, gc, mr, mc, vr, vc, load_sem, store_sem = rest
    layers = o_down.shape[0]
    wide = gr.shape[-1]
    tall = gc.shape[-2]
    quarter = colbuf.shape[-1]
    t = Torus(side)
    factor = factor_ref[0:1, 0:1]

    def at_a(ref, layer, c, a):
        return ref.at[layer, a] if c < 2 else ref.at[layer, :, a]

    def low_at_a(ref, c, a):
        columns = pl.ds(c * quarter, quarter)
        return ref.at[:, a, :, :, columns] if c < 2 else ref.at[:, :, a, :, columns]

    jobs = []
    slots = {"rows": (rowbuf, 0), "cols": (colbuf, 1)}
    made = {"rows": 0, "cols": 0, "mr": 0, "mc": 0}
    depth = {"rows": rowbuf.shape[0], "cols": colbuf.shape[0], "mr": gr.shape[0], "mc": gc.shape[0]}
    base = {"rows": 0, "cols": depth["rows"], "mr": depth["rows"] + depth["cols"], "mc": depth["rows"] + depth["cols"] + depth["mr"]}

    def job(what, loads, stores, work=None):
        slot = made[what] % depth[what]
        made[what] += 1
        jobs.append((what, slot, [f(slot) for f in loads], [f(slot) for f in stores], work and functools.partial(work, slot)))

    def copy_job(what, src, dst):
        ref = slots[what][0]
        job(what, [lambda slot: (src, ref.at[slot])], [lambda slot: (ref.at[slot], dst)])

    def step(gs, ms, vs, parts, where, slot):
        @pl.loop(0, parts)
        def _(k):
            at = (slot, *where(k))
            g = gs[at].astype(F32) * factor
            ms[at], vs[at] = moments(ms[at], vs[at], g)

    def moment_job(what, g, m, v, nm, nv):
        gs, ms, vs = (gr, mr, vr) if what == "mr" else (gc, mc, vc)
        if what == "mr":
            size = divisor(wide, 128, 384)
            parts = gs.shape[1] * (wide // size)
            each = wide // size
            where = lambda k: (k // each, slice(None), pl.ds(pl.multiple_of(lax.rem(k, each) * size, 128), size))
        else:
            size = divisor(tall, 8, 24)
            parts = tall // size
            where = lambda k: (pl.ds(pl.multiple_of(k * size, 8), size), slice(None))
        job(
            what,
            [lambda slot: (g, gs.at[slot]), lambda slot: (m, ms.at[slot]), lambda slot: (v, vs.at[slot])],
            [lambda slot: (ms.at[slot], nm), lambda slot: (vs.at[slot], nv)],
            functools.partial(step, gs, ms, vs, parts, where),
        )

    big = ((t_gate, o_gate), (t_up, o_up))
    small = ((g_gate, m_gate, v_gate, nm_gate, nv_gate), (g_up, m_up, v_up, nm_up, nv_up), (g_down, m_down, v_down, nm_down, nv_down))
    for c in COLOURS:
        layer = c % layers
        src, dst = big[c // layers]
        for back in range(side - 2):
            a, _ = t.back(c, back, 0)
            copy_job("rows", at_a(src, layer, c, a), at_a(dst, layer, c, a))
        moment_job("mr", *(one.at[layer] for one in small[c // layers]))
        a, _ = t.back(c, side - 2, 0)
        ref = rowbuf
        first = 0
        parts = []
        for k, size in enumerate(SPLIT):
            parts.append((stay[c * len(SPLIT) + k], first, size))
            first += size
        job(
            "rows",
            [lambda slot, s=s, f=f, z=z: (s, ref.at[slot, :, pl.ds(f, z)]) for s, f, z in parts],
            [lambda slot, layer=layer, c=c, a=a, dst=dst: (ref.at[slot], at_a(dst, layer, c, a))],
        )
        for back in range(side - 2):
            a, _ = t.back(c, back, 0)
            copy_job("cols", low_at_a(t_down, c, a), low_at_a(o_down, c, a))
        a, _ = t.back(c, side - 2, 0)
        copy_job("cols", low_stay[c], low_at_a(o_down, c, a))
        if c // layers == 1:
            moment_job("mc", *(one.at[layer] for one in small[2]))

    def copies(k, which):
        what, slot = jobs[k][:2]
        sem = (load_sem, store_sem)[which]
        return [local(src, dst, sem.at[base[what] + slot, z]) for z, (src, dst) in enumerate(jobs[k][2 + which])]

    ahead, stored = 4, [False] * len(jobs)

    def start_loads(k):
        for one in range(k):
            if jobs[one][:2] == jobs[k][:2] and not stored[one]:
                for copy in copies(one, 1):
                    copy.wait()
                stored[one] = True
        for copy in copies(k, 0):
            copy.start()

    for k in range(ahead):
        start_loads(k)
    for k, (*_, work) in enumerate(jobs):
        for copy in copies(k, 0):
            copy.wait()
        if work is not None:
            work()
        for copy in copies(k, 1):
            copy.start()
        if k + ahead < len(jobs):
            start_loads(k + ahead)
    for k in range(len(jobs)):
        if not stored[k]:
            for copy in copies(k, 1):
                copy.wait()


def place_kernel(side, first, size, in_gate, in_up, r0, r1, r2, r3, o_gate, o_up, sem):
    del in_gate, in_up
    t = Torus(side)
    layers = o_gate.shape[0]
    moves = []
    for c, src in enumerate((r0, r1, r2, r3)):
        a, _ = t.back(c, side - 1, 0)
        dst = (o_gate, o_up)[c // layers]
        dst = dst.at[c % layers, a] if c < 2 else dst.at[c % layers, :, a]
        moves.append(local(src, dst.at[:, pl.ds(first, size)], sem.at[c]))
    for move in moves:
        move.start()
    for move in moves:
        move.wait()


def low_place_kernel(side, in_down, r0, r1, r2, r3, o_down, sem):
    del in_down
    t = Torus(side)
    quarter = r0.shape[-1]
    moves = []
    for c, src in enumerate((r0, r1, r2, r3)):
        a, _ = t.back(c, side - 1, 0)
        columns = pl.ds(c * quarter, quarter)
        moves.append(local(src, o_down.at[:, a, :, :, columns] if c < 2 else o_down.at[:, :, a, :, columns], sem.at[c]))
    for move in moves:
        move.start()
    for move in moves:
        move.wait()


def solution(mesh):
    n = mesh.shape["dp"]
    side = math.isqrt(n)
    dma = pltpu.SemaphoreType.DMA
    anywhere, in_vmem = pl.BlockSpec(memory_space=pl.ANY), pl.BlockSpec(memory_space=pltpu.VMEM)

    def shape(*dims, dtype=BF16):
        return jax.ShapeDtypeStruct(dims, dtype)

    def in_hbm(*some):
        return [pltpu.with_memory_space_constraint(one, pltpu.HBM) for one in some]

    def permutation(c):
        moved = []
        for i in range(n):
            a, b = (i // side, i % side) if c < 2 else (i % side, i // side)
            a = (a + sign(c)) % side
            moved.append((i, a * side + b if c < 2 else b * side + a))
        return moved

    def step(*arrays):
        terms, weights, m, v = (arrays[i : i + 3] for i in (0, 3, 6, 9))
        layers, rows, wide = m[0].shape
        tall, narrow = m[2].shape[1:]
        assert side == 4 and side * side == n and layers * 2 == len(COLOURS), (n, layers)
        r, quarter = rows // PIECES, narrow // len(COLOURS)
        kinds = PIECES + layers
        block, low_block = (PIECES, r, wide), (tall, narrow)

        def cut(whole, *lead):
            return [one.reshape(layers, *lead, *dims) for one, dims in zip(whole, (block, block, low_block), strict=True)]

        m, v = cut(m), cut(v)
        assert r * wide == tall * quarter and kinds == 6
        stays = [shape(side, size, r, wide) for _ in COLOURS for size in SPLIT] + [shape(layers, side, tall, quarter)] * 4
        out = pl.pallas_call(
            functools.partial(main_kernel, n, side, float(n * sum(one.size for one in m))),
            name="sum_step_gather",
            out_shape=(
                *(shape(layers, n, *block),) * 2, shape(layers, n, *low_block),
                *(shape(layers, *block),) * 2, shape(layers, *low_block),
                shape(8, 128, dtype=F32), *stays,
            ),
            in_specs=[anywhere] * 12,
            out_specs=[anywhere] * 6 + [in_vmem] + [anywhere] * len(stays),
            scratch_shapes=[
                pltpu.VMEM((2, 4, side, *block), BF16),
                pltpu.VMEM((2, 4, side, layers, tall, quarter), BF16),
                pltpu.VMEM((2, 4, *block), BF16),
                pltpu.VMEM((2, 4, layers, tall, quarter), BF16),
                pltpu.VMEM((4, 2, r, wide), F32),
                pltpu.VMEM((4, layers, tall, quarter), F32),
                pltpu.VMEM((4, 2, r, wide), F32),
                pltpu.VMEM((4, layers, tall, quarter), F32),
                pltpu.VMEM((8, 128), F32),
                pltpu.VMEM((n, 8, 128), F32),
                dma((2, 4, side)),
                dma((2, 4, side)),
                dma((4, kinds)),
                dma((4, 2)),
                dma((2, 4)),
                dma((4, 3)),
                pltpu.SemaphoreType.REGULAR((4,)),
                pltpu.SemaphoreType.REGULAR((4,)),
                dma((2,)),
                dma((2, 2)),
            ],
            compiler_params=pltpu.CompilerParams(collective_id=0, has_side_effects=True, vmem_limit_bytes=66_000_000),
        )(*cut([one[0] for one in terms], n), *cut(weights, n), *m, *v)
        gathered, g, factor, stay = out[:3], out[3:6], out[6], out[7:]

        moved, order = {}, (0, 2, 1, 3)
        for k in (0, len(SPLIT), *range(1, len(SPLIT))):
            for c in order:
                moved[c, k] = lax.ppermute(stay[c * len(SPLIT) + k] if k < len(SPLIT) else stay[4 * k + c], "dp", permutation(c))

        square = (layers, side, side)
        copied = pl.pallas_call(
            functools.partial(copy_kernel, side),
            name="copy_and_moments",
            out_shape=(
                *(shape(*square, *block),) * 2, shape(*square, *low_block),
                *((shape(layers, *block, dtype=F32),) * 2 + (shape(layers, *low_block, dtype=F32),)) * 2,
            ),
            in_specs=[anywhere] * 6 + [in_vmem] + [anywhere] * (6 + len(stay)),
            out_specs=[anywhere] * 9,
            scratch_shapes=[
                pltpu.VMEM((3, side, *block), BF16),
                pltpu.VMEM((4, layers, side, tall, quarter), BF16),
                pltpu.VMEM((1, *block), BF16),
                pltpu.VMEM((1, *low_block), BF16),
                pltpu.VMEM((1, *block), F32),
                pltpu.VMEM((1, *low_block), F32),
                pltpu.VMEM((1, *block), F32),
                pltpu.VMEM((1, *low_block), F32),
                dma((9, 3)),
                dma((9, 2)),
            ],
            cost_estimate=pl.CostEstimate(flops=10**9, bytes_accessed=200_000_000, transcendentals=0),
            compiler_params=pltpu.CompilerParams(vmem_limit_bytes=32_000_000),
        )(*in_hbm(*(one.reshape(*square, *one.shape[2:]) for one in gathered), *g), factor, *in_hbm(*m, *v, *stay))
        new_w, new_m, new_v = list(copied[:3]), copied[3:6], copied[6:]

        first = 0
        for k, size in enumerate(SPLIT):
            new_w[:2] = pl.pallas_call(
                functools.partial(place_kernel, side, first, size),
                name=f"place_{k}",
                out_shape=(shape(*square, *block),) * 2,
                in_specs=[anywhere] * 2 + [in_vmem] * 4,
                out_specs=[anywhere] * 2,
                scratch_shapes=[dma((4,))],
                input_output_aliases={0: 0, 1: 1},
                compiler_params=pltpu.CompilerParams(vmem_limit_bytes=16_000_000),
            )(*new_w[:2], *(moved[c, k] for c in COLOURS))
            first += size
            if k == 0:
                new_w[2] = pl.pallas_call(
                    functools.partial(low_place_kernel, side),
                    name="place_low",
                    out_shape=shape(*square, *low_block),
                    in_specs=[anywhere] + [in_vmem] * 4,
                    out_specs=anywhere,
                    scratch_shapes=[dma((4,))],
                    input_output_aliases={0: 0},
                    compiler_params=pltpu.CompilerParams(vmem_limit_bytes=16_000_000),
                )(new_w[2], *(moved[c, len(SPLIT)] for c in COLOURS))
        return tuple(one.reshape(old.shape) for one, old in zip((*new_w, *new_m, *new_v), (*weights, *arrays[6:]), strict=True))

    all_of, part = P(None, None, None), P(None, "dp", None)
    return jax.shard_map(
        step,
        mesh=mesh,
        in_specs=(P(("rep", "dp"), None, None, None),) * 3 + (all_of,) * 3 + (part,) * 6,
        out_specs=(P("rep", None, None),) * 3 + (P("rep", "dp", None),) * 6,
        check_vma=False,
    )
```

```python
import functools
import math

import jax
import jax.numpy as jnp
from jax import lax
from jax.experimental import pallas as pl
from jax.experimental.pallas import tpu as pltpu
from jax.sharding import PartitionSpec as P

MESH = pl.DeviceIdType.MESH
F32, BF16 = jnp.float32, jnp.bfloat16
COLOURS = range(4)
PIECES = 4
SPLIT = (3, 1)
ROWS, COLS = 0, 1
LATE_CORE, LATE_BY = 0, 8_000


def divisor(whole, unit, most):
    return max(d for d in range(unit, most + 1, unit) if whole % d == 0)


def moments(m, v, g):
    m = 0.9 * m + 0.1 * g
    v = 0.95 * v + 0.05 * g * g
    return m, v


def new_weight(w, m, v):
    step = m * lax.rsqrt(v + 1e-8) + 0.1 * w
    return (w - 0.02 * step).astype(BF16)


class Torus:
    def __init__(self, side):
        self.side = side
        self.me = lax.axis_index("dp")
        self.x, self.y = self.me // side, lax.rem(self.me, side)

    def around(self, v):
        return lax.rem(v + 4 * self.side, self.side)

    def ab(self, c):
        return (self.x, self.y) if c < 2 else (self.y, self.x)

    def dev(self, c, a, b):
        return a * self.side + b if c < 2 else b * self.side + a

    def along_a(self, c, k):
        a, b = self.ab(c)
        return self.dev(c, self.around(a + k * sign(c)), b)

    def along_b(self, c, k):
        a, b = self.ab(c)
        return self.dev(c, a, self.around(b + k * sign(c)))

    def back(self, c, back_a, back_b):
        a, b = self.ab(c)
        return self.around(a - back_a * sign(c)), self.around(b - back_b * sign(c))

    def block(self, c, back_a, back_b):
        return self.dev(c, *self.back(c, back_a, back_b))


def sign(c):
    return 1 if c % 2 == 0 else -1


def remote(src, dst, send, recv, device):
    return pltpu.make_async_remote_copy(src, dst, send, recv, device_id={"dp": device}, device_id_type=MESH)


def local(src, dst, sem):
    return pltpu.make_async_copy(src, dst, sem)


def got(ref, sem):
    pltpu.make_async_copy(ref, ref, sem).wait()


def tell(sem, device):
    pl.semaphore_signal(sem, inc=1, device_id={"dp": device}, device_id_type=MESH)


def main_kernel(n, side, count,
                g_gate, g_up, g_down, w_gate, w_up, w_down, m_gate, m_up, m_down, v_gate, v_up, v_down,
                o_gate, o_up, o_down, og_gate, og_up, og_down, factor_ref, *rest):
    stay, low_stay, rest = rest[: len(SPLIT) * 4], rest[len(SPLIT) * 4 : len(SPLIT) * 4 + 4], rest[len(SPLIT) * 4 + 4 :]
    bufr, bufc, ownr, ownc, mr, mc, vr, vc, acc, sq, rs, ss, p2r, p2s, own_sem, mv_sem, cred1, cred2, sq_sem, loc = rest
    layers = g_gate.shape[0]
    wide = bufr.shape[-1]
    tall, quarter = bufc.shape[-2:]
    cstep, rstep = divisor(wide, 128, 384), divisor(tall, 8, 24)
    kinds = PIECES + layers
    t = Torus(side)
    me = t.me

    gates = (g_gate, g_up), (w_gate, w_up), (m_gate, m_up), (v_gate, v_up), (o_gate, o_up), (og_gate, og_up)
    downs = g_down, w_down, m_down, v_down, o_down, og_down
    TERM, WEIGHT, M, V, OUT, SUM = range(6)

    def pick(which, c):
        return gates[which][c // layers], c % layers

    def cols(c):
        return pl.ds(c * quarter, quarter)

    def group(which, c, kind, j):
        if kind == ROWS:
            ref, layer = pick(which, c)
            return ref.at[layer, j]
        return downs[which].at[:, j, :, cols(c)]

    def piece(which, c, i, j):
        if i < PIECES:
            ref, layer = pick(which, c)
            return ref.at[layer, j, i]
        return downs[which].at[i - PIECES, j, :, cols(c)]

    def own_group(which, c, kind):
        if kind == ROWS:
            ref, layer = pick(which, c)
            return ref.at[layer]
        return downs[which].at[:, :, cols(c)]

    def own_piece(which, c, i):
        if i < PIECES:
            ref, layer = pick(which, c)
            return ref.at[layer, i]
        return downs[which].at[i - PIECES, :, cols(c)]

    def buf(kind, *lead):
        return (bufr, bufc)[kind].at[lead]

    def own(kind, *lead):
        return (ownr, ownc)[kind].at[lead]

    def part(ref, kind, i):
        return ref.at[i if kind == ROWS else i - PIECES]

    def kind_of(i):
        return ROWS if i < PIECES else COLS

    def pieces(kind):
        return range(PIECES) if kind == ROWS else range(PIECES, kinds)

    def tiles(kind, body):
        if kind == ROWS:
            @pl.loop(0, wide // cstep)
            def _(k):
                body((slice(None), pl.ds(pl.multiple_of(k * cstep, 128), cstep)))
        else:
            @pl.loop(0, tall // rstep)
            def _(k):
                body((pl.ds(pl.multiple_of(k * rstep, 8), rstep), slice(None)))

    def add(kind, dst, *more):
        def body(at):
            total = dst[at].astype(F32)
            for one in more:
                total += one[at].astype(F32)
            dst[at] = total.astype(BF16)

        tiles(kind, body)

    def six(sem):
        got(bufr.at[0, 0, pl.ds(0, kinds // 3), pl.ds(0, 3)], sem)

    barrier = pltpu.get_barrier_semaphore()
    for c in COLOURS:
        tell(barrier, t.along_a(c, 1))
    pl.semaphore_wait(barrier, len(COLOURS))

    @pl.when(lax.rem(lax.axis_index("rep"), 2) == LATE_CORE)
    def _():
        pl.delay(LATE_BY)

    @pl.loop(0, side)
    def _(q):
        for kind in (ROWS, COLS):
            for c in COLOURS:
                remote(group(TERM, c, kind, t.block(c, 1, q + 1)), buf(kind, 0, c, q), ss.at[0, c, q], rs.at[0, c, q], t.along_a(c, 1)).start()

    def own_load(step, c, kind):
        stage, q = 1 + step // side, lax.rem(step, side)
        par = lax.rem(step, 2)
        return local(group(TERM, c, kind, t.block(c, stage + 1, q + 1)), own(kind, par, c), own_sem.at[par, c])

    def start_own(step):
        for kind in (ROWS, COLS):
            for c in COLOURS:
                own_load(step, c, kind).start()

    def mv_load(c, i):
        kind = kind_of(i)
        if kind == ROWS:
            return [local(own_piece(which, c, i), ref.at[c, i % 2], mv_sem.at[c, i % 2]) for which, ref in ((M, mr), (V, vr))]
        return [local(own_group(which, c, COLS), ref.at[c], mv_sem.at[c, 2]) for which, ref in ((M, mc), (V, vc))]

    def mv_wait(c, i):
        if kind_of(i) == ROWS:
            got(mr.at[c], mv_sem.at[c, i % 2])
        else:
            got(mc.at[pl.ds(0, 2)], mv_sem.at[c, 2])

    start_own(0)
    for i in (0, 1, PIECES):
        for c in COLOURS:
            for copy in mv_load(c, i):
                copy.start()

    @pl.loop(0, 2 * side)
    def _(step):
        par, q = step // side, lax.rem(step, side)
        start_own(step + 1)
        for c in COLOURS:
            six(rs.at[par, c, q])
            six(ss.at[par, c, q])

            @pl.when(par == 1)
            def _():
                tell(cred1.at[c], t.along_a(c, -1))

            six(own_sem.at[lax.rem(step, 2), c])
            for kind in (ROWS, COLS):
                here, mine = buf(kind, par, c, q), own(kind, lax.rem(step, 2), c)
                for i in pieces(kind):
                    add(kind, part(here, kind, i), part(mine, kind, i))
        for c in COLOURS:
            @pl.when(par == 1)
            def _():
                pl.semaphore_wait(cred1.at[c], 1)

            for kind in (ROWS, COLS):
                remote(buf(kind, par, c, q), buf(kind, 1 - par, c, q), ss.at[1 - par, c, q], rs.at[1 - par, c, q], t.along_a(c, 1)).start()

    acc[...] = jnp.zeros_like(acc)
    last_own = (3 * side) % 2
    for q in range(side):
        step = 2 * side + q
        if q < side - 1:
            start_own(step + 1)
        else:
            for kind in (ROWS, COLS):
                for c in COLOURS:
                    local(group(WEIGHT, c, kind, me), own(kind, last_own, c), own_sem.at[last_own, c]).start()
        for i in range(kinds):
            kind = kind_of(i)
            for c in COLOURS:
                whole, mine = buf(kind, 0, c, q), own(kind, step % 2, c)
                here = part(whole, kind, i)
                if i == 0:
                    six(rs.at[0, c, q])
                    six(ss.at[0, c, q])
                    six(own_sem.at[step % 2, c])
                more = [part(mine, kind, i)]
                if q:
                    got(here, p2r.at[c, i])
                    more.append(part(buf(kind, 1, c, q - 1), kind, i))
                if q < side - 1:
                    tell(cred2.at[c], t.along_b(c, -1))
                    add(kind, here, *more)
                    continue

                def last(at, here=here, more=more):
                    total = here[at].astype(F32)
                    for one in more:
                        total += one[at].astype(F32)
                    total = total.astype(BF16)
                    here[at] = total
                    square = total.astype(F32)
                    square = square * square
                    rows, columns = square.shape
                    acc[...] += sum(square[a : a + 8, b : b + 128] for a in range(0, rows, 8) for b in range(0, columns, 128))

                tiles(kind, last)
            if q < side - 1:
                for c in COLOURS:
                    pl.semaphore_wait(cred2.at[c], 1)
                    remote(part(buf(kind, 0, c, q), kind, i), part(buf(kind, 1, c, q), kind, i), p2s.at[c, kind], p2r.at[c, i], t.along_b(c, 1)).start()

    sq[me] = acc[...]
    for k in range(1, n):
        remote(sq.at[me], sq.at[me], sq_sem.at[0], sq_sem.at[1], lax.rem(me + k, n)).start()
    for c in COLOURS:
        for kind in (ROWS, COLS):
            got((bufr, bufc)[kind].at[0, c, pl.ds(0, side - 1)], p2s.at[c, kind])
    got(sq.at[pl.ds(0, n - 1)], sq_sem.at[1])
    total = sum(sq[k] for k in range(n))
    total = jnp.sum(total, axis=(0, 1), keepdims=True)
    factor = jnp.minimum(1.0, 0.5 * lax.rsqrt(total / count + 1e-30))
    factor_ref[...] = jnp.broadcast_to(factor, factor_ref.shape)

    def arrived_b(c, hop):
        return p2r.at[c, hop - 1]

    def arrived_a(c, hop, q):
        return rs.at[hop - 1, c, q]

    def sent(c, kind):
        return p2s.at[c, kind]

    for i in range(kinds):
        kind = kind_of(i)
        for c in COLOURS:
            if i == 0:
                six(own_sem.at[last_own, c])
            if i <= PIECES:
                mv_wait(c, i)
            w_ref, g_ref = (part(ref, kind, i) for ref in (own(kind, last_own, c), buf(kind, 0, c, side - 1)))
            m_ref, v_ref = (rows.at[c, i % 2] if kind == ROWS else columns.at[c, i - PIECES] for rows, columns in ((mr, mc), (vr, vc)))

            def body(at, w_ref=w_ref, g_ref=g_ref, m_ref=m_ref, v_ref=v_ref):
                g = g_ref[at].astype(F32) * factor
                m, v = moments(m_ref[at], v_ref[at], g)
                w_ref[at] = new_weight(w_ref[at].astype(F32), m, v)

            tiles(kind, body)
            if i + 2 < PIECES:
                for copy in mv_load(c, i + 2):
                    copy.start()
            there = piece(OUT, c, i, me)
            remote(w_ref, there, sent(c, kind), arrived_b(c, 1), t.along_b(c, 1)).start()
            remote(w_ref, there, sent(c, kind), arrived_a(c, 1, 0), t.along_a(c, 1)).start()
            local(w_ref, there, loc.at[0, kind]).start()
            local(g_ref, own_piece(SUM, c, i), loc.at[1, kind]).start()

    for hop in range(1, side):
        for c in COLOURS:
            six(arrived_b(c, hop))
            for kind in (ROWS, COLS):
                here = group(OUT, c, kind, t.block(c, 0, hop))
                if hop < side - 1:
                    remote(here, here, sent(c, kind), arrived_b(c, hop + 1), t.along_b(c, 1)).start()
                remote(here, here, sent(c, kind), arrived_a(c, 1, hop), t.along_a(c, 1)).start()

    starts = [sum(SPLIT[:k]) for k in range(len(SPLIT))]
    for hop in range(1, side - 2):
        for q in range(side):
            for c in COLOURS:
                six(arrived_a(c, hop, q))
                a, b = t.back(c, hop, q)
                next_hop = functools.partial(remote, recv=arrived_a(c, hop + 1, q), device=t.along_a(c, 1))
                rows, columns = (group(OUT, c, kind, t.dev(c, a, b)) for kind in (ROWS, COLS))
                if hop < side - 3:
                    next_hop(rows, rows, send=sent(c, ROWS)).start()
                    next_hop(columns, columns, send=sent(c, COLS)).start()
                    continue
                for k, size in enumerate(SPLIT):
                    next_hop(rows.at[pl.ds(starts[k], size)], stay[c * len(SPLIT) + k].at[b], send=sent(c, ROWS)).start()
                next_hop(columns, low_stay[c].at[:, b], send=sent(c, COLS)).start()
    for q in range(side):
        for c in COLOURS:
            six(arrived_a(c, side - 2, q))

    got(sq.at[pl.ds(0, n - 1)], sq_sem.at[0])
    for kind in (ROWS, COLS):
        for k in range(2):
            got((ownr, ownc)[kind].at[last_own], loc.at[k, kind])
    for c in COLOURS:
        ref, layer = pick(OUT, c)
        got(ref.at[layer, pl.ds(0, n - 1 - side)], sent(c, ROWS))
        got(o_down.at[:, pl.ds(0, n - 1 - side), :, cols(c)], sent(c, COLS))


def copy_kernel(side, t_gate, t_up, t_down, g_gate, g_up, g_down, factor_ref, m_gate, m_up, m_down, v_gate, v_up, v_down, *rest):
    stay, low_stay, rest = rest[: 4 * len(SPLIT)], rest[4 * len(SPLIT) : 4 * len(SPLIT) + 4], rest[4 * len(SPLIT) + 4 :]
    o_gate, o_up, o_down, nm_gate, nm_up, nm_down, nv_gate, nv_up, nv_down, rowbuf, colbuf, gr, gc, mr, mc, vr, vc, load_sem, store_sem = rest
    layers = o_down.shape[0]
    wide = gr.shape[-1]
    tall = gc.shape[-2]
    quarter = colbuf.shape[-1]
    t = Torus(side)
    factor = factor_ref[0:1, 0:1]

    def at_a(ref, layer, c, a):
        return ref.at[layer, a] if c < 2 else ref.at[layer, :, a]

    def low_at_a(ref, c, a):
        columns = pl.ds(c * quarter, quarter)
        return ref.at[:, a, :, :, columns] if c < 2 else ref.at[:, :, a, :, columns]

    jobs = []
    slots = {"rows": (rowbuf, 0), "cols": (colbuf, 1)}
    made = {"rows": 0, "cols": 0, "mr": 0, "mc": 0}
    depth = {"rows": rowbuf.shape[0], "cols": colbuf.shape[0], "mr": gr.shape[0], "mc": gc.shape[0]}
    base = {"rows": 0, "cols": depth["rows"], "mr": depth["rows"] + depth["cols"], "mc": depth["rows"] + depth["cols"] + depth["mr"]}

    def job(what, loads, stores, work=None):
        slot = made[what] % depth[what]
        made[what] += 1
        jobs.append((what, slot, [f(slot) for f in loads], [f(slot) for f in stores], work and functools.partial(work, slot)))

    def copy_job(what, src, dst):
        ref = slots[what][0]
        job(what, [lambda slot: (src, ref.at[slot])], [lambda slot: (ref.at[slot], dst)])

    def step(gs, ms, vs, parts, where, slot):
        @pl.loop(0, parts)
        def _(k):
            at = (slot, *where(k))
            g = gs[at].astype(F32) * factor
            ms[at], vs[at] = moments(ms[at], vs[at], g)

    def moment_job(what, g, m, v, nm, nv):
        gs, ms, vs = (gr, mr, vr) if what == "mr" else (gc, mc, vc)
        if what == "mr":
            size = divisor(wide, 128, 384)
            parts = gs.shape[1] * (wide // size)
            each = wide // size
            where = lambda k: (k // each, slice(None), pl.ds(pl.multiple_of(lax.rem(k, each) * size, 128), size))
        else:
            size = divisor(tall, 8, 24)
            parts = tall // size
            where = lambda k: (pl.ds(pl.multiple_of(k * size, 8), size), slice(None))
        job(
            what,
            [lambda slot: (g, gs.at[slot]), lambda slot: (m, ms.at[slot]), lambda slot: (v, vs.at[slot])],
            [lambda slot: (ms.at[slot], nm), lambda slot: (vs.at[slot], nv)],
            functools.partial(step, gs, ms, vs, parts, where),
        )

    big = ((t_gate, o_gate), (t_up, o_up))
    small = ((g_gate, m_gate, v_gate, nm_gate, nv_gate), (g_up, m_up, v_up, nm_up, nv_up), (g_down, m_down, v_down, nm_down, nv_down))
    for c in COLOURS:
        layer = c % layers
        src, dst = big[c // layers]
        for back in range(side - 2):
            a, _ = t.back(c, back, 0)
            copy_job("rows", at_a(src, layer, c, a), at_a(dst, layer, c, a))
        moment_job("mr", *(one.at[layer] for one in small[c // layers]))
        a, _ = t.back(c, side - 2, 0)
        ref = rowbuf
        first = 0
        parts = []
        for k, size in enumerate(SPLIT):
            parts.append((stay[c * len(SPLIT) + k], first, size))
            first += size
        job(
            "rows",
            [lambda slot, s=s, f=f, z=z: (s, ref.at[slot, :, pl.ds(f, z)]) for s, f, z in parts],
            [lambda slot, layer=layer, c=c, a=a, dst=dst: (ref.at[slot], at_a(dst, layer, c, a))],
        )
        for back in range(side - 2):
            a, _ = t.back(c, back, 0)
            copy_job("cols", low_at_a(t_down, c, a), low_at_a(o_down, c, a))
        a, _ = t.back(c, side - 2, 0)
        copy_job("cols", low_stay[c], low_at_a(o_down, c, a))
        if c // layers == 1:
            moment_job("mc", *(one.at[layer] for one in small[2]))

    def copies(k, which):
        what, slot = jobs[k][:2]
        sem = (load_sem, store_sem)[which]
        return [local(src, dst, sem.at[base[what] + slot, z]) for z, (src, dst) in enumerate(jobs[k][2 + which])]

    ahead, stored = 4, [False] * len(jobs)

    def start_loads(k):
        for one in range(k):
            if jobs[one][:2] == jobs[k][:2] and not stored[one]:
                for copy in copies(one, 1):
                    copy.wait()
                stored[one] = True
        for copy in copies(k, 0):
            copy.start()

    for k in range(ahead):
        start_loads(k)
    for k, (*_, work) in enumerate(jobs):
        for copy in copies(k, 0):
            copy.wait()
        if work is not None:
            work()
        for copy in copies(k, 1):
            copy.start()
        if k + ahead < len(jobs):
            start_loads(k + ahead)
    for k in range(len(jobs)):
        if not stored[k]:
            for copy in copies(k, 1):
                copy.wait()


def place_kernel(side, first, size, in_gate, in_up, r0, r1, r2, r3, o_gate, o_up, sem):
    del in_gate, in_up
    t = Torus(side)
    layers = o_gate.shape[0]
    moves = []
    for c, src in enumerate((r0, r1, r2, r3)):
        a, _ = t.back(c, side - 1, 0)
        dst = (o_gate, o_up)[c // layers]
        dst = dst.at[c % layers, a] if c < 2 else dst.at[c % layers, :, a]
        moves.append(local(src, dst.at[:, pl.ds(first, size)], sem.at[c]))
    for move in moves:
        move.start()
    for move in moves:
        move.wait()


def low_place_kernel(side, in_down, r0, r1, r2, r3, o_down, sem):
    del in_down
    t = Torus(side)
    quarter = r0.shape[-1]
    moves = []
    for c, src in enumerate((r0, r1, r2, r3)):
        a, _ = t.back(c, side - 1, 0)
        columns = pl.ds(c * quarter, quarter)
        moves.append(local(src, o_down.at[:, a, :, :, columns] if c < 2 else o_down.at[:, :, a, :, columns], sem.at[c]))
    for move in moves:
        move.start()
    for move in moves:
        move.wait()


def solution(mesh):
    n = mesh.shape["dp"]
    side = math.isqrt(n)
    dma = pltpu.SemaphoreType.DMA
    anywhere, in_vmem = pl.BlockSpec(memory_space=pl.ANY), pl.BlockSpec(memory_space=pltpu.VMEM)

    def shape(*dims, dtype=BF16):
        return jax.ShapeDtypeStruct(dims, dtype)

    def in_hbm(*some):
        return [pltpu.with_memory_space_constraint(one, pltpu.HBM) for one in some]

    def permutation(c):
        moved = []
        for i in range(n):
            a, b = (i // side, i % side) if c < 2 else (i % side, i // side)
            a = (a + sign(c)) % side
            moved.append((i, a * side + b if c < 2 else b * side + a))
        return moved

    def step(*arrays):
        terms, weights, m, v = (arrays[i : i + 3] for i in (0, 3, 6, 9))
        layers, rows, wide = m[0].shape
        tall, narrow = m[2].shape[1:]
        assert side == 4 and side * side == n and layers * 2 == len(COLOURS), (n, layers)
        r, quarter = rows // PIECES, narrow // len(COLOURS)
        kinds = PIECES + layers
        block, low_block = (PIECES, r, wide), (tall, narrow)

        def cut(whole, *lead):
            return [one.reshape(layers, *lead, *dims) for one, dims in zip(whole, (block, block, low_block), strict=True)]

        m, v = cut(m), cut(v)
        assert r * wide == tall * quarter and kinds == 6
        stays = [shape(side, size, r, wide) for _ in COLOURS for size in SPLIT] + [shape(layers, side, tall, quarter)] * 4
        out = pl.pallas_call(
            functools.partial(main_kernel, n, side, float(n * sum(one.size for one in m))),
            name="sum_step_gather",
            out_shape=(
                *(shape(layers, n, *block),) * 2, shape(layers, n, *low_block),
                *(shape(layers, *block),) * 2, shape(layers, *low_block),
                shape(8, 128, dtype=F32), *stays,
            ),
            in_specs=[anywhere] * 12,
            out_specs=[anywhere] * 6 + [in_vmem] + [anywhere] * len(stays),
            scratch_shapes=[
                pltpu.VMEM((2, 4, side, *block), BF16),
                pltpu.VMEM((2, 4, side, layers, tall, quarter), BF16),
                pltpu.VMEM((2, 4, *block), BF16),
                pltpu.VMEM((2, 4, layers, tall, quarter), BF16),
                pltpu.VMEM((4, 2, r, wide), F32),
                pltpu.VMEM((4, layers, tall, quarter), F32),
                pltpu.VMEM((4, 2, r, wide), F32),
                pltpu.VMEM((4, layers, tall, quarter), F32),
                pltpu.VMEM((8, 128), F32),
                pltpu.VMEM((n, 8, 128), F32),
                dma((2, 4, side)),
                dma((2, 4, side)),
                dma((4, kinds)),
                dma((4, 2)),
                dma((2, 4)),
                dma((4, 3)),
                pltpu.SemaphoreType.REGULAR((4,)),
                pltpu.SemaphoreType.REGULAR((4,)),
                dma((2,)),
                dma((2, 2)),
            ],
            compiler_params=pltpu.CompilerParams(collective_id=0, has_side_effects=True, vmem_limit_bytes=66_000_000),
        )(*cut([one[0] for one in terms], n), *cut(weights, n), *m, *v)
        gathered, g, factor, stay = out[:3], out[3:6], out[6], out[7:]

        moved, order = {}, (0, 2, 1, 3)
        for k in (0, len(SPLIT), *range(1, len(SPLIT))):
            for c in order:
                moved[c, k] = lax.ppermute(stay[c * len(SPLIT) + k] if k < len(SPLIT) else stay[4 * k + c], "dp", permutation(c))

        square = (layers, side, side)
        copied = pl.pallas_call(
            functools.partial(copy_kernel, side),
            name="copy_and_moments",
            out_shape=(
                *(shape(*square, *block),) * 2, shape(*square, *low_block),
                *((shape(layers, *block, dtype=F32),) * 2 + (shape(layers, *low_block, dtype=F32),)) * 2,
            ),
            in_specs=[anywhere] * 6 + [in_vmem] + [anywhere] * (6 + len(stay)),
            out_specs=[anywhere] * 9,
            scratch_shapes=[
                pltpu.VMEM((3, side, *block), BF16),
                pltpu.VMEM((4, layers, side, tall, quarter), BF16),
                pltpu.VMEM((1, *block), BF16),
                pltpu.VMEM((1, *low_block), BF16),
                pltpu.VMEM((1, *block), F32),
                pltpu.VMEM((1, *low_block), F32),
                pltpu.VMEM((1, *block), F32),
                pltpu.VMEM((1, *low_block), F32),
                dma((9, 3)),
                dma((9, 2)),
            ],
            cost_estimate=pl.CostEstimate(flops=10**9, bytes_accessed=200_000_000, transcendentals=0),
            compiler_params=pltpu.CompilerParams(vmem_limit_bytes=32_000_000),
        )(*in_hbm(*(one.reshape(*square, *one.shape[2:]) for one in gathered), *g), factor, *in_hbm(*m, *v, *stay))
        new_w, new_m, new_v = list(copied[:3]), copied[3:6], copied[6:]

        first = 0
        for k, size in enumerate(SPLIT):
            new_w[:2] = pl.pallas_call(
                functools.partial(place_kernel, side, first, size),
                name=f"place_{k}",
                out_shape=(shape(*square, *block),) * 2,
                in_specs=[anywhere] * 2 + [in_vmem] * 4,
                out_specs=[anywhere] * 2,
                scratch_shapes=[dma((4,))],
                input_output_aliases={0: 0, 1: 1},
                compiler_params=pltpu.CompilerParams(vmem_limit_bytes=16_000_000),
            )(*new_w[:2], *(moved[c, k] for c in COLOURS))
            first += size
            if k == 0:
                new_w[2] = pl.pallas_call(
                    functools.partial(low_place_kernel, side),
                    name="place_low",
                    out_shape=shape(*square, *low_block),
                    in_specs=[anywhere] + [in_vmem] * 4,
                    out_specs=anywhere,
                    scratch_shapes=[dma((4,))],
                    input_output_aliases={0: 0},
                    compiler_params=pltpu.CompilerParams(vmem_limit_bytes=16_000_000),
                )(new_w[2], *(moved[c, len(SPLIT)] for c in COLOURS))
        return tuple(one.reshape(old.shape) for one, old in zip((*new_w, *new_m, *new_v), (*weights, *arrays[6:]), strict=True))

    all_of, part = P(None, None, None), P(None, "dp", None)
    return jax.shard_map(
        step,
        mesh=mesh,
        in_specs=(P(("rep", "dp"), None, None, None),) * 3 + (all_of,) * 3 + (part,) * 6,
        out_specs=(P("rep", None, None),) * 3 + (P("rep", "dp", None),) * 6,
        check_vma=False,
    )
```

```python
import functools
import math

import jax
import jax.numpy as jnp
from jax import lax
from jax.experimental import pallas as pl
from jax.experimental.pallas import tpu as pltpu
from jax.sharding import PartitionSpec as P

MESH = pl.DeviceIdType.MESH
F32, BF16 = jnp.float32, jnp.bfloat16
COLOURS = range(4)
PIECES = 4
ROWS, COLS = 0, 1
LATE_CORE, LATE_BY = 0, 11_000


def divisor(whole, unit, most):
    return max(d for d in range(unit, most + 1, unit) if whole % d == 0)


def row_parts(r):
    rest = [(PIECES - 1, 1, 0, r - 8), (PIECES - 1, 1, r - 8, 8)] if r > 8 else [(PIECES - 1, 1, 0, r)]
    return [(0, PIECES - 1, 0, r), *rest]


def cut_rows(ref, part, lead=()):
    return ref.at[(*lead, pl.ds(*part[:2]), pl.ds(*part[2:]))]


def moments(m, v, g):
    m = 0.9 * m + 0.1 * g
    v = 0.95 * v + 0.05 * g * g
    return m, v


def new_weight(w, m, v):
    step = m * lax.rsqrt(v + 1e-8) + 0.1 * w
    return (w - 0.02 * step).astype(BF16)


class Torus:
    def __init__(self, side):
        self.side = side
        self.me = lax.axis_index("dp")
        self.x, self.y = self.me // side, lax.rem(self.me, side)

    def around(self, v):
        return lax.rem(v + 4 * self.side, self.side)

    def ab(self, c):
        return (self.x, self.y) if c < 2 else (self.y, self.x)

    def dev(self, c, a, b):
        return a * self.side + b if c < 2 else b * self.side + a

    def along_a(self, c, k):
        a, b = self.ab(c)
        return self.dev(c, self.around(a + k * sign(c)), b)

    def along_b(self, c, k):
        a, b = self.ab(c)
        return self.dev(c, a, self.around(b + k * sign(c)))

    def back(self, c, back_a, back_b):
        a, b = self.ab(c)
        return self.around(a - back_a * sign(c)), self.around(b - back_b * sign(c))

    def block(self, c, back_a, back_b):
        return self.dev(c, *self.back(c, back_a, back_b))


def sign(c):
    return 1 if c % 2 == 0 else -1


def remote(src, dst, send, recv, device):
    return pltpu.make_async_remote_copy(src, dst, send, recv, device_id={"dp": device}, device_id_type=MESH)


def local(src, dst, sem):
    return pltpu.make_async_copy(src, dst, sem)


def got(ref, sem):
    pltpu.make_async_copy(ref, ref, sem).wait()


def tell(sem, device):
    pl.semaphore_signal(sem, inc=1, device_id={"dp": device}, device_id_type=MESH)


def main_kernel(n, side, count,
                g_gate, g_up, g_down, w_gate, w_up, w_down, m_gate, m_up, m_down, v_gate, v_up, v_down,
                o_gate, o_up, o_down, og_gate, og_up, og_down, factor_ref, *rest):
    parts = row_parts(m_gate.shape[-2])
    stay, low_stay, rest = rest[: len(parts) * 4], rest[len(parts) * 4 : len(parts) * 4 + 4], rest[len(parts) * 4 + 4 :]
    first, bufr, bufc, ownr, ownc, mr, mc, vr, vc, acc, sq, rs, ss, p2r, p2s, own_sem, mv_sem, cred1, cred2, sq_sem, loc = rest
    layers = g_gate.shape[0]
    wide = bufr.shape[-1]
    tall, quarter = bufc.shape[-2:]
    cstep, rstep = divisor(wide, 128, 384), divisor(tall, 8, 24)
    kinds = PIECES + layers
    t = Torus(side)
    me = t.me

    gates = (g_gate, g_up), (w_gate, w_up), (m_gate, m_up), (v_gate, v_up), (o_gate, o_up), (og_gate, og_up)
    downs = g_down, w_down, m_down, v_down, o_down, og_down
    TERM, WEIGHT, M, V, OUT, SUM = range(6)

    def pick(which, c):
        return gates[which][c // layers], c % layers

    def cols(c):
        return pl.ds(c * quarter, quarter)

    def group(which, c, kind, j):
        if kind == ROWS:
            ref, layer = pick(which, c)
            return ref.at[layer, j]
        return downs[which].at[:, j, :, cols(c)]

    def piece(which, c, i, j):
        if i < PIECES:
            ref, layer = pick(which, c)
            return ref.at[layer, j, i]
        return downs[which].at[i - PIECES, j, :, cols(c)]

    def own_group(which, c, kind):
        if kind == ROWS:
            ref, layer = pick(which, c)
            return ref.at[layer]
        return downs[which].at[:, :, cols(c)]

    def own_piece(which, c, i):
        if i < PIECES:
            ref, layer = pick(which, c)
            return ref.at[layer, i]
        return downs[which].at[i - PIECES, :, cols(c)]

    def buf(kind, *lead):
        return (bufr, bufc)[kind].at[lead]

    def own(kind, *lead):
        return (ownr, ownc)[kind].at[lead]

    def part(ref, kind, i):
        return ref.at[i if kind == ROWS else i - PIECES]

    def kind_of(i):
        return ROWS if i < PIECES else COLS

    def pieces(kind):
        return range(PIECES) if kind == ROWS else range(PIECES, kinds)

    def tiles(kind, body):
        if kind == ROWS:
            @pl.loop(0, wide // cstep)
            def _(k):
                body((slice(None), pl.ds(pl.multiple_of(k * cstep, 128), cstep)))
        else:
            @pl.loop(0, tall // rstep)
            def _(k):
                body((pl.ds(pl.multiple_of(k * rstep, 8), rstep), slice(None)))

    def add(kind, dst, *more):
        def body(at):
            total = dst[at].astype(F32)
            for one in more:
                total += one[at].astype(F32)
            dst[at] = total.astype(BF16)

        tiles(kind, body)

    def six(sem):
        got(bufr.at[0, 0, pl.ds(0, kinds // 3), pl.ds(0, 3)], sem)

    for c in COLOURS:
        local(piece(TERM, c, 0, t.block(c, 1, 1)), first.at[c], own_sem.at[1, c]).start()

    barrier = pltpu.get_barrier_semaphore()
    for c in COLOURS:
        tell(barrier, t.along_a(c, 1))
    pl.semaphore_wait(barrier, len(COLOURS))

    @pl.when(lax.rem(lax.axis_index("rep"), 2) == LATE_CORE)
    def _():
        pl.delay(LATE_BY)

    for c in COLOURS:
        got(first.at[c], own_sem.at[1, c])
        remote(first.at[c], bufr.at[0, c, 0, 0], ss.at[0, c, 0], rs.at[0, c, 0], t.along_a(c, 1)).start()
    more = pl.ds(1, PIECES - 1)
    for c in COLOURS:
        remote(group(TERM, c, ROWS, t.block(c, 1, 1)).at[more], bufr.at[0, c, 0, more], ss.at[0, c, 0], rs.at[0, c, 0], t.along_a(c, 1)).start()
    for c in COLOURS:
        remote(group(TERM, c, COLS, t.block(c, 1, 1)), bufc.at[0, c, 0], ss.at[0, c, 0], rs.at[0, c, 0], t.along_a(c, 1)).start()

    @pl.loop(1, side)
    def _(q):
        for kind in (ROWS, COLS):
            for c in COLOURS:
                remote(group(TERM, c, kind, t.block(c, 1, q + 1)), buf(kind, 0, c, q), ss.at[0, c, q], rs.at[0, c, q], t.along_a(c, 1)).start()

    def own_load(step, c, kind):
        stage, q = 1 + step // side, lax.rem(step, side)
        par = lax.rem(step, 2)
        return local(group(TERM, c, kind, t.block(c, stage + 1, q + 1)), own(kind, par, c), own_sem.at[par, c])

    def start_own(step):
        for kind in (ROWS, COLS):
            for c in COLOURS:
                own_load(step, c, kind).start()

    def mv_load(c, i):
        kind = kind_of(i)
        if kind == ROWS:
            return [local(own_piece(which, c, i), ref.at[c, i % 2], mv_sem.at[c, i % 2]) for which, ref in ((M, mr), (V, vr))]
        return [local(own_group(which, c, COLS), ref.at[c], mv_sem.at[c, 2]) for which, ref in ((M, mc), (V, vc))]

    def mv_wait(c, i):
        if kind_of(i) == ROWS:
            got(mr.at[c], mv_sem.at[c, i % 2])
        else:
            got(mc.at[pl.ds(0, 2)], mv_sem.at[c, 2])

    start_own(0)
    for i in (0, 1, PIECES):
        for c in COLOURS:
            for copy in mv_load(c, i):
                copy.start()

    @pl.loop(0, 2 * side)
    def _(step):
        par, q = step // side, lax.rem(step, side)
        start_own(step + 1)
        for c in COLOURS:
            six(rs.at[par, c, q])
            six(ss.at[par, c, q])

            @pl.when(par == 1)
            def _():
                tell(cred1.at[c], t.along_a(c, -1))

            six(own_sem.at[lax.rem(step, 2), c])
            for kind in (ROWS, COLS):
                here, mine = buf(kind, par, c, q), own(kind, lax.rem(step, 2), c)
                for i in pieces(kind):
                    add(kind, part(here, kind, i), part(mine, kind, i))
        for c in COLOURS:
            @pl.when(par == 1)
            def _():
                pl.semaphore_wait(cred1.at[c], 1)

            for kind in (ROWS, COLS):
                remote(buf(kind, par, c, q), buf(kind, 1 - par, c, q), ss.at[1 - par, c, q], rs.at[1 - par, c, q], t.along_a(c, 1)).start()

    acc[...] = jnp.zeros_like(acc)
    last_own = (3 * side) % 2
    for q in range(side):
        step = 2 * side + q
        if q < side - 1:
            start_own(step + 1)
        else:
            for kind in (ROWS, COLS):
                for c in COLOURS:
                    local(group(WEIGHT, c, kind, me), own(kind, last_own, c), own_sem.at[last_own, c]).start()
        for i in range(kinds):
            kind = kind_of(i)
            for c in COLOURS:
                whole, mine = buf(kind, 0, c, q), own(kind, step % 2, c)
                here = part(whole, kind, i)
                if i == 0:
                    six(rs.at[0, c, q])
                    six(ss.at[0, c, q])
                    six(own_sem.at[step % 2, c])
                more = [part(mine, kind, i)]
                if q:
                    got(here, p2r.at[c, i])
                    more.append(part(buf(kind, 1, c, q - 1), kind, i))
                if q < side - 1:
                    tell(cred2.at[c], t.along_b(c, -1))
                    add(kind, here, *more)
                    continue

                def last(at, here=here, more=more):
                    total = here[at].astype(F32)
                    for one in more:
                        total += one[at].astype(F32)
                    total = total.astype(BF16)
                    here[at] = total
                    square = total.astype(F32)
                    square = square * square
                    rows, columns = square.shape
                    acc[...] += sum(square[a : a + 8, b : b + 128] for a in range(0, rows, 8) for b in range(0, columns, 128))

                tiles(kind, last)
            if q < side - 1:
                for c in COLOURS:
                    pl.semaphore_wait(cred2.at[c], 1)
                    remote(part(buf(kind, 0, c, q), kind, i), part(buf(kind, 1, c, q), kind, i), p2s.at[c, kind], p2r.at[c, i], t.along_b(c, 1)).start()

    sq[me] = acc[...]
    for k in range(1, n):
        remote(sq.at[me], sq.at[me], sq_sem.at[0], sq_sem.at[1], lax.rem(me + k, n)).start()
    for c in COLOURS:
        for kind in (ROWS, COLS):
            got((bufr, bufc)[kind].at[0, c, pl.ds(0, side - 1)], p2s.at[c, kind])
    got(sq.at[pl.ds(0, n - 1)], sq_sem.at[1])
    total = sum(sq[k] for k in range(n))
    total = jnp.sum(total, axis=(0, 1), keepdims=True)
    factor = jnp.minimum(1.0, 0.5 * lax.rsqrt(total / count + 1e-30))
    factor_ref[...] = jnp.broadcast_to(factor, factor_ref.shape)

    def arrived_b(c, hop):
        return p2r.at[c, hop - 1]

    def arrived_a(c, hop, q):
        return rs.at[hop - 1, c, q]

    def sent(c, kind):
        return p2s.at[c, kind]

    for i in range(kinds):
        kind = kind_of(i)
        for c in COLOURS:
            if i == 0:
                six(own_sem.at[last_own, c])
            if i <= PIECES:
                mv_wait(c, i)
            w_ref, g_ref = (part(ref, kind, i) for ref in (own(kind, last_own, c), buf(kind, 0, c, side - 1)))
            m_ref, v_ref = (rows.at[c, i % 2] if kind == ROWS else columns.at[c, i - PIECES] for rows, columns in ((mr, mc), (vr, vc)))

            def body(at, w_ref=w_ref, g_ref=g_ref, m_ref=m_ref, v_ref=v_ref):
                g = g_ref[at].astype(F32) * factor
                m, v = moments(m_ref[at], v_ref[at], g)
                w_ref[at] = new_weight(w_ref[at].astype(F32), m, v)

            tiles(kind, body)
            if i + 2 < PIECES:
                for copy in mv_load(c, i + 2):
                    copy.start()
        for c in COLOURS:
            remote(part(own(kind, last_own, c), kind, i), piece(OUT, c, i, me), sent(c, kind), arrived_b(c, 1), t.along_b(c, 1)).start()
    for kind in (ROWS, COLS):
        for c in COLOURS:
            mine, there = own(kind, last_own, c), group(OUT, c, kind, me)
            remote(mine, there, sent(c, kind), arrived_a(c, 1, 0), t.along_a(c, 1)).start()
            local(mine, there, loc.at[0, kind]).start()
            local(buf(kind, 0, c, side - 1), own_group(SUM, c, kind), loc.at[1, kind]).start()

    for hop in range(1, side):
        for c in COLOURS:
            six(arrived_b(c, hop))
            for kind in (ROWS, COLS):
                here = group(OUT, c, kind, t.block(c, 0, hop))
                if hop < side - 1:
                    remote(here, here, sent(c, kind), arrived_b(c, hop + 1), t.along_b(c, 1)).start()
                remote(here, here, sent(c, kind), arrived_a(c, 1, hop), t.along_a(c, 1)).start()

    for hop in range(1, side - 2):
        for q in range(side):
            for c in COLOURS:
                six(arrived_a(c, hop, q))
                a, b = t.back(c, hop, q)
                next_hop = functools.partial(remote, recv=arrived_a(c, hop + 1, q), device=t.along_a(c, 1))
                rows, columns = (group(OUT, c, kind, t.dev(c, a, b)) for kind in (ROWS, COLS))
                if hop < side - 3:
                    next_hop(rows, rows, send=sent(c, ROWS)).start()
                    next_hop(columns, columns, send=sent(c, COLS)).start()
                    continue
                for k, one in enumerate(parts):
                    next_hop(cut_rows(rows, one), stay[c * len(parts) + k].at[b], send=sent(c, ROWS)).start()
                next_hop(columns, low_stay[c].at[:, b], send=sent(c, COLS)).start()
    for q in range(side):
        for c in COLOURS:
            six(arrived_a(c, side - 2, q))

    got(sq.at[pl.ds(0, n - 1)], sq_sem.at[0])
    for kind in (ROWS, COLS):
        for k in range(2):
            got((ownr, ownc)[kind].at[last_own], loc.at[k, kind])
    for c in COLOURS:
        ref, layer = pick(OUT, c)
        got(ref.at[layer, pl.ds(0, n - 1 - side)], sent(c, ROWS))
        got(o_down.at[:, pl.ds(0, n - 1 - side), :, cols(c)], sent(c, COLS))


def copy_kernel(side, t_gate, t_up, t_down, g_gate, g_up, g_down, factor_ref, m_gate, m_up, m_down, v_gate, v_up, v_down, *rest):
    parts = row_parts(m_gate.shape[-2])
    stay, low_stay, rest = rest[: 4 * len(parts)], rest[4 * len(parts) : 4 * len(parts) + 4], rest[4 * len(parts) + 4 :]
    o_gate, o_up, o_down, nm_gate, nm_up, nm_down, nv_gate, nv_up, nv_down, rowbuf, colbuf, gr, gc, mr, mc, vr, vc, load_sem, store_sem = rest
    layers = o_down.shape[0]
    wide = gr.shape[-1]
    tall = gc.shape[-2]
    quarter = colbuf.shape[-1]
    t = Torus(side)
    factor = factor_ref[0:1, 0:1]

    def at_a(ref, layer, c, a):
        return ref.at[layer, a] if c < 2 else ref.at[layer, :, a]

    def low_at_a(ref, c, a):
        columns = pl.ds(c * quarter, quarter)
        return ref.at[:, a, :, :, columns] if c < 2 else ref.at[:, :, a, :, columns]

    jobs = []
    slots = {"rows": (rowbuf, 0), "cols": (colbuf, 1)}
    made = {"rows": 0, "cols": 0, "mr": 0, "mc": 0}
    depth = {"rows": rowbuf.shape[0], "cols": colbuf.shape[0], "mr": gr.shape[0], "mc": gc.shape[0]}
    base = {"rows": 0, "cols": depth["rows"], "mr": depth["rows"] + depth["cols"], "mc": depth["rows"] + depth["cols"] + depth["mr"]}

    def job(what, loads, stores, work=None):
        slot = made[what] % depth[what]
        made[what] += 1
        jobs.append((what, slot, [f(slot) for f in loads], [f(slot) for f in stores], work and functools.partial(work, slot)))

    def copy_job(what, src, dst):
        ref = slots[what][0]
        job(what, [lambda slot: (src, ref.at[slot])], [lambda slot: (ref.at[slot], dst)])

    def step(gs, ms, vs, parts, where, slot):
        @pl.loop(0, parts)
        def _(k):
            at = (slot, *where(k))
            g = gs[at].astype(F32) * factor
            ms[at], vs[at] = moments(ms[at], vs[at], g)

    def moment_job(what, g, m, v, nm, nv):
        gs, ms, vs = (gr, mr, vr) if what == "mr" else (gc, mc, vc)
        if what == "mr":
            size = divisor(wide, 128, 384)
            parts = gs.shape[1] * (wide // size)
            each = wide // size
            where = lambda k: (k // each, slice(None), pl.ds(pl.multiple_of(lax.rem(k, each) * size, 128), size))
        else:
            size = divisor(tall, 8, 24)
            parts = tall // size
            where = lambda k: (pl.ds(pl.multiple_of(k * size, 8), size), slice(None))
        job(
            what,
            [lambda slot: (g, gs.at[slot]), lambda slot: (m, ms.at[slot]), lambda slot: (v, vs.at[slot])],
            [lambda slot: (ms.at[slot], nm), lambda slot: (vs.at[slot], nv)],
            functools.partial(step, gs, ms, vs, parts, where),
        )

    big = ((t_gate, o_gate), (t_up, o_up))
    small = ((g_gate, m_gate, v_gate, nm_gate, nv_gate), (g_up, m_up, v_up, nm_up, nv_up), (g_down, m_down, v_down, nm_down, nv_down))
    for c in COLOURS:
        layer = c % layers
        src, dst = big[c // layers]
        for back in range(side - 2):
            a, _ = t.back(c, back, 0)
            copy_job("rows", at_a(src, layer, c, a), at_a(dst, layer, c, a))
        moment_job("mr", *(one.at[layer] for one in small[c // layers]))
        a, _ = t.back(c, side - 2, 0)
        ref = rowbuf
        job(
            "rows",
            [lambda slot, src=stay[c * len(parts) + k], one=one: (src, cut_rows(ref, one, (slot, slice(None)))) for k, one in enumerate(parts)],
            [lambda slot, layer=layer, c=c, a=a, dst=dst: (ref.at[slot], at_a(dst, layer, c, a))],
        )
        for back in range(side - 2):
            a, _ = t.back(c, back, 0)
            copy_job("cols", low_at_a(t_down, c, a), low_at_a(o_down, c, a))
        a, _ = t.back(c, side - 2, 0)
        copy_job("cols", low_stay[c], low_at_a(o_down, c, a))
        if c // layers == 1:
            moment_job("mc", *(one.at[layer] for one in small[2]))

    def copies(k, which):
        what, slot = jobs[k][:2]
        sem = (load_sem, store_sem)[which]
        return [local(src, dst, sem.at[base[what] + slot, z]) for z, (src, dst) in enumerate(jobs[k][2 + which])]

    ahead, stored = 4, [False] * len(jobs)

    def start_loads(k):
        for one in range(k):
            if jobs[one][:2] == jobs[k][:2] and not stored[one]:
                for copy in copies(one, 1):
                    copy.wait()
                stored[one] = True
        for copy in copies(k, 0):
            copy.start()

    for k in range(ahead):
        start_loads(k)
    for k, (*_, work) in enumerate(jobs):
        for copy in copies(k, 0):
            copy.wait()
        if work is not None:
            work()
        for copy in copies(k, 1):
            copy.start()
        if k + ahead < len(jobs):
            start_loads(k + ahead)
    for k in range(len(jobs)):
        if not stored[k]:
            for copy in copies(k, 1):
                copy.wait()


def place_kernel(side, part, *refs):
    *ins, sem = refs
    wholes = 2 + (part[0] == 0)
    ins, outs = ins[wholes:-wholes], ins[-wholes:]
    t = Torus(side)
    layers = outs[0].shape[0]
    moves = []
    for c in COLOURS:
        a, _ = t.back(c, side - 1, 0)
        dst = outs[c // layers]
        dst = dst.at[c % layers, a] if c < 2 else dst.at[c % layers, :, a]
        moves.append(local(ins[c], cut_rows(dst, part, (slice(None),)), sem.at[c]))
        if wholes > 2:
            columns = pl.ds(c * ins[4].shape[-1], ins[4].shape[-1])
            dst = outs[2].at[:, a, :, :, columns] if c < 2 else outs[2].at[:, :, a, :, columns]
            moves.append(local(ins[4 + c], dst, sem.at[4 + c]))
    for move in moves:
        move.start()
    for move in moves:
        move.wait()


def solution(mesh):
    n = mesh.shape["dp"]
    side = math.isqrt(n)
    dma = pltpu.SemaphoreType.DMA
    anywhere, in_vmem = pl.BlockSpec(memory_space=pl.ANY), pl.BlockSpec(memory_space=pltpu.VMEM)

    def shape(*dims, dtype=BF16):
        return jax.ShapeDtypeStruct(dims, dtype)

    def in_hbm(*some):
        return [pltpu.with_memory_space_constraint(one, pltpu.HBM) for one in some]

    def permutation(c):
        moved = []
        for i in range(n):
            a, b = (i // side, i % side) if c < 2 else (i % side, i // side)
            a = (a + sign(c)) % side
            moved.append((i, a * side + b if c < 2 else b * side + a))
        return moved

    def step(*arrays):
        terms, weights, m, v = (arrays[i : i + 3] for i in (0, 3, 6, 9))
        layers, rows, wide = m[0].shape
        tall, narrow = m[2].shape[1:]
        assert side == 4 and side * side == n and layers * 2 == len(COLOURS), (n, layers)
        r, quarter = rows // PIECES, narrow // len(COLOURS)
        kinds = PIECES + layers
        block, low_block = (PIECES, r, wide), (tall, narrow)

        def cut(whole, *lead):
            return [one.reshape(layers, *lead, *dims) for one, dims in zip(whole, (block, block, low_block), strict=True)]

        m, v = cut(m), cut(v)
        assert r * wide == tall * quarter and kinds == 6
        parts = row_parts(r)
        stays = [shape(side, one[1], one[3], wide) for _ in COLOURS for one in parts] + [shape(layers, side, tall, quarter)] * 4
        out = pl.pallas_call(
            functools.partial(main_kernel, n, side, float(n * sum(one.size for one in m))),
            name="sum_step_gather",
            out_shape=(
                *(shape(layers, n, *block),) * 2, shape(layers, n, *low_block),
                *(shape(layers, *block),) * 2, shape(layers, *low_block),
                shape(8, 128, dtype=F32), *stays,
            ),
            in_specs=[anywhere] * 12,
            out_specs=[anywhere] * 6 + [in_vmem] + [anywhere] * len(stays),
            scratch_shapes=[
                pltpu.VMEM((4, r, wide), BF16),
                pltpu.VMEM((2, 4, side, *block), BF16),
                pltpu.VMEM((2, 4, side, layers, tall, quarter), BF16),
                pltpu.VMEM((2, 4, *block), BF16),
                pltpu.VMEM((2, 4, layers, tall, quarter), BF16),
                pltpu.VMEM((4, 2, r, wide), F32),
                pltpu.VMEM((4, layers, tall, quarter), F32),
                pltpu.VMEM((4, 2, r, wide), F32),
                pltpu.VMEM((4, layers, tall, quarter), F32),
                pltpu.VMEM((8, 128), F32),
                pltpu.VMEM((n, 8, 128), F32),
                dma((2, 4, side)),
                dma((2, 4, side)),
                dma((4, kinds)),
                dma((4, 2)),
                dma((2, 4)),
                dma((4, 3)),
                pltpu.SemaphoreType.REGULAR((4,)),
                pltpu.SemaphoreType.REGULAR((4,)),
                dma((2,)),
                dma((2, 2)),
            ],
            compiler_params=pltpu.CompilerParams(collective_id=0, has_side_effects=True, vmem_limit_bytes=66_000_000),
        )(*cut([one[0] for one in terms], n), *cut(weights, n), *m, *v)
        gathered, g, factor, stay = out[:3], out[3:6], out[6], out[7:]

        moved = {}
        for k in (0, len(parts), *range(1, len(parts))):
            for c in COLOURS:
                moved[c, k] = lax.ppermute(stay[c * len(parts) + k] if k < len(parts) else stay[4 * k + c], "dp", permutation(c))

        square = (layers, side, side)
        copied = pl.pallas_call(
            functools.partial(copy_kernel, side),
            name="copy_and_moments",
            out_shape=(
                *(shape(*square, *block),) * 2, shape(*square, *low_block),
                *((shape(layers, *block, dtype=F32),) * 2 + (shape(layers, *low_block, dtype=F32),)) * 2,
            ),
            in_specs=[anywhere] * 6 + [in_vmem] + [anywhere] * (6 + len(stay)),
            out_specs=[anywhere] * 9,
            scratch_shapes=[
                pltpu.VMEM((3, side, *block), BF16),
                pltpu.VMEM((4, layers, side, tall, quarter), BF16),
                pltpu.VMEM((1, *block), BF16),
                pltpu.VMEM((1, *low_block), BF16),
                pltpu.VMEM((1, *block), F32),
                pltpu.VMEM((1, *low_block), F32),
                pltpu.VMEM((1, *block), F32),
                pltpu.VMEM((1, *low_block), F32),
                dma((9, 3)),
                dma((9, 2)),
            ],
            cost_estimate=pl.CostEstimate(flops=10**9, bytes_accessed=200_000_000, transcendentals=0),
            compiler_params=pltpu.CompilerParams(vmem_limit_bytes=32_000_000),
        )(*in_hbm(*(one.reshape(*square, *one.shape[2:]) for one in gathered), *g), factor, *in_hbm(*m, *v, *stay))
        new_w, new_m, new_v = list(copied[:3]), copied[3:6], copied[6:]

        for k, one in enumerate(parts):
            wholes = 3 if k == 0 else 2
            arrived = [moved[c, k] for c in COLOURS] + [moved[c, len(parts)] for c in COLOURS if k == 0]
            new_w[:wholes] = pl.pallas_call(
                functools.partial(place_kernel, side, one),
                name=f"place_{k}",
                out_shape=[shape(*old.shape) for old in new_w[:wholes]],
                in_specs=[anywhere] * wholes + [in_vmem] * len(arrived),
                out_specs=[anywhere] * wholes,
                scratch_shapes=[dma((8,))],
                input_output_aliases={i: i for i in range(wholes)},
                compiler_params=pltpu.CompilerParams(vmem_limit_bytes=24_000_000),
            )(*new_w[:wholes], *arrived)
        return tuple(one.reshape(old.shape) for one, old in zip((*new_w, *new_m, *new_v), (*weights, *arrays[6:]), strict=True))

    all_of, part = P(None, None, None), P(None, "dp", None)
    return jax.shard_map(
        step,
        mesh=mesh,
        in_specs=(P(("rep", "dp"), None, None, None),) * 3 + (all_of,) * 3 + (part,) * 6,
        out_specs=(P("rep", None, None),) * 3 + (P("rep", "dp", None),) * 6,
        check_vma=False,
    )
```

```python
import functools
import math

import jax
import jax.numpy as jnp
from jax import lax
from jax.experimental import pallas as pl
from jax.experimental.pallas import tpu as pltpu
from jax.sharding import PartitionSpec as P

MESH = pl.DeviceIdType.MESH
F32, BF16 = jnp.float32, jnp.bfloat16
COLOURS = range(4)
PIECES = 4
ROWS, COLS = 0, 1
LATE_CORE, LATE_BY = 0, 11_000


def divisor(whole, unit, most):
    return max(d for d in range(unit, most + 1, unit) if whole % d == 0)


def row_parts(r):
    rest = [(PIECES - 1, 1, 0, r - 8), (PIECES - 1, 1, r - 8, 8)] if r > 8 else [(PIECES - 1, 1, 0, r)]
    return [(0, PIECES - 1, 0, r), *rest]


def cut_rows(ref, part, lead=()):
    return ref.at[(*lead, pl.ds(*part[:2]), pl.ds(*part[2:]))]


def moments(m, v, g):
    m = 0.9 * m + 0.1 * g
    v = 0.95 * v + 0.05 * g * g
    return m, v


def new_weight(w, m, v):
    step = m * lax.rsqrt(v + 1e-8) + 0.1 * w
    return (w - 0.02 * step).astype(BF16)


class Torus:
    def __init__(self, side):
        self.side = side
        self.me = lax.axis_index("dp")
        self.x, self.y = self.me // side, lax.rem(self.me, side)

    def around(self, v):
        return lax.rem(v + 4 * self.side, self.side)

    def ab(self, c):
        return (self.x, self.y) if c < 2 else (self.y, self.x)

    def dev(self, c, a, b):
        return a * self.side + b if c < 2 else b * self.side + a

    def along_a(self, c, k):
        a, b = self.ab(c)
        return self.dev(c, self.around(a + k * sign(c)), b)

    def along_b(self, c, k):
        a, b = self.ab(c)
        return self.dev(c, a, self.around(b + k * sign(c)))

    def back(self, c, back_a, back_b):
        a, b = self.ab(c)
        return self.around(a - back_a * sign(c)), self.around(b - back_b * sign(c))

    def block(self, c, back_a, back_b):
        return self.dev(c, *self.back(c, back_a, back_b))


def sign(c):
    return 1 if c % 2 == 0 else -1


def remote(src, dst, send, recv, device):
    return pltpu.make_async_remote_copy(src, dst, send, recv, device_id={"dp": device}, device_id_type=MESH)


def local(src, dst, sem):
    return pltpu.make_async_copy(src, dst, sem)


def got(ref, sem):
    pltpu.make_async_copy(ref, ref, sem).wait()


def tell(sem, device):
    pl.semaphore_signal(sem, inc=1, device_id={"dp": device}, device_id_type=MESH)


def main_kernel(n, side, count,
                g_gate, g_up, g_down, w_gate, w_up, w_down, m_gate, m_up, m_down, v_gate, v_up, v_down,
                o_gate, o_up, o_down, og_gate, og_up, og_down, factor_ref, *rest):
    parts = row_parts(m_gate.shape[-2])
    stay, low_stay, rest = rest[: len(parts) * 4], rest[len(parts) * 4 : len(parts) * 4 + 4], rest[len(parts) * 4 + 4 :]
    bufr, bufc, ownr, ownc, mr, mc, vr, vc, acc, sq, rs, ss, p2r, p2s, own_sem, mv_sem, cred1, cred2, sq_sem, loc = rest
    layers = g_gate.shape[0]
    wide = bufr.shape[-1]
    tall, quarter = bufc.shape[-2:]
    cstep, rstep = divisor(wide, 128, 384), divisor(tall, 8, 24)
    kinds = PIECES + layers
    t = Torus(side)
    me = t.me

    gates = (g_gate, g_up), (w_gate, w_up), (m_gate, m_up), (v_gate, v_up), (o_gate, o_up), (og_gate, og_up)
    downs = g_down, w_down, m_down, v_down, o_down, og_down
    TERM, WEIGHT, M, V, OUT, SUM = range(6)

    def pick(which, c):
        return gates[which][c // layers], c % layers

    def cols(c):
        return pl.ds(c * quarter, quarter)

    def group(which, c, kind, j):
        if kind == ROWS:
            ref, layer = pick(which, c)
            return ref.at[layer, j]
        return downs[which].at[:, j, :, cols(c)]

    def piece(which, c, i, j):
        if i < PIECES:
            ref, layer = pick(which, c)
            return ref.at[layer, j, i]
        return downs[which].at[i - PIECES, j, :, cols(c)]

    def own_group(which, c, kind):
        if kind == ROWS:
            ref, layer = pick(which, c)
            return ref.at[layer]
        return downs[which].at[:, :, cols(c)]

    def own_piece(which, c, i):
        if i < PIECES:
            ref, layer = pick(which, c)
            return ref.at[layer, i]
        return downs[which].at[i - PIECES, :, cols(c)]

    def buf(kind, *lead):
        return (bufr, bufc)[kind].at[lead]

    def own(kind, *lead):
        return (ownr, ownc)[kind].at[lead]

    def part(ref, kind, i):
        return ref.at[i if kind == ROWS else i - PIECES]

    def kind_of(i):
        return ROWS if i < PIECES else COLS

    def pieces(kind):
        return range(PIECES) if kind == ROWS else range(PIECES, kinds)

    def tiles(kind, body):
        if kind == ROWS:
            @pl.loop(0, wide // cstep)
            def _(k):
                body((slice(None), pl.ds(pl.multiple_of(k * cstep, 128), cstep)))
        else:
            @pl.loop(0, tall // rstep)
            def _(k):
                body((pl.ds(pl.multiple_of(k * rstep, 8), rstep), slice(None)))

    def add(kind, dst, *more):
        def body(at):
            total = dst[at].astype(F32)
            for one in more:
                total += one[at].astype(F32)
            dst[at] = total.astype(BF16)

        tiles(kind, body)

    def six(sem):
        got(bufr.at[0, 0, pl.ds(0, kinds // 3), pl.ds(0, 3)], sem)

    barrier = pltpu.get_barrier_semaphore()
    for c in COLOURS:
        tell(barrier, t.along_a(c, 1))
    pl.semaphore_wait(barrier, len(COLOURS))

    @pl.when(lax.rem(lax.axis_index("rep"), 2) == LATE_CORE)
    def _():
        pl.delay(LATE_BY)

    @pl.loop(0, side)
    def _(q):
        for kind in (ROWS, COLS):
            for c in COLOURS:
                remote(group(TERM, c, kind, t.block(c, 1, q + 1)), buf(kind, 0, c, q), ss.at[0, c, q], rs.at[0, c, q], t.along_a(c, 1)).start()

    def own_load(step, c, kind):
        stage, q = 1 + step // side, lax.rem(step, side)
        par = lax.rem(step, 2)
        return local(group(TERM, c, kind, t.block(c, stage + 1, q + 1)), own(kind, par, c), own_sem.at[par, c])

    def start_own(step):
        for kind in (ROWS, COLS):
            for c in COLOURS:
                own_load(step, c, kind).start()

    def mv_load(c, i):
        kind = kind_of(i)
        if kind == ROWS:
            return [local(own_piece(which, c, i), ref.at[c, i % 2], mv_sem.at[c, i % 2]) for which, ref in ((M, mr), (V, vr))]
        return [local(own_group(which, c, COLS), ref.at[c], mv_sem.at[c, 2]) for which, ref in ((M, mc), (V, vc))]

    def mv_wait(c, i):
        if kind_of(i) == ROWS:
            got(mr.at[c], mv_sem.at[c, i % 2])
        else:
            got(mc.at[pl.ds(0, 2)], mv_sem.at[c, 2])

    start_own(0)
    for i in (0, 1, PIECES):
        for c in COLOURS:
            for copy in mv_load(c, i):
                copy.start()

    @pl.loop(0, 2 * side)
    def _(step):
        par, q = step // side, lax.rem(step, side)
        start_own(step + 1)
        for c in COLOURS:
            six(rs.at[par, c, q])
            six(ss.at[par, c, q])

            @pl.when(par == 1)
            def _():
                tell(cred1.at[c], t.along_a(c, -1))

            six(own_sem.at[lax.rem(step, 2), c])
            for kind in (ROWS, COLS):
                here, mine = buf(kind, par, c, q), own(kind, lax.rem(step, 2), c)
                for i in pieces(kind):
                    add(kind, part(here, kind, i), part(mine, kind, i))
        for c in COLOURS:
            @pl.when(par == 1)
            def _():
                pl.semaphore_wait(cred1.at[c], 1)

            for kind in (ROWS, COLS):
                remote(buf(kind, par, c, q), buf(kind, 1 - par, c, q), ss.at[1 - par, c, q], rs.at[1 - par, c, q], t.along_a(c, 1)).start()

    acc[...] = jnp.zeros_like(acc)
    last_own = (3 * side) % 2
    for q in range(side):
        step = 2 * side + q
        if q < side - 1:
            start_own(step + 1)
        else:
            for kind in (ROWS, COLS):
                for c in COLOURS:
                    local(group(WEIGHT, c, kind, me), own(kind, last_own, c), own_sem.at[last_own, c]).start()
        for i in range(kinds):
            kind = kind_of(i)
            for c in COLOURS:
                whole, mine = buf(kind, 0, c, q), own(kind, step % 2, c)
                here = part(whole, kind, i)
                if i == 0:
                    six(rs.at[0, c, q])
                    six(ss.at[0, c, q])
                    six(own_sem.at[step % 2, c])
                more = [part(mine, kind, i)]
                if q:
                    got(here, p2r.at[c, i])
                    more.append(part(buf(kind, 1, c, q - 1), kind, i))
                if q < side - 1:
                    tell(cred2.at[c], t.along_b(c, -1))
                    add(kind, here, *more)
                    continue

                def last(at, here=here, more=more):
                    total = here[at].astype(F32)
                    for one in more:
                        total += one[at].astype(F32)
                    total = total.astype(BF16)
                    here[at] = total
                    square = total.astype(F32)
                    square = square * square
                    rows, columns = square.shape
                    acc[...] += sum(square[a : a + 8, b : b + 128] for a in range(0, rows, 8) for b in range(0, columns, 128))

                tiles(kind, last)
            if q < side - 1:
                for c in COLOURS:
                    pl.semaphore_wait(cred2.at[c], 1)
                    remote(part(buf(kind, 0, c, q), kind, i), part(buf(kind, 1, c, q), kind, i), p2s.at[c, kind], p2r.at[c, i], t.along_b(c, 1)).start()

    sq[me] = jnp.sum(acc[...], axis=0, keepdims=True)
    for k in range(1, n):
        remote(sq.at[me], sq.at[me], sq_sem.at[0], sq_sem.at[1], lax.rem(me + k, n)).start()
    for c in COLOURS:
        for kind in (ROWS, COLS):
            got((bufr, bufc)[kind].at[0, c, pl.ds(0, side - 1)], p2s.at[c, kind])
    got(sq.at[pl.ds(0, n - 1)], sq_sem.at[1])
    total = sum(sq[k] for k in range(n))
    total = jnp.sum(total, axis=(0, 1), keepdims=True)
    factor = jnp.minimum(1.0, 0.5 * lax.rsqrt(total / count + 1e-30))
    factor_ref[...] = jnp.broadcast_to(factor, factor_ref.shape)

    def arrived_b(c, hop):
        return p2r.at[c, hop - 1]

    def arrived_a(c, hop, q):
        return rs.at[hop - 1, c, q]

    def sent(c, kind):
        return p2s.at[c, kind]

    for i in range(kinds):
        kind = kind_of(i)
        for c in COLOURS:
            if i == 0:
                six(own_sem.at[last_own, c])
            if i <= PIECES:
                mv_wait(c, i)
            w_ref, g_ref = (part(ref, kind, i) for ref in (own(kind, last_own, c), buf(kind, 0, c, side - 1)))
            m_ref, v_ref = (rows.at[c, i % 2] if kind == ROWS else columns.at[c, i - PIECES] for rows, columns in ((mr, mc), (vr, vc)))

            def body(at, w_ref=w_ref, g_ref=g_ref, m_ref=m_ref, v_ref=v_ref):
                g = g_ref[at].astype(F32) * factor
                m, v = moments(m_ref[at], v_ref[at], g)
                w_ref[at] = new_weight(w_ref[at].astype(F32), m, v)

            tiles(kind, body)
            if i + 2 < PIECES:
                for copy in mv_load(c, i + 2):
                    copy.start()
        for c in COLOURS:
            remote(part(own(kind, last_own, c), kind, i), piece(OUT, c, i, me), sent(c, kind), arrived_b(c, 1), t.along_b(c, 1)).start()
    for kind in (ROWS, COLS):
        for c in COLOURS:
            mine, there = own(kind, last_own, c), group(OUT, c, kind, me)
            remote(mine, there, sent(c, kind), arrived_a(c, 1, 0), t.along_a(c, 1)).start()
            local(mine, there, loc.at[0, kind]).start()
            local(buf(kind, 0, c, side - 1), own_group(SUM, c, kind), loc.at[1, kind]).start()

    for hop in range(1, side):
        for c in COLOURS:
            six(arrived_b(c, hop))
            for kind in (ROWS, COLS):
                here = group(OUT, c, kind, t.block(c, 0, hop))
                if hop < side - 1:
                    remote(here, here, sent(c, kind), arrived_b(c, hop + 1), t.along_b(c, 1)).start()
                remote(here, here, sent(c, kind), arrived_a(c, 1, hop), t.along_a(c, 1)).start()

    for hop in range(1, side - 2):
        for q in range(side):
            for c in COLOURS:
                six(arrived_a(c, hop, q))
                a, b = t.back(c, hop, q)
                next_hop = functools.partial(remote, recv=arrived_a(c, hop + 1, q), device=t.along_a(c, 1))
                rows, columns = (group(OUT, c, kind, t.dev(c, a, b)) for kind in (ROWS, COLS))
                if hop < side - 3:
                    next_hop(rows, rows, send=sent(c, ROWS)).start()
                    next_hop(columns, columns, send=sent(c, COLS)).start()
                    continue
                for k, one in enumerate(parts):
                    next_hop(cut_rows(rows, one), stay[c * len(parts) + k].at[b], send=sent(c, ROWS)).start()
                next_hop(columns, low_stay[c].at[:, b], send=sent(c, COLS)).start()
    for q in range(side):
        for c in COLOURS:
            six(arrived_a(c, side - 2, q))

    got(sq.at[pl.ds(0, n - 1)], sq_sem.at[0])
    for kind in (ROWS, COLS):
        for k in range(2):
            got((ownr, ownc)[kind].at[last_own], loc.at[k, kind])
    for c in COLOURS:
        ref, layer = pick(OUT, c)
        got(ref.at[layer, pl.ds(0, n - 1 - side)], sent(c, ROWS))
        got(o_down.at[:, pl.ds(0, n - 1 - side), :, cols(c)], sent(c, COLS))


def copy_kernel(side, t_gate, t_up, t_down, g_gate, g_up, g_down, factor_ref, m_gate, m_up, m_down, v_gate, v_up, v_down, *rest):
    parts = row_parts(m_gate.shape[-2])
    stay, low_stay, rest = rest[: 4 * len(parts)], rest[4 * len(parts) : 4 * len(parts) + 4], rest[4 * len(parts) + 4 :]
    o_gate, o_up, o_down, nm_gate, nm_up, nm_down, nv_gate, nv_up, nv_down, rowbuf, colbuf, gr, gc, mr, mc, vr, vc, load_sem, store_sem = rest
    layers = o_down.shape[0]
    wide = gr.shape[-1]
    tall = gc.shape[-2]
    quarter = colbuf.shape[-1]
    t = Torus(side)
    factor = factor_ref[0:1, 0:1]

    def at_a(ref, layer, c, a):
        return ref.at[layer, a] if c < 2 else ref.at[layer, :, a]

    def low_at_a(ref, c, a):
        columns = pl.ds(c * quarter, quarter)
        return ref.at[:, a, :, :, columns] if c < 2 else ref.at[:, :, a, :, columns]

    jobs = []
    slots = {"rows": (rowbuf, 0), "cols": (colbuf, 1)}
    made = {"rows": 0, "cols": 0, "mr": 0, "mc": 0}
    depth = {"rows": rowbuf.shape[0], "cols": colbuf.shape[0], "mr": gr.shape[0], "mc": gc.shape[0]}
    base = {"rows": 0, "cols": depth["rows"], "mr": depth["rows"] + depth["cols"], "mc": depth["rows"] + depth["cols"] + depth["mr"]}

    def job(what, loads, stores, work=None):
        slot = made[what] % depth[what]
        made[what] += 1
        jobs.append((what, slot, [f(slot) for f in loads], [f(slot) for f in stores], work and functools.partial(work, slot)))

    def copy_job(what, src, dst):
        ref = slots[what][0]
        job(what, [lambda slot: (src, ref.at[slot])], [lambda slot: (ref.at[slot], dst)])

    def step(gs, ms, vs, parts, where, slot):
        @pl.loop(0, parts)
        def _(k):
            at = (slot, *where(k))
            g = gs[at].astype(F32) * factor
            ms[at], vs[at] = moments(ms[at], vs[at], g)

    def moment_job(what, g, m, v, nm, nv):
        gs, ms, vs = (gr, mr, vr) if what == "mr" else (gc, mc, vc)
        if what == "mr":
            size = divisor(wide, 128, 384)
            parts = gs.shape[1] * (wide // size)
            each = wide // size
            where = lambda k: (k // each, slice(None), pl.ds(pl.multiple_of(lax.rem(k, each) * size, 128), size))
        else:
            size = divisor(tall, 8, 24)
            parts = tall // size
            where = lambda k: (pl.ds(pl.multiple_of(k * size, 8), size), slice(None))
        job(
            what,
            [lambda slot: (g, gs.at[slot]), lambda slot: (m, ms.at[slot]), lambda slot: (v, vs.at[slot])],
            [lambda slot: (ms.at[slot], nm), lambda slot: (vs.at[slot], nv)],
            functools.partial(step, gs, ms, vs, parts, where),
        )

    big = ((t_gate, o_gate), (t_up, o_up))
    small = ((g_gate, m_gate, v_gate, nm_gate, nv_gate), (g_up, m_up, v_up, nm_up, nv_up), (g_down, m_down, v_down, nm_down, nv_down))
    for c in COLOURS:
        layer = c % layers
        src, dst = big[c // layers]
        for back in range(side - 2):
            a, _ = t.back(c, back, 0)
            copy_job("rows", at_a(src, layer, c, a), at_a(dst, layer, c, a))
        moment_job("mr", *(one.at[layer] for one in small[c // layers]))
        a, _ = t.back(c, side - 2, 0)
        ref = rowbuf
        job(
            "rows",
            [lambda slot, src=stay[c * len(parts) + k], one=one: (src, cut_rows(ref, one, (slot, slice(None)))) for k, one in enumerate(parts)],
            [lambda slot, layer=layer, c=c, a=a, dst=dst: (ref.at[slot], at_a(dst, layer, c, a))],
        )
        for back in range(side - 2):
            a, _ = t.back(c, back, 0)
            copy_job("cols", low_at_a(t_down, c, a), low_at_a(o_down, c, a))
        a, _ = t.back(c, side - 2, 0)
        copy_job("cols", low_stay[c], low_at_a(o_down, c, a))
        if c // layers == 1:
            moment_job("mc", *(one.at[layer] for one in small[2]))

    def copies(k, which):
        what, slot = jobs[k][:2]
        sem = (load_sem, store_sem)[which]
        return [local(src, dst, sem.at[base[what] + slot, z]) for z, (src, dst) in enumerate(jobs[k][2 + which])]

    ahead, stored = 4, [False] * len(jobs)

    def start_loads(k):
        for one in range(k):
            if jobs[one][:2] == jobs[k][:2] and not stored[one]:
                for copy in copies(one, 1):
                    copy.wait()
                stored[one] = True
        for copy in copies(k, 0):
            copy.start()

    for k in range(ahead):
        start_loads(k)
    for k, (*_, work) in enumerate(jobs):
        for copy in copies(k, 0):
            copy.wait()
        if work is not None:
            work()
        for copy in copies(k, 1):
            copy.start()
        if k + ahead < len(jobs):
            start_loads(k + ahead)
    for k in range(len(jobs)):
        if not stored[k]:
            for copy in copies(k, 1):
                copy.wait()


def place_kernel(side, part, *refs):
    *ins, sem = refs
    wholes = 2 + (part[0] == 0)
    ins, outs = ins[wholes:-wholes], ins[-wholes:]
    t = Torus(side)
    layers = outs[0].shape[0]
    moves = []
    for c in COLOURS:
        a, _ = t.back(c, side - 1, 0)
        dst = outs[c // layers]
        dst = dst.at[c % layers, a] if c < 2 else dst.at[c % layers, :, a]
        moves.append(local(ins[c], cut_rows(dst, part, (slice(None),)), sem.at[c]))
        if wholes > 2:
            columns = pl.ds(c * ins[4].shape[-1], ins[4].shape[-1])
            dst = outs[2].at[:, a, :, :, columns] if c < 2 else outs[2].at[:, :, a, :, columns]
            moves.append(local(ins[4 + c], dst, sem.at[4 + c]))
    for move in moves:
        move.start()
    for move in moves:
        move.wait()


def solution(mesh):
    n = mesh.shape["dp"]
    side = math.isqrt(n)
    dma = pltpu.SemaphoreType.DMA
    anywhere, in_vmem = pl.BlockSpec(memory_space=pl.ANY), pl.BlockSpec(memory_space=pltpu.VMEM)

    def shape(*dims, dtype=BF16):
        return jax.ShapeDtypeStruct(dims, dtype)

    def in_hbm(*some):
        return [pltpu.with_memory_space_constraint(one, pltpu.HBM) for one in some]

    def permutation(c):
        moved = []
        for i in range(n):
            a, b = (i // side, i % side) if c < 2 else (i % side, i // side)
            a = (a + sign(c)) % side
            moved.append((i, a * side + b if c < 2 else b * side + a))
        return moved

    def step(*arrays):
        terms, weights, m, v = (arrays[i : i + 3] for i in (0, 3, 6, 9))
        layers, rows, wide = m[0].shape
        tall, narrow = m[2].shape[1:]
        assert side == 4 and side * side == n and layers * 2 == len(COLOURS), (n, layers)
        r, quarter = rows // PIECES, narrow // len(COLOURS)
        kinds = PIECES + layers
        block, low_block = (PIECES, r, wide), (tall, narrow)

        def cut(whole, *lead):
            return [one.reshape(layers, *lead, *dims) for one, dims in zip(whole, (block, block, low_block), strict=True)]

        m, v = cut(m), cut(v)
        assert r * wide == tall * quarter and kinds == 6
        parts = row_parts(r)
        stays = [shape(side, one[1], one[3], wide) for _ in COLOURS for one in parts] + [shape(layers, side, tall, quarter)] * 4
        out = pl.pallas_call(
            functools.partial(main_kernel, n, side, float(n * sum(one.size for one in m))),
            name="sum_step_gather",
            out_shape=(
                *(shape(layers, n, *block),) * 2, shape(layers, n, *low_block),
                *(shape(layers, *block),) * 2, shape(layers, *low_block),
                shape(8, 128, dtype=F32), *stays,
            ),
            in_specs=[anywhere] * 12,
            out_specs=[anywhere] * 6 + [in_vmem] + [anywhere] * len(stays),
            scratch_shapes=[
                pltpu.VMEM((2, 4, side, *block), BF16),
                pltpu.VMEM((2, 4, side, layers, tall, quarter), BF16),
                pltpu.VMEM((2, 4, *block), BF16),
                pltpu.VMEM((2, 4, layers, tall, quarter), BF16),
                pltpu.VMEM((4, 2, r, wide), F32),
                pltpu.VMEM((4, layers, tall, quarter), F32),
                pltpu.VMEM((4, 2, r, wide), F32),
                pltpu.VMEM((4, layers, tall, quarter), F32),
                pltpu.VMEM((8, 128), F32),
                pltpu.VMEM((n, 1, 128), F32),
                dma((2, 4, side)),
                dma((2, 4, side)),
                dma((4, kinds)),
                dma((4, 2)),
                dma((2, 4)),
                dma((4, 3)),
                pltpu.SemaphoreType.REGULAR((4,)),
                pltpu.SemaphoreType.REGULAR((4,)),
                dma((2,)),
                dma((2, 2)),
            ],
            compiler_params=pltpu.CompilerParams(collective_id=0, has_side_effects=True, vmem_limit_bytes=66_000_000),
        )(*cut([one[0] for one in terms], n), *cut(weights, n), *m, *v)
        gathered, g, factor, stay = out[:3], out[3:6], out[6], out[7:]

        moved = {}
        for k in (0, len(parts), *range(1, len(parts))):
            for c in COLOURS:
                moved[c, k] = lax.ppermute(stay[c * len(parts) + k] if k < len(parts) else stay[4 * k + c], "dp", permutation(c))

        square = (layers, side, side)
        copied = pl.pallas_call(
            functools.partial(copy_kernel, side),
            name="copy_and_moments",
            out_shape=(
                *(shape(*square, *block),) * 2, shape(*square, *low_block),
                *((shape(layers, *block, dtype=F32),) * 2 + (shape(layers, *low_block, dtype=F32),)) * 2,
            ),
            in_specs=[anywhere] * 6 + [in_vmem] + [anywhere] * (6 + len(stay)),
            out_specs=[anywhere] * 9,
            scratch_shapes=[
                pltpu.VMEM((3, side, *block), BF16),
                pltpu.VMEM((4, layers, side, tall, quarter), BF16),
                pltpu.VMEM((1, *block), BF16),
                pltpu.VMEM((1, *low_block), BF16),
                pltpu.VMEM((1, *block), F32),
                pltpu.VMEM((1, *low_block), F32),
                pltpu.VMEM((1, *block), F32),
                pltpu.VMEM((1, *low_block), F32),
                dma((9, 3)),
                dma((9, 2)),
            ],
            cost_estimate=pl.CostEstimate(flops=10**9, bytes_accessed=200_000_000, transcendentals=0),
            compiler_params=pltpu.CompilerParams(vmem_limit_bytes=32_000_000),
        )(*in_hbm(*(one.reshape(*square, *one.shape[2:]) for one in gathered), *g), factor, *in_hbm(*m, *v, *stay))
        new_w, new_m, new_v = list(copied[:3]), copied[3:6], copied[6:]

        for k, one in enumerate(parts):
            wholes = 3 if k == 0 else 2
            arrived = [moved[c, k] for c in COLOURS] + [moved[c, len(parts)] for c in COLOURS if k == 0]
            new_w[:wholes] = pl.pallas_call(
                functools.partial(place_kernel, side, one),
                name=f"place_{k}",
                out_shape=[shape(*old.shape) for old in new_w[:wholes]],
                in_specs=[anywhere] * wholes + [in_vmem] * len(arrived),
                out_specs=[anywhere] * wholes,
                scratch_shapes=[dma((8,))],
                input_output_aliases={i: i for i in range(wholes)},
                compiler_params=pltpu.CompilerParams(vmem_limit_bytes=24_000_000),
            )(*new_w[:wholes], *arrived)
        return tuple(one.reshape(old.shape) for one, old in zip((*new_w, *new_m, *new_v), (*weights, *arrays[6:]), strict=True))

    all_of, part = P(None, None, None), P(None, "dp", None)
    return jax.shard_map(
        step,
        mesh=mesh,
        in_specs=(P(("rep", "dp"), None, None, None),) * 3 + (all_of,) * 3 + (part,) * 6,
        out_specs=(P("rep", None, None),) * 3 + (P("rep", "dp", None),) * 6,
        check_vma=False,
    )
```

```python
import functools
import math

import jax
import jax.numpy as jnp
from jax import lax
from jax.experimental import pallas as pl
from jax.experimental.pallas import tpu as pltpu
from jax.sharding import PartitionSpec as P

MESH = pl.DeviceIdType.MESH
F32, BF16 = jnp.float32, jnp.bfloat16
COLOURS = range(4)
PIECES = 4
ROWS, COLS = 0, 1
LATE_CORE, LATE_BY = 0, 16_000


def divisor(whole, unit, most):
    return max(d for d in range(unit, most + 1, unit) if whole % d == 0)


def row_parts(r):
    rest = [(PIECES - 1, 1, 0, r - 8), (PIECES - 1, 1, r - 8, 8)] if r > 8 else [(PIECES - 1, 1, 0, r)]
    return [(0, PIECES - 1, 0, r), *rest]


def cut_rows(ref, part, lead=()):
    return ref.at[(*lead, pl.ds(*part[:2]), pl.ds(*part[2:]))]


def moments(m, v, g):
    m = 0.9 * m + 0.1 * g
    v = 0.95 * v + 0.05 * g * g
    return m, v


def new_weight(w, m, v):
    step = m * lax.rsqrt(v + 1e-8) + 0.1 * w
    return (w - 0.02 * step).astype(BF16)


class Torus:
    def __init__(self, side):
        self.side = side
        self.me = lax.axis_index("dp")
        self.x, self.y = self.me // side, lax.rem(self.me, side)

    def around(self, v):
        return lax.rem(v + 4 * self.side, self.side)

    def ab(self, c):
        return (self.x, self.y) if c < 2 else (self.y, self.x)

    def dev(self, c, a, b):
        return a * self.side + b if c < 2 else b * self.side + a

    def along_a(self, c, k):
        a, b = self.ab(c)
        return self.dev(c, self.around(a + k * sign(c)), b)

    def along_b(self, c, k):
        a, b = self.ab(c)
        return self.dev(c, a, self.around(b + k * sign(c)))

    def back(self, c, back_a, back_b):
        a, b = self.ab(c)
        return self.around(a - back_a * sign(c)), self.around(b - back_b * sign(c))

    def block(self, c, back_a, back_b):
        return self.dev(c, *self.back(c, back_a, back_b))


def sign(c):
    return 1 if c % 2 == 0 else -1


def remote(src, dst, send, recv, device):
    return pltpu.make_async_remote_copy(src, dst, send, recv, device_id={"dp": device}, device_id_type=MESH)


def local(src, dst, sem):
    return pltpu.make_async_copy(src, dst, sem)


def got(ref, sem):
    pltpu.make_async_copy(ref, ref, sem).wait()


def tell(sem, device):
    pl.semaphore_signal(sem, inc=1, device_id={"dp": device}, device_id_type=MESH)


def main_kernel(n, side, count,
                g_gate, g_up, g_down, w_gate, w_up, w_down, m_gate, m_up, m_down, v_gate, v_up, v_down,
                o_gate, o_up, o_down, og_gate, og_up, og_down, factor_ref, *rest):
    parts = row_parts(m_gate.shape[-2])
    stay, low_stay, rest = rest[: len(parts) * 4], rest[len(parts) * 4 : len(parts) * 4 + 4], rest[len(parts) * 4 + 4 :]
    bufr, bufc, ownr, ownc, mr, mc, vr, vc, acc, sq, rs, ss, p2r, p2s, own_sem, mv_sem, cred1, cred2, behind, sq_sem, loc = rest
    layers = g_gate.shape[0]
    wide = bufr.shape[-1]
    tall, quarter = bufc.shape[-2:]
    cstep, rstep = divisor(wide, 128, 384), divisor(tall, 8, 24)
    kinds = PIECES + layers
    t = Torus(side)
    me = t.me

    gates = (g_gate, g_up), (w_gate, w_up), (m_gate, m_up), (v_gate, v_up), (o_gate, o_up), (og_gate, og_up)
    downs = g_down, w_down, m_down, v_down, o_down, og_down
    TERM, WEIGHT, M, V, OUT, SUM = range(6)

    def pick(which, c):
        return gates[which][c // layers], c % layers

    def cols(c):
        return pl.ds(c * quarter, quarter)

    def group(which, c, kind, j):
        if kind == ROWS:
            ref, layer = pick(which, c)
            return ref.at[layer, j]
        return downs[which].at[:, j, :, cols(c)]

    def piece(which, c, i, j):
        if i < PIECES:
            ref, layer = pick(which, c)
            return ref.at[layer, j, i]
        return downs[which].at[i - PIECES, j, :, cols(c)]

    def own_group(which, c, kind):
        if kind == ROWS:
            ref, layer = pick(which, c)
            return ref.at[layer]
        return downs[which].at[:, :, cols(c)]

    def own_piece(which, c, i):
        if i < PIECES:
            ref, layer = pick(which, c)
            return ref.at[layer, i]
        return downs[which].at[i - PIECES, :, cols(c)]

    def buf(kind, *lead):
        return (bufr, bufc)[kind].at[lead]

    def own(kind, *lead):
        return (ownr, ownc)[kind].at[lead]

    def part(ref, kind, i):
        return ref.at[i if kind == ROWS else i - PIECES]

    def kind_of(i):
        return ROWS if i < PIECES else COLS

    def pieces(kind):
        return range(PIECES) if kind == ROWS else range(PIECES, kinds)

    def tiles(kind, body):
        if kind == ROWS:
            @pl.loop(0, wide // cstep)
            def _(k):
                body((slice(None), pl.ds(pl.multiple_of(k * cstep, 128), cstep)))
        else:
            @pl.loop(0, tall // rstep)
            def _(k):
                body((pl.ds(pl.multiple_of(k * rstep, 8), rstep), slice(None)))

    def add(kind, dst, *more):
        def body(at):
            total = dst[at].astype(F32)
            for one in more:
                total += one[at].astype(F32)
            dst[at] = total.astype(BF16)

        tiles(kind, body)

    def six(sem):
        got(bufr.at[0, 0, pl.ds(0, kinds // 3), pl.ds(0, 3)], sem)

    barrier = pltpu.get_barrier_semaphore()
    for c in (0, 2):
        tell(barrier, t.along_a(c, -1))
    pl.semaphore_wait(barrier, 2)
    for c in (0, 2):
        tell(behind.at[c // 2], t.along_a(c, 1))

    def first_hop(q, c):
        for kind in (ROWS, COLS):
            remote(group(TERM, c, kind, t.block(c, 1, q + 1)), buf(kind, 0, c, q), ss.at[0, c, q], rs.at[0, c, q], t.along_a(c, 1)).start()

    @pl.when(lax.rem(lax.axis_index("rep"), 2) == LATE_CORE)
    def _():
        pl.delay(LATE_BY)

    for c in (0, 2):
        first_hop(0, c)
    for now, order in ((t.y == 0, (1, 3)), (t.y != 0, (3, 1))):
        @pl.when(now)
        def _():
            for c in order:
                pl.semaphore_wait(behind.at[c // 2], 1)
                first_hop(0, c)

    @pl.loop(1, side)
    def _(q):
        for c in COLOURS:
            first_hop(q, c)

    def own_load(step, c, kind):
        stage, q = 1 + step // side, lax.rem(step, side)
        par = lax.rem(step, 2)
        return local(group(TERM, c, kind, t.block(c, stage + 1, q + 1)), own(kind, par, c), own_sem.at[par, c])

    def start_own(step):
        for kind in (ROWS, COLS):
            for c in COLOURS:
                own_load(step, c, kind).start()

    def mv_load(c, i):
        kind = kind_of(i)
        if kind == ROWS:
            return [local(own_piece(which, c, i), ref.at[c, i % 2], mv_sem.at[c, i % 2]) for which, ref in ((M, mr), (V, vr))]
        return [local(own_group(which, c, COLS), ref.at[c], mv_sem.at[c, 2]) for which, ref in ((M, mc), (V, vc))]

    def mv_wait(c, i):
        if kind_of(i) == ROWS:
            got(mr.at[c], mv_sem.at[c, i % 2])
        else:
            got(mc.at[pl.ds(0, 2)], mv_sem.at[c, 2])

    start_own(0)
    for i in (0, 1, PIECES):
        for c in COLOURS:
            for copy in mv_load(c, i):
                copy.start()

    @pl.loop(0, 2 * side)
    def _(step):
        par, q = step // side, lax.rem(step, side)
        start_own(step + 1)
        for c in COLOURS:
            six(rs.at[par, c, q])
            six(ss.at[par, c, q])

            @pl.when(par == 1)
            def _():
                tell(cred1.at[c], t.along_a(c, -1))

            six(own_sem.at[lax.rem(step, 2), c])
            for kind in (ROWS, COLS):
                here, mine = buf(kind, par, c, q), own(kind, lax.rem(step, 2), c)
                for i in pieces(kind):
                    add(kind, part(here, kind, i), part(mine, kind, i))
        for c in COLOURS:
            @pl.when(par == 1)
            def _():
                pl.semaphore_wait(cred1.at[c], 1)

            for kind in (ROWS, COLS):
                remote(buf(kind, par, c, q), buf(kind, 1 - par, c, q), ss.at[1 - par, c, q], rs.at[1 - par, c, q], t.along_a(c, 1)).start()

    acc[...] = jnp.zeros_like(acc)
    last_own = (3 * side) % 2
    for q in range(side):
        step = 2 * side + q
        if q < side - 1:
            start_own(step + 1)
        else:
            for kind in (ROWS, COLS):
                for c in COLOURS:
                    local(group(WEIGHT, c, kind, me), own(kind, last_own, c), own_sem.at[last_own, c]).start()
        for i in range(kinds):
            kind = kind_of(i)
            for c in COLOURS:
                whole, mine = buf(kind, 0, c, q), own(kind, step % 2, c)
                here = part(whole, kind, i)
                if i == 0:
                    six(rs.at[0, c, q])
                    six(ss.at[0, c, q])
                    six(own_sem.at[step % 2, c])
                more = [part(mine, kind, i)]
                if q:
                    got(here, p2r.at[c, i])
                    more.append(part(buf(kind, 1, c, q - 1), kind, i))
                if q < side - 1:
                    tell(cred2.at[c], t.along_b(c, -1))
                    add(kind, here, *more)
                    continue

                def last(at, here=here, more=more):
                    total = here[at].astype(F32)
                    for one in more:
                        total += one[at].astype(F32)
                    total = total.astype(BF16)
                    here[at] = total
                    square = total.astype(F32)
                    square = square * square
                    rows, columns = square.shape
                    acc[...] += sum(square[a : a + 8, b : b + 128] for a in range(0, rows, 8) for b in range(0, columns, 128))

                tiles(kind, last)
            if q < side - 1:
                for c in COLOURS:
                    pl.semaphore_wait(cred2.at[c], 1)
                    remote(part(buf(kind, 0, c, q), kind, i), part(buf(kind, 1, c, q), kind, i), p2s.at[c, kind], p2r.at[c, i], t.along_b(c, 1)).start()

    sq[me] = jnp.sum(acc[...], axis=0, keepdims=True)
    for k in range(1, n):
        remote(sq.at[me], sq.at[me], sq_sem.at[0], sq_sem.at[1], lax.rem(me + k, n)).start()
    for c in COLOURS:
        for kind in (ROWS, COLS):
            got((bufr, bufc)[kind].at[0, c, pl.ds(0, side - 1)], p2s.at[c, kind])
    got(sq.at[pl.ds(0, n - 1)], sq_sem.at[1])
    total = sum(sq[k] for k in range(n))
    total = jnp.sum(total, axis=(0, 1), keepdims=True)
    factor = jnp.minimum(1.0, 0.5 * lax.rsqrt(total / count + 1e-30))
    factor_ref[...] = jnp.broadcast_to(factor, factor_ref.shape)

    def arrived_b(c, hop):
        return p2r.at[c, hop - 1]

    def arrived_a(c, hop, q):
        return rs.at[hop - 1, c, q]

    def sent(c, kind):
        return p2s.at[c, kind]

    for i in range(kinds):
        kind = kind_of(i)
        for c in COLOURS:
            if i == 0:
                six(own_sem.at[last_own, c])
            if i <= PIECES:
                mv_wait(c, i)
            w_ref, g_ref = (part(ref, kind, i) for ref in (own(kind, last_own, c), buf(kind, 0, c, side - 1)))
            m_ref, v_ref = (rows.at[c, i % 2] if kind == ROWS else columns.at[c, i - PIECES] for rows, columns in ((mr, mc), (vr, vc)))

            def body(at, w_ref=w_ref, g_ref=g_ref, m_ref=m_ref, v_ref=v_ref):
                g = g_ref[at].astype(F32) * factor
                m, v = moments(m_ref[at], v_ref[at], g)
                w_ref[at] = new_weight(w_ref[at].astype(F32), m, v)

            tiles(kind, body)
            if i + 2 < PIECES:
                for copy in mv_load(c, i + 2):
                    copy.start()
        for c in COLOURS:
            remote(part(own(kind, last_own, c), kind, i), piece(OUT, c, i, me), sent(c, kind), arrived_b(c, 1), t.along_b(c, 1)).start()
    for kind in (ROWS, COLS):
        for c in COLOURS:
            mine, there = own(kind, last_own, c), group(OUT, c, kind, me)
            remote(mine, there, sent(c, kind), arrived_a(c, 1, 0), t.along_a(c, 1)).start()
            local(mine, there, loc.at[0, kind]).start()
            local(buf(kind, 0, c, side - 1), own_group(SUM, c, kind), loc.at[1, kind]).start()

    for hop in range(1, side):
        for c in COLOURS:
            six(arrived_b(c, hop))
            for kind in (ROWS, COLS):
                here = group(OUT, c, kind, t.block(c, 0, hop))
                if hop < side - 1:
                    remote(here, here, sent(c, kind), arrived_b(c, hop + 1), t.along_b(c, 1)).start()
                remote(here, here, sent(c, kind), arrived_a(c, 1, hop), t.along_a(c, 1)).start()

    for hop in range(1, side - 2):
        for q in range(side):
            for c in COLOURS:
                six(arrived_a(c, hop, q))
                a, b = t.back(c, hop, q)
                next_hop = functools.partial(remote, recv=arrived_a(c, hop + 1, q), device=t.along_a(c, 1))
                rows, columns = (group(OUT, c, kind, t.dev(c, a, b)) for kind in (ROWS, COLS))
                if hop < side - 3:
                    next_hop(rows, rows, send=sent(c, ROWS)).start()
                    next_hop(columns, columns, send=sent(c, COLS)).start()
                    continue
                for k, one in enumerate(parts):
                    next_hop(cut_rows(rows, one), stay[c * len(parts) + k].at[b], send=sent(c, ROWS)).start()
                next_hop(columns, low_stay[c].at[:, b], send=sent(c, COLS)).start()
    for q in range(side):
        for c in COLOURS:
            six(arrived_a(c, side - 2, q))

    got(sq.at[pl.ds(0, n - 1)], sq_sem.at[0])
    for kind in (ROWS, COLS):
        for k in range(2):
            got((ownr, ownc)[kind].at[last_own], loc.at[k, kind])
    for c in COLOURS:
        ref, layer = pick(OUT, c)
        got(ref.at[layer, pl.ds(0, n - 1 - side)], sent(c, ROWS))
        got(o_down.at[:, pl.ds(0, n - 1 - side), :, cols(c)], sent(c, COLS))


def copy_kernel(side, t_gate, t_up, t_down, g_gate, g_up, g_down, factor_ref, m_gate, m_up, m_down, v_gate, v_up, v_down, *rest):
    parts = row_parts(m_gate.shape[-2])
    stay, low_stay, rest = rest[: 4 * len(parts)], rest[4 * len(parts) : 4 * len(parts) + 4], rest[4 * len(parts) + 4 :]
    o_gate, o_up, o_down, nm_gate, nm_up, nm_down, nv_gate, nv_up, nv_down, rowbuf, colbuf, gr, gc, mr, mc, vr, vc, load_sem, store_sem = rest
    layers = o_down.shape[0]
    wide = gr.shape[-1]
    tall = gc.shape[-2]
    quarter = colbuf.shape[-1]
    t = Torus(side)
    factor = factor_ref[0:1, 0:1]

    def at_a(ref, layer, c, a):
        return ref.at[layer, a] if c < 2 else ref.at[layer, :, a]

    def low_at_a(ref, c, a):
        columns = pl.ds(c * quarter, quarter)
        return ref.at[:, a, :, :, columns] if c < 2 else ref.at[:, :, a, :, columns]

    jobs = []
    slots = {"rows": (rowbuf, 0), "cols": (colbuf, 1)}
    made = {"rows": 0, "cols": 0, "mr": 0, "mc": 0}
    depth = {"rows": rowbuf.shape[0], "cols": colbuf.shape[0], "mr": gr.shape[0], "mc": gc.shape[0]}
    base = {"rows": 0, "cols": depth["rows"], "mr": depth["rows"] + depth["cols"], "mc": depth["rows"] + depth["cols"] + depth["mr"]}

    def job(what, loads, stores, work=None):
        slot = made[what] % depth[what]
        made[what] += 1
        jobs.append((what, slot, [f(slot) for f in loads], [f(slot) for f in stores], work and functools.partial(work, slot)))

    def copy_job(what, src, dst):
        ref = slots[what][0]
        job(what, [lambda slot: (src, ref.at[slot])], [lambda slot: (ref.at[slot], dst)])

    def step(gs, ms, vs, parts, where, slot):
        @pl.loop(0, parts)
        def _(k):
            at = (slot, *where(k))
            g = gs[at].astype(F32) * factor
            ms[at], vs[at] = moments(ms[at], vs[at], g)

    def moment_job(what, g, m, v, nm, nv):
        gs, ms, vs = (gr, mr, vr) if what == "mr" else (gc, mc, vc)
        if what == "mr":
            size = divisor(wide, 128, 384)
            parts = gs.shape[1] * (wide // size)
            each = wide // size
            where = lambda k: (k // each, slice(None), pl.ds(pl.multiple_of(lax.rem(k, each) * size, 128), size))
        else:
            size = divisor(tall, 8, 24)
            parts = tall // size
            where = lambda k: (pl.ds(pl.multiple_of(k * size, 8), size), slice(None))
        job(
            what,
            [lambda slot: (g, gs.at[slot]), lambda slot: (m, ms.at[slot]), lambda slot: (v, vs.at[slot])],
            [lambda slot: (ms.at[slot], nm), lambda slot: (vs.at[slot], nv)],
            functools.partial(step, gs, ms, vs, parts, where),
        )

    big = ((t_gate, o_gate), (t_up, o_up))
    small = ((g_gate, m_gate, v_gate, nm_gate, nv_gate), (g_up, m_up, v_up, nm_up, nv_up), (g_down, m_down, v_down, nm_down, nv_down))
    for c in COLOURS:
        layer = c % layers
        src, dst = big[c // layers]
        for back in range(side - 2):
            a, _ = t.back(c, back, 0)
            copy_job("rows", at_a(src, layer, c, a), at_a(dst, layer, c, a))
        moment_job("mr", *(one.at[layer] for one in small[c // layers]))
        a, _ = t.back(c, side - 2, 0)
        ref = rowbuf
        job(
            "rows",
            [lambda slot, src=stay[c * len(parts) + k], one=one: (src, cut_rows(ref, one, (slot, slice(None)))) for k, one in enumerate(parts)],
            [lambda slot, layer=layer, c=c, a=a, dst=dst: (ref.at[slot], at_a(dst, layer, c, a))],
        )
        for back in range(side - 2):
            a, _ = t.back(c, back, 0)
            copy_job("cols", low_at_a(t_down, c, a), low_at_a(o_down, c, a))
        a, _ = t.back(c, side - 2, 0)
        copy_job("cols", low_stay[c], low_at_a(o_down, c, a))
        if c // layers == 1:
            moment_job("mc", *(one.at[layer] for one in small[2]))

    def copies(k, which):
        what, slot = jobs[k][:2]
        sem = (load_sem, store_sem)[which]
        return [local(src, dst, sem.at[base[what] + slot, z]) for z, (src, dst) in enumerate(jobs[k][2 + which])]

    ahead, stored = 4, [False] * len(jobs)

    def start_loads(k):
        for one in range(k):
            if jobs[one][:2] == jobs[k][:2] and not stored[one]:
                for copy in copies(one, 1):
                    copy.wait()
                stored[one] = True
        for copy in copies(k, 0):
            copy.start()

    for k in range(ahead):
        start_loads(k)
    for k, (*_, work) in enumerate(jobs):
        for copy in copies(k, 0):
            copy.wait()
        if work is not None:
            work()
        for copy in copies(k, 1):
            copy.start()
        if k + ahead < len(jobs):
            start_loads(k + ahead)
    for k in range(len(jobs)):
        if not stored[k]:
            for copy in copies(k, 1):
                copy.wait()


def place_kernel(side, part, *refs):
    *ins, sem = refs
    wholes = 2 + (part[0] == 0)
    ins, outs = ins[wholes:-wholes], ins[-wholes:]
    t = Torus(side)
    layers = outs[0].shape[0]
    moves = []
    for c in COLOURS:
        a, _ = t.back(c, side - 1, 0)
        dst = outs[c // layers]
        dst = dst.at[c % layers, a] if c < 2 else dst.at[c % layers, :, a]
        moves.append(local(ins[c], cut_rows(dst, part, (slice(None),)), sem.at[c]))
        if wholes > 2:
            columns = pl.ds(c * ins[4].shape[-1], ins[4].shape[-1])
            dst = outs[2].at[:, a, :, :, columns] if c < 2 else outs[2].at[:, :, a, :, columns]
            moves.append(local(ins[4 + c], dst, sem.at[4 + c]))
    for move in moves:
        move.start()
    for move in moves:
        move.wait()


def solution(mesh):
    n = mesh.shape["dp"]
    side = math.isqrt(n)
    dma = pltpu.SemaphoreType.DMA
    anywhere, in_vmem = pl.BlockSpec(memory_space=pl.ANY), pl.BlockSpec(memory_space=pltpu.VMEM)

    def shape(*dims, dtype=BF16):
        return jax.ShapeDtypeStruct(dims, dtype)

    def in_hbm(*some):
        return [pltpu.with_memory_space_constraint(one, pltpu.HBM) for one in some]

    def permutation(c):
        moved = []
        for i in range(n):
            a, b = (i // side, i % side) if c < 2 else (i % side, i // side)
            a = (a + sign(c)) % side
            moved.append((i, a * side + b if c < 2 else b * side + a))
        return moved

    def step(*arrays):
        terms, weights, m, v = (arrays[i : i + 3] for i in (0, 3, 6, 9))
        layers, rows, wide = m[0].shape
        tall, narrow = m[2].shape[1:]
        assert side == 4 and side * side == n and layers * 2 == len(COLOURS), (n, layers)
        r, quarter = rows // PIECES, narrow // len(COLOURS)
        kinds = PIECES + layers
        block, low_block = (PIECES, r, wide), (tall, narrow)

        def cut(whole, *lead):
            return [one.reshape(layers, *lead, *dims) for one, dims in zip(whole, (block, block, low_block), strict=True)]

        m, v = cut(m), cut(v)
        assert r * wide == tall * quarter and kinds == 6
        parts = row_parts(r)
        stays = [shape(side, one[1], one[3], wide) for _ in COLOURS for one in parts] + [shape(layers, side, tall, quarter)] * 4
        out = pl.pallas_call(
            functools.partial(main_kernel, n, side, float(n * sum(one.size for one in m))),
            name="sum_step_gather",
            out_shape=(
                *(shape(layers, n, *block),) * 2, shape(layers, n, *low_block),
                *(shape(layers, *block),) * 2, shape(layers, *low_block),
                shape(8, 128, dtype=F32), *stays,
            ),
            in_specs=[anywhere] * 12,
            out_specs=[anywhere] * 6 + [in_vmem] + [anywhere] * len(stays),
            scratch_shapes=[
                pltpu.VMEM((2, 4, side, *block), BF16),
                pltpu.VMEM((2, 4, side, layers, tall, quarter), BF16),
                pltpu.VMEM((2, 4, *block), BF16),
                pltpu.VMEM((2, 4, layers, tall, quarter), BF16),
                pltpu.VMEM((4, 2, r, wide), F32),
                pltpu.VMEM((4, layers, tall, quarter), F32),
                pltpu.VMEM((4, 2, r, wide), F32),
                pltpu.VMEM((4, layers, tall, quarter), F32),
                pltpu.VMEM((8, 128), F32),
                pltpu.VMEM((n, 1, 128), F32),
                dma((2, 4, side)),
                dma((2, 4, side)),
                dma((4, kinds)),
                dma((4, 2)),
                dma((2, 4)),
                dma((4, 3)),
                pltpu.SemaphoreType.REGULAR((4,)),
                pltpu.SemaphoreType.REGULAR((4,)),
                pltpu.SemaphoreType.REGULAR((2,)),
                dma((2,)),
                dma((2, 2)),
            ],
            compiler_params=pltpu.CompilerParams(collective_id=0, has_side_effects=True, vmem_limit_bytes=66_000_000),
        )(*cut([one[0] for one in terms], n), *cut(weights, n), *m, *v)
        gathered, g, factor, stay = out[:3], out[3:6], out[6], out[7:]

        moved = {}
        for k in (0, len(parts), *range(1, len(parts))):
            for c in COLOURS:
                moved[c, k] = lax.ppermute(stay[c * len(parts) + k] if k < len(parts) else stay[4 * k + c], "dp", permutation(c))

        square = (layers, side, side)
        copied = pl.pallas_call(
            functools.partial(copy_kernel, side),
            name="copy_and_moments",
            out_shape=(
                *(shape(*square, *block),) * 2, shape(*square, *low_block),
                *((shape(layers, *block, dtype=F32),) * 2 + (shape(layers, *low_block, dtype=F32),)) * 2,
            ),
            in_specs=[anywhere] * 6 + [in_vmem] + [anywhere] * (6 + len(stay)),
            out_specs=[anywhere] * 9,
            scratch_shapes=[
                pltpu.VMEM((3, side, *block), BF16),
                pltpu.VMEM((4, layers, side, tall, quarter), BF16),
                pltpu.VMEM((1, *block), BF16),
                pltpu.VMEM((1, *low_block), BF16),
                pltpu.VMEM((1, *block), F32),
                pltpu.VMEM((1, *low_block), F32),
                pltpu.VMEM((1, *block), F32),
                pltpu.VMEM((1, *low_block), F32),
                dma((9, 3)),
                dma((9, 2)),
            ],
            cost_estimate=pl.CostEstimate(flops=10**9, bytes_accessed=200_000_000, transcendentals=0),
            compiler_params=pltpu.CompilerParams(vmem_limit_bytes=32_000_000),
        )(*in_hbm(*(one.reshape(*square, *one.shape[2:]) for one in gathered), *g), factor, *in_hbm(*m, *v, *stay))
        new_w, new_m, new_v = list(copied[:3]), copied[3:6], copied[6:]

        for k, one in enumerate(parts):
            wholes = 3 if k == 0 else 2
            arrived = [moved[c, k] for c in COLOURS] + [moved[c, len(parts)] for c in COLOURS if k == 0]
            new_w[:wholes] = pl.pallas_call(
                functools.partial(place_kernel, side, one),
                name=f"place_{k}",
                out_shape=[shape(*old.shape) for old in new_w[:wholes]],
                in_specs=[anywhere] * wholes + [in_vmem] * len(arrived),
                out_specs=[anywhere] * wholes,
                scratch_shapes=[dma((8,))],
                input_output_aliases={i: i for i in range(wholes)},
                compiler_params=pltpu.CompilerParams(vmem_limit_bytes=24_000_000),
            )(*new_w[:wholes], *arrived)
        return tuple(one.reshape(old.shape) for one, old in zip((*new_w, *new_m, *new_v), (*weights, *arrays[6:]), strict=True))

    all_of, part = P(None, None, None), P(None, "dp", None)
    return jax.shard_map(
        step,
        mesh=mesh,
        in_specs=(P(("rep", "dp"), None, None, None),) * 3 + (all_of,) * 3 + (part,) * 6,
        out_specs=(P("rep", None, None),) * 3 + (P("rep", "dp", None),) * 6,
        check_vma=False,
    )
```

```python
import functools
import math

import jax
import jax.numpy as jnp
from jax import lax
from jax.experimental import pallas as pl
from jax.experimental.pallas import tpu as pltpu
from jax.sharding import PartitionSpec as P

MESH = pl.DeviceIdType.MESH
F32, BF16 = jnp.float32, jnp.bfloat16
COLOURS = range(4)
PIECES = 4
ROWS, COLS = 0, 1
LATE_CORE, LATE_BY = 0, 15_000


def divisor(whole, unit, most):
    return max(d for d in range(unit, most + 1, unit) if whole % d == 0)


def row_parts(wide):
    end = 128 * max(1, 2 * (wide // 128) // 11)
    return [(0, PIECES - 1, 0, wide), (PIECES - 1, 1, 0, wide - end), (PIECES - 1, 1, wide - end, end)]


def cut_rows(ref, part, lead=()):
    return ref.at[(*lead, pl.ds(*part[:2]), slice(None), pl.ds(*part[2:]))]


def moments(m, v, g):
    m = 0.9 * m + 0.1 * g
    v = 0.95 * v + 0.05 * g * g
    return m, v


def new_weight(w, m, v):
    step = m * lax.rsqrt(v + 1e-8) + 0.1 * w
    return (w - 0.02 * step).astype(BF16)


class Torus:
    def __init__(self, side):
        self.side = side
        self.me = lax.axis_index("dp")
        self.x, self.y = self.me // side, lax.rem(self.me, side)

    def around(self, v):
        return lax.rem(v + 4 * self.side, self.side)

    def ab(self, c):
        return (self.x, self.y) if c < 2 else (self.y, self.x)

    def dev(self, c, a, b):
        return a * self.side + b if c < 2 else b * self.side + a

    def along_a(self, c, k):
        a, b = self.ab(c)
        return self.dev(c, self.around(a + k * sign(c)), b)

    def along_b(self, c, k):
        a, b = self.ab(c)
        return self.dev(c, a, self.around(b + k * sign(c)))

    def back(self, c, back_a, back_b):
        a, b = self.ab(c)
        return self.around(a - back_a * sign(c)), self.around(b - back_b * sign(c))

    def block(self, c, back_a, back_b):
        return self.dev(c, *self.back(c, back_a, back_b))


def sign(c):
    return 1 if c % 2 == 0 else -1


def remote(src, dst, send, recv, device):
    return pltpu.make_async_remote_copy(src, dst, send, recv, device_id={"dp": device}, device_id_type=MESH)


def local(src, dst, sem):
    return pltpu.make_async_copy(src, dst, sem)


def got(ref, sem):
    pltpu.make_async_copy(ref, ref, sem).wait()


def tell(sem, device):
    pl.semaphore_signal(sem, inc=1, device_id={"dp": device}, device_id_type=MESH)


def main_kernel(n, side, count,
                g_gate, g_up, g_down, w_gate, w_up, w_down, m_gate, m_up, m_down, v_gate, v_up, v_down,
                o_gate, o_up, o_down, og_gate, og_up, og_down, factor_ref, *rest):
    parts = row_parts(m_gate.shape[-1])
    stay, low_stay, rest = rest[: len(parts) * 4], rest[len(parts) * 4 : len(parts) * 4 + 4], rest[len(parts) * 4 + 4 :]
    bufr, bufc, ownr, ownc, mr, mc, vr, vc, acc, sq, rs, ss, p2r, p2s, own_sem, mv_sem, cred1, cred2, ready, sq_sem, loc = rest
    layers = g_gate.shape[0]
    wide = bufr.shape[-1]
    tall, quarter = bufc.shape[-2:]
    cstep, rstep = divisor(wide, 128, 384), divisor(tall, 8, 24)
    kinds = PIECES + layers
    t = Torus(side)
    me = t.me

    gates = (g_gate, g_up), (w_gate, w_up), (m_gate, m_up), (v_gate, v_up), (o_gate, o_up), (og_gate, og_up)
    downs = g_down, w_down, m_down, v_down, o_down, og_down
    TERM, WEIGHT, M, V, OUT, SUM = range(6)

    def pick(which, c):
        return gates[which][c // layers], c % layers

    def cols(c):
        return pl.ds(c * quarter, quarter)

    def group(which, c, kind, j):
        if kind == ROWS:
            ref, layer = pick(which, c)
            return ref.at[layer, j]
        return downs[which].at[:, j, :, cols(c)]

    def piece(which, c, i, j):
        if i < PIECES:
            ref, layer = pick(which, c)
            return ref.at[layer, j, i]
        return downs[which].at[i - PIECES, j, :, cols(c)]

    def own_group(which, c, kind):
        if kind == ROWS:
            ref, layer = pick(which, c)
            return ref.at[layer]
        return downs[which].at[:, :, cols(c)]

    def own_piece(which, c, i):
        if i < PIECES:
            ref, layer = pick(which, c)
            return ref.at[layer, i]
        return downs[which].at[i - PIECES, :, cols(c)]

    def buf(kind, *lead):
        return (bufr, bufc)[kind].at[lead]

    def own(kind, *lead):
        return (ownr, ownc)[kind].at[lead]

    def part(ref, kind, i):
        return ref.at[i if kind == ROWS else i - PIECES]

    def kind_of(i):
        return ROWS if i < PIECES else COLS

    def pieces(kind):
        return range(PIECES) if kind == ROWS else range(PIECES, kinds)

    def tiles(kind, body):
        if kind == ROWS:
            @pl.loop(0, wide // cstep)
            def _(k):
                body((slice(None), pl.ds(pl.multiple_of(k * cstep, 128), cstep)))
        else:
            @pl.loop(0, tall // rstep)
            def _(k):
                body((pl.ds(pl.multiple_of(k * rstep, 8), rstep), slice(None)))

    def add(kind, dst, *more):
        def body(at):
            total = dst[at].astype(F32)
            for one in more:
                total += one[at].astype(F32)
            dst[at] = total.astype(BF16)

        tiles(kind, body)

    def six(sem):
        got(bufr.at[0, 0, pl.ds(0, kinds // 3), pl.ds(0, 3)], sem)

    last = side - 1
    later = t.x < last, t.x == 0, t.y < last, t.y == 0
    there = tuple(t.along_a(c, 1) for c in COLOURS)
    towards = (0, 2, 1, 3)
    barrier = pltpu.get_barrier_semaphore()
    for c in towards:
        @pl.when(later[c])
        def _():
            tell(barrier, there[c])
    earlier = (t.x + 1) // 2 + (t.y + 1) // 2

    @pl.when(earlier > 0)
    def _():
        pl.semaphore_wait(barrier, earlier)

    for c in towards:
        @pl.when(jnp.logical_not(later[c]))
        def _():
            tell(ready.at[c ^ 1], there[c])

    @pl.when(lax.rem(lax.axis_index("rep"), 2) == LATE_CORE)
    def _():
        pl.delay(LATE_BY)

    def first_hop(q, c):
        for kind in (ROWS, COLS):
            remote(group(TERM, c, kind, t.block(c, 1, q + 1)), buf(kind, 0, c, q), ss.at[0, c, q], rs.at[0, c, q], there[c]).start()

    for c in towards:
        @pl.when(jnp.logical_not(later[c]))
        def _():
            first_hop(0, c)
    for c in towards:
        @pl.when(later[c])
        def _():
            pl.semaphore_wait(ready.at[c], 1)
            first_hop(0, c)

    @pl.loop(1, side)
    def _(q):
        for c in COLOURS:
            first_hop(q, c)

    def own_load(step, c, kind):
        stage, q = 1 + step // side, lax.rem(step, side)
        par = lax.rem(step, 2)
        return local(group(TERM, c, kind, t.block(c, stage + 1, q + 1)), own(kind, par, c), own_sem.at[par, c])

    def start_own(step):
        for kind in (ROWS, COLS):
            for c in COLOURS:
                own_load(step, c, kind).start()

    def mv_load(c, i):
        kind = kind_of(i)
        if kind == ROWS:
            return [local(own_piece(which, c, i), ref.at[c, i % 2], mv_sem.at[c, i % 2]) for which, ref in ((M, mr), (V, vr))]
        return [local(own_group(which, c, COLS), ref.at[c], mv_sem.at[c, 2]) for which, ref in ((M, mc), (V, vc))]

    def mv_wait(c, i):
        if kind_of(i) == ROWS:
            got(mr.at[c], mv_sem.at[c, i % 2])
        else:
            got(mc.at[pl.ds(0, 2)], mv_sem.at[c, 2])

    start_own(0)
    for i in (0, 1, PIECES):
        for c in COLOURS:
            for copy in mv_load(c, i):
                copy.start()

    @pl.loop(0, 2 * side)
    def _(step):
        par, q = step // side, lax.rem(step, side)
        start_own(step + 1)
        for c in COLOURS:
            six(rs.at[par, c, q])
            six(ss.at[par, c, q])

            @pl.when(par == 1)
            def _():
                tell(cred1.at[c], t.along_a(c, -1))

            six(own_sem.at[lax.rem(step, 2), c])
            for kind in (ROWS, COLS):
                here, mine = buf(kind, par, c, q), own(kind, lax.rem(step, 2), c)
                for i in pieces(kind):
                    add(kind, part(here, kind, i), part(mine, kind, i))
        for c in COLOURS:
            @pl.when(par == 1)
            def _():
                pl.semaphore_wait(cred1.at[c], 1)

            for kind in (ROWS, COLS):
                remote(buf(kind, par, c, q), buf(kind, 1 - par, c, q), ss.at[1 - par, c, q], rs.at[1 - par, c, q], t.along_a(c, 1)).start()

    acc[...] = jnp.zeros_like(acc)
    last_own = (3 * side) % 2
    for q in range(side):
        step = 2 * side + q
        if q < side - 1:
            start_own(step + 1)
        else:
            for kind in (ROWS, COLS):
                for c in COLOURS:
                    local(group(WEIGHT, c, kind, me), own(kind, last_own, c), own_sem.at[last_own, c]).start()
        for i in range(kinds):
            kind = kind_of(i)
            for c in COLOURS:
                whole, mine = buf(kind, 0, c, q), own(kind, step % 2, c)
                here = part(whole, kind, i)
                if i == 0:
                    six(rs.at[0, c, q])
                    six(ss.at[0, c, q])
                    six(own_sem.at[step % 2, c])
                more = [part(mine, kind, i)]
                if q:
                    got(here, p2r.at[c, i])
                    more.append(part(buf(kind, 1, c, q - 1), kind, i))
                if q < side - 1:
                    tell(cred2.at[c], t.along_b(c, -1))
                    add(kind, here, *more)
                    continue

                def last(at, here=here, more=more):
                    total = here[at].astype(F32)
                    for one in more:
                        total += one[at].astype(F32)
                    total = total.astype(BF16)
                    here[at] = total
                    square = total.astype(F32)
                    square = square * square
                    rows, columns = square.shape
                    acc[...] += sum(square[a : a + 8, b : b + 128] for a in range(0, rows, 8) for b in range(0, columns, 128))

                tiles(kind, last)
            if q < side - 1:
                for c in COLOURS:
                    pl.semaphore_wait(cred2.at[c], 1)
                    remote(part(buf(kind, 0, c, q), kind, i), part(buf(kind, 1, c, q), kind, i), p2s.at[c, kind], p2r.at[c, i], t.along_b(c, 1)).start()

    sq[me] = jnp.sum(acc[...], axis=0, keepdims=True)
    for k in range(1, n):
        remote(sq.at[me], sq.at[me], sq_sem.at[0], sq_sem.at[1], lax.rem(me + k, n)).start()
    for c in COLOURS:
        for kind in (ROWS, COLS):
            got((bufr, bufc)[kind].at[0, c, pl.ds(0, side - 1)], p2s.at[c, kind])
    got(sq.at[pl.ds(0, n - 1)], sq_sem.at[1])
    total = sum(sq[k] for k in range(n))
    total = jnp.sum(total, axis=(0, 1), keepdims=True)
    factor = jnp.minimum(1.0, 0.5 * lax.rsqrt(total / count + 1e-30))
    factor_ref[...] = jnp.broadcast_to(factor, factor_ref.shape)

    def arrived_b(c, hop):
        return p2r.at[c, hop - 1]

    def arrived_a(c, hop, q):
        return rs.at[hop - 1, c, q]

    def sent(c, kind):
        return p2s.at[c, kind]

    for i in range(kinds):
        kind = kind_of(i)
        for c in COLOURS:
            if i == 0:
                six(own_sem.at[last_own, c])
            if i <= PIECES:
                mv_wait(c, i)
            w_ref, g_ref = (part(ref, kind, i) for ref in (own(kind, last_own, c), buf(kind, 0, c, side - 1)))
            m_ref, v_ref = (rows.at[c, i % 2] if kind == ROWS else columns.at[c, i - PIECES] for rows, columns in ((mr, mc), (vr, vc)))

            def body(at, w_ref=w_ref, g_ref=g_ref, m_ref=m_ref, v_ref=v_ref):
                g = g_ref[at].astype(F32) * factor
                m, v = moments(m_ref[at], v_ref[at], g)
                w_ref[at] = new_weight(w_ref[at].astype(F32), m, v)

            tiles(kind, body)
            if i + 2 < PIECES:
                for copy in mv_load(c, i + 2):
                    copy.start()
        for c in COLOURS:
            remote(part(own(kind, last_own, c), kind, i), piece(OUT, c, i, me), sent(c, kind), arrived_b(c, 1), t.along_b(c, 1)).start()
    for kind in (ROWS, COLS):
        for c in COLOURS:
            mine, there = own(kind, last_own, c), group(OUT, c, kind, me)
            remote(mine, there, sent(c, kind), arrived_a(c, 1, 0), t.along_a(c, 1)).start()
            local(mine, there, loc.at[0, kind]).start()
            local(buf(kind, 0, c, side - 1), own_group(SUM, c, kind), loc.at[1, kind]).start()

    for hop in range(1, side):
        for c in COLOURS:
            six(arrived_b(c, hop))
            for kind in (ROWS, COLS):
                here = group(OUT, c, kind, t.block(c, 0, hop))
                if hop < side - 1:
                    remote(here, here, sent(c, kind), arrived_b(c, hop + 1), t.along_b(c, 1)).start()
                remote(here, here, sent(c, kind), arrived_a(c, 1, hop), t.along_a(c, 1)).start()

    for hop in range(1, side - 2):
        for q in range(side):
            for c in COLOURS:
                six(arrived_a(c, hop, q))
                a, b = t.back(c, hop, q)
                next_hop = functools.partial(remote, recv=arrived_a(c, hop + 1, q), device=t.along_a(c, 1))
                rows, columns = (group(OUT, c, kind, t.dev(c, a, b)) for kind in (ROWS, COLS))
                if hop < side - 3:
                    next_hop(rows, rows, send=sent(c, ROWS)).start()
                    next_hop(columns, columns, send=sent(c, COLS)).start()
                    continue
                for k, one in enumerate(parts):
                    next_hop(cut_rows(rows, one), stay[c * len(parts) + k].at[b], send=sent(c, ROWS)).start()
                next_hop(columns, low_stay[c].at[:, b], send=sent(c, COLS)).start()
    for q in range(side):
        for c in COLOURS:
            six(arrived_a(c, side - 2, q))

    got(sq.at[pl.ds(0, n - 1)], sq_sem.at[0])
    for kind in (ROWS, COLS):
        for k in range(2):
            got((ownr, ownc)[kind].at[last_own], loc.at[k, kind])
    for c in COLOURS:
        ref, layer = pick(OUT, c)
        got(ref.at[layer, pl.ds(0, n - 1 - side)], sent(c, ROWS))
        got(o_down.at[:, pl.ds(0, n - 1 - side), :, cols(c)], sent(c, COLS))


def copy_kernel(side, t_gate, t_up, t_down, g_gate, g_up, g_down, factor_ref, m_gate, m_up, m_down, v_gate, v_up, v_down, *rest):
    parts = row_parts(m_gate.shape[-1])
    stay, low_stay, rest = rest[: 4 * len(parts)], rest[4 * len(parts) : 4 * len(parts) + 4], rest[4 * len(parts) + 4 :]
    o_gate, o_up, o_down, nm_gate, nm_up, nm_down, nv_gate, nv_up, nv_down, rowbuf, colbuf, gr, gc, mr, mc, vr, vc, load_sem, store_sem = rest
    layers = o_down.shape[0]
    wide = gr.shape[-1]
    tall = gc.shape[-2]
    quarter = colbuf.shape[-1]
    t = Torus(side)
    factor = factor_ref[0:1, 0:1]

    def at_a(ref, layer, c, a):
        return ref.at[layer, a] if c < 2 else ref.at[layer, :, a]

    def low_at_a(ref, c, a):
        columns = pl.ds(c * quarter, quarter)
        return ref.at[:, a, :, :, columns] if c < 2 else ref.at[:, :, a, :, columns]

    jobs = []
    slots = {"rows": (rowbuf, 0), "cols": (colbuf, 1)}
    made = {"rows": 0, "cols": 0, "mr": 0, "mc": 0}
    depth = {"rows": rowbuf.shape[0], "cols": colbuf.shape[0], "mr": gr.shape[0], "mc": gc.shape[0]}
    base = {"rows": 0, "cols": depth["rows"], "mr": depth["rows"] + depth["cols"], "mc": depth["rows"] + depth["cols"] + depth["mr"]}

    def job(what, loads, stores, work=None):
        slot = made[what] % depth[what]
        made[what] += 1
        jobs.append((what, slot, [f(slot) for f in loads], [f(slot) for f in stores], work and functools.partial(work, slot)))

    def copy_job(what, src, dst):
        ref = slots[what][0]
        job(what, [lambda slot: (src, ref.at[slot])], [lambda slot: (ref.at[slot], dst)])

    def step(gs, ms, vs, parts, where, slot):
        @pl.loop(0, parts)
        def _(k):
            at = (slot, *where(k))
            g = gs[at].astype(F32) * factor
            ms[at], vs[at] = moments(ms[at], vs[at], g)

    def moment_job(what, g, m, v, nm, nv):
        gs, ms, vs = (gr, mr, vr) if what == "mr" else (gc, mc, vc)
        if what == "mr":
            size = divisor(wide, 128, 384)
            parts = gs.shape[1] * (wide // size)
            each = wide // size
            where = lambda k: (k // each, slice(None), pl.ds(pl.multiple_of(lax.rem(k, each) * size, 128), size))
        else:
            size = divisor(tall, 8, 24)
            parts = tall // size
            where = lambda k: (pl.ds(pl.multiple_of(k * size, 8), size), slice(None))
        job(
            what,
            [lambda slot: (g, gs.at[slot]), lambda slot: (m, ms.at[slot]), lambda slot: (v, vs.at[slot])],
            [lambda slot: (ms.at[slot], nm), lambda slot: (vs.at[slot], nv)],
            functools.partial(step, gs, ms, vs, parts, where),
        )

    big = ((t_gate, o_gate), (t_up, o_up))
    small = ((g_gate, m_gate, v_gate, nm_gate, nv_gate), (g_up, m_up, v_up, nm_up, nv_up), (g_down, m_down, v_down, nm_down, nv_down))
    for c in COLOURS:
        layer = c % layers
        src, dst = big[c // layers]
        for back in range(side - 2):
            a, _ = t.back(c, back, 0)
            copy_job("rows", at_a(src, layer, c, a), at_a(dst, layer, c, a))
        moment_job("mr", *(one.at[layer] for one in small[c // layers]))
        a, _ = t.back(c, side - 2, 0)
        ref = rowbuf
        job(
            "rows",
            [lambda slot, src=stay[c * len(parts) + k], one=one: (src, cut_rows(ref, one, (slot, slice(None)))) for k, one in enumerate(parts)],
            [lambda slot, layer=layer, c=c, a=a, dst=dst: (ref.at[slot], at_a(dst, layer, c, a))],
        )
        for back in range(side - 2):
            a, _ = t.back(c, back, 0)
            copy_job("cols", low_at_a(t_down, c, a), low_at_a(o_down, c, a))
        a, _ = t.back(c, side - 2, 0)
        copy_job("cols", low_stay[c], low_at_a(o_down, c, a))
        if c // layers == 1:
            moment_job("mc", *(one.at[layer] for one in small[2]))

    def copies(k, which):
        what, slot = jobs[k][:2]
        sem = (load_sem, store_sem)[which]
        return [local(src, dst, sem.at[base[what] + slot, z]) for z, (src, dst) in enumerate(jobs[k][2 + which])]

    ahead, stored = 4, [False] * len(jobs)

    def start_loads(k):
        for one in range(k):
            if jobs[one][:2] == jobs[k][:2] and not stored[one]:
                for copy in copies(one, 1):
                    copy.wait()
                stored[one] = True
        for copy in copies(k, 0):
            copy.start()

    for k in range(ahead):
        start_loads(k)
    for k, (*_, work) in enumerate(jobs):
        for copy in copies(k, 0):
            copy.wait()
        if work is not None:
            work()
        for copy in copies(k, 1):
            copy.start()
        if k + ahead < len(jobs):
            start_loads(k + ahead)
    for k in range(len(jobs)):
        if not stored[k]:
            for copy in copies(k, 1):
                copy.wait()


def place_kernel(side, part, *refs):
    *ins, sem = refs
    wholes = 2 + (part[0] == 0)
    ins, outs = ins[wholes:-wholes], ins[-wholes:]
    t = Torus(side)
    layers = outs[0].shape[0]
    moves = []
    for c in COLOURS:
        a, _ = t.back(c, side - 1, 0)
        dst = outs[c // layers]
        dst = dst.at[c % layers, a] if c < 2 else dst.at[c % layers, :, a]
        moves.append(local(ins[c], cut_rows(dst, part, (slice(None),)), sem.at[c]))
        if wholes > 2:
            columns = pl.ds(c * ins[4].shape[-1], ins[4].shape[-1])
            dst = outs[2].at[:, a, :, :, columns] if c < 2 else outs[2].at[:, :, a, :, columns]
            moves.append(local(ins[4 + c], dst, sem.at[4 + c]))
    for move in moves:
        move.start()
    for move in moves:
        move.wait()


def solution(mesh):
    n = mesh.shape["dp"]
    side = math.isqrt(n)
    dma = pltpu.SemaphoreType.DMA
    anywhere, in_vmem = pl.BlockSpec(memory_space=pl.ANY), pl.BlockSpec(memory_space=pltpu.VMEM)

    def shape(*dims, dtype=BF16):
        return jax.ShapeDtypeStruct(dims, dtype)

    def in_hbm(*some):
        return [pltpu.with_memory_space_constraint(one, pltpu.HBM) for one in some]

    def permutation(c):
        moved = []
        for i in range(n):
            a, b = (i // side, i % side) if c < 2 else (i % side, i // side)
            a = (a + sign(c)) % side
            moved.append((i, a * side + b if c < 2 else b * side + a))
        return moved

    def step(*arrays):
        terms, weights, m, v = (arrays[i : i + 3] for i in (0, 3, 6, 9))
        layers, rows, wide = m[0].shape
        tall, narrow = m[2].shape[1:]
        assert side == 4 and side * side == n and layers * 2 == len(COLOURS), (n, layers)
        r, quarter = rows // PIECES, narrow // len(COLOURS)
        kinds = PIECES + layers
        block, low_block = (PIECES, r, wide), (tall, narrow)

        def cut(whole, *lead):
            return [one.reshape(layers, *lead, *dims) for one, dims in zip(whole, (block, block, low_block), strict=True)]

        m, v = cut(m), cut(v)
        assert r * wide == tall * quarter and kinds == 6
        parts = row_parts(wide)
        stays = [shape(side, one[1], r, one[3]) for _ in COLOURS for one in parts] + [shape(layers, side, tall, quarter)] * 4
        out = pl.pallas_call(
            functools.partial(main_kernel, n, side, float(n * sum(one.size for one in m))),
            name="sum_step_gather",
            out_shape=(
                *(shape(layers, n, *block),) * 2, shape(layers, n, *low_block),
                *(shape(layers, *block),) * 2, shape(layers, *low_block),
                shape(8, 128, dtype=F32), *stays,
            ),
            in_specs=[anywhere] * 12,
            out_specs=[anywhere] * 6 + [in_vmem] + [anywhere] * len(stays),
            scratch_shapes=[
                pltpu.VMEM((2, 4, side, *block), BF16),
                pltpu.VMEM((2, 4, side, layers, tall, quarter), BF16),
                pltpu.VMEM((2, 4, *block), BF16),
                pltpu.VMEM((2, 4, layers, tall, quarter), BF16),
                pltpu.VMEM((4, 2, r, wide), F32),
                pltpu.VMEM((4, layers, tall, quarter), F32),
                pltpu.VMEM((4, 2, r, wide), F32),
                pltpu.VMEM((4, layers, tall, quarter), F32),
                pltpu.VMEM((8, 128), F32),
                pltpu.VMEM((n, 1, 128), F32),
                dma((2, 4, side)),
                dma((2, 4, side)),
                dma((4, kinds)),
                dma((4, 2)),
                dma((2, 4)),
                dma((4, 3)),
                pltpu.SemaphoreType.REGULAR((4,)),
                pltpu.SemaphoreType.REGULAR((4,)),
                pltpu.SemaphoreType.REGULAR((4,)),
                dma((2,)),
                dma((2, 2)),
            ],
            compiler_params=pltpu.CompilerParams(collective_id=0, has_side_effects=True, vmem_limit_bytes=66_000_000),
        )(*cut([one[0] for one in terms], n), *cut(weights, n), *m, *v)
        gathered, g, factor, stay = out[:3], out[3:6], out[6], out[7:]

        moved = {}
        for k in (0, len(parts), *range(1, len(parts))):
            for c in COLOURS:
                moved[c, k] = lax.ppermute(stay[c * len(parts) + k] if k < len(parts) else stay[4 * k + c], "dp", permutation(c))

        square = (layers, side, side)
        copied = pl.pallas_call(
            functools.partial(copy_kernel, side),
            name="copy_and_moments",
            out_shape=(
                *(shape(*square, *block),) * 2, shape(*square, *low_block),
                *((shape(layers, *block, dtype=F32),) * 2 + (shape(layers, *low_block, dtype=F32),)) * 2,
            ),
            in_specs=[anywhere] * 6 + [in_vmem] + [anywhere] * (6 + len(stay)),
            out_specs=[anywhere] * 9,
            scratch_shapes=[
                pltpu.VMEM((3, side, *block), BF16),
                pltpu.VMEM((4, layers, side, tall, quarter), BF16),
                pltpu.VMEM((1, *block), BF16),
                pltpu.VMEM((1, *low_block), BF16),
                pltpu.VMEM((1, *block), F32),
                pltpu.VMEM((1, *low_block), F32),
                pltpu.VMEM((1, *block), F32),
                pltpu.VMEM((1, *low_block), F32),
                dma((9, 3)),
                dma((9, 2)),
            ],
            cost_estimate=pl.CostEstimate(flops=10**9, bytes_accessed=200_000_000, transcendentals=0),
            compiler_params=pltpu.CompilerParams(vmem_limit_bytes=32_000_000),
        )(*in_hbm(*(one.reshape(*square, *one.shape[2:]) for one in gathered), *g), factor, *in_hbm(*m, *v, *stay))
        new_w, new_m, new_v = list(copied[:3]), copied[3:6], copied[6:]

        for k, one in enumerate(parts):
            wholes = 3 if k == 0 else 2
            arrived = [moved[c, k] for c in COLOURS] + [moved[c, len(parts)] for c in COLOURS if k == 0]
            new_w[:wholes] = pl.pallas_call(
                functools.partial(place_kernel, side, one),
                name=f"place_{k}",
                out_shape=[shape(*old.shape) for old in new_w[:wholes]],
                in_specs=[anywhere] * wholes + [in_vmem] * len(arrived),
                out_specs=[anywhere] * wholes,
                scratch_shapes=[dma((8,))],
                input_output_aliases={i: i for i in range(wholes)},
                compiler_params=pltpu.CompilerParams(vmem_limit_bytes=24_000_000),
            )(*new_w[:wholes], *arrived)
        return tuple(one.reshape(old.shape) for one, old in zip((*new_w, *new_m, *new_v), (*weights, *arrays[6:]), strict=True))

    all_of, part = P(None, None, None), P(None, "dp", None)
    return jax.shard_map(
        step,
        mesh=mesh,
        in_specs=(P(("rep", "dp"), None, None, None),) * 3 + (all_of,) * 3 + (part,) * 6,
        out_specs=(P("rep", None, None),) * 3 + (P("rep", "dp", None),) * 6,
        check_vma=False,
    )
```

```python
import functools
import math

import jax
import jax.numpy as jnp
from jax import lax
from jax.experimental import pallas as pl
from jax.experimental.pallas import tpu as pltpu
from jax.sharding import PartitionSpec as P

MESH = pl.DeviceIdType.MESH
F32, BF16 = jnp.float32, jnp.bfloat16
COLOURS = range(4)
PIECES = 4
PARTS = 3
ROWS, COLS = 0, 1
SPARED = 2
LATE_CORE, LATE_BY = 0, 15_000


def divisor(whole, unit, most):
    return max(d for d in range(unit, most + 1, unit) if whole % d == 0)


def last_columns(wide):
    tiles = wide // 128
    return 128 * max(2, 2 * tiles // 11), 128 * max(1, tiles // 33)


def row_parts(wide, c):
    end, aside = last_columns(wide)
    return [(0, PIECES - 1, 0, wide), (PIECES - 1, 1, 0, wide - end), (PIECES - 1, 1, wide - end, end - aside * (c == SPARED))]


def aside_part(wide):
    _, aside = last_columns(wide)
    return PIECES - 1, 1, wide - aside, aside


def cut_rows(ref, part, lead=()):
    return ref.at[(*lead, pl.ds(*part[:2]), slice(None), pl.ds(*part[2:]))]


def moments(m, v, g):
    m = 0.9 * m + 0.1 * g
    v = 0.95 * v + 0.05 * g * g
    return m, v


def new_weight(w, m, v):
    step = m * lax.rsqrt(v + 1e-8) + 0.1 * w
    return (w - 0.02 * step).astype(BF16)


class Torus:
    def __init__(self, side):
        self.side = side
        self.me = lax.axis_index("dp")
        self.x, self.y = self.me // side, lax.rem(self.me, side)

    def around(self, v):
        return lax.rem(v + 4 * self.side, self.side)

    def ab(self, c):
        return (self.x, self.y) if c < 2 else (self.y, self.x)

    def dev(self, c, a, b):
        return a * self.side + b if c < 2 else b * self.side + a

    def along_a(self, c, k):
        a, b = self.ab(c)
        return self.dev(c, self.around(a + k * sign(c)), b)

    def along_b(self, c, k):
        a, b = self.ab(c)
        return self.dev(c, a, self.around(b + k * sign(c)))

    def back(self, c, back_a, back_b):
        a, b = self.ab(c)
        return self.around(a - back_a * sign(c)), self.around(b - back_b * sign(c))

    def block(self, c, back_a, back_b):
        return self.dev(c, *self.back(c, back_a, back_b))


def sign(c):
    return 1 if c % 2 == 0 else -1


def remote(src, dst, send, recv, device):
    return pltpu.make_async_remote_copy(src, dst, send, recv, device_id={"dp": device}, device_id_type=MESH)


def local(src, dst, sem):
    return pltpu.make_async_copy(src, dst, sem)


def got(ref, sem):
    pltpu.make_async_copy(ref, ref, sem).wait()


def tell(sem, device):
    pl.semaphore_signal(sem, inc=1, device_id={"dp": device}, device_id_type=MESH)


def main_kernel(n, side, count,
                g_gate, g_up, g_down, w_gate, w_up, w_down, m_gate, m_up, m_down, v_gate, v_up, v_down,
                o_gate, o_up, o_down, og_gate, og_up, og_down, factor_ref, *rest):
    stay, low_stay, rest = rest[: PARTS * 4], rest[PARTS * 4 : PARTS * 4 + 4], rest[PARTS * 4 + 4 :]
    bufr, bufc, ownr, ownc, mr, mc, vr, vc, acc, sq, rs, ss, p2r, p2s, own_sem, mv_sem, cred1, cred2, ready, sq_sem, loc = rest
    layers = g_gate.shape[0]
    wide = bufr.shape[-1]
    tall, quarter = bufc.shape[-2:]
    cstep, rstep = divisor(wide, 128, 384), divisor(tall, 8, 24)
    kinds = PIECES + layers
    t = Torus(side)
    me = t.me

    gates = (g_gate, g_up), (w_gate, w_up), (m_gate, m_up), (v_gate, v_up), (o_gate, o_up), (og_gate, og_up)
    downs = g_down, w_down, m_down, v_down, o_down, og_down
    TERM, WEIGHT, M, V, OUT, SUM = range(6)

    def pick(which, c):
        return gates[which][c // layers], c % layers

    def cols(c):
        return pl.ds(c * quarter, quarter)

    def group(which, c, kind, j):
        if kind == ROWS:
            ref, layer = pick(which, c)
            return ref.at[layer, j]
        return downs[which].at[:, j, :, cols(c)]

    def piece(which, c, i, j):
        if i < PIECES:
            ref, layer = pick(which, c)
            return ref.at[layer, j, i]
        return downs[which].at[i - PIECES, j, :, cols(c)]

    def own_group(which, c, kind):
        if kind == ROWS:
            ref, layer = pick(which, c)
            return ref.at[layer]
        return downs[which].at[:, :, cols(c)]

    def own_piece(which, c, i):
        if i < PIECES:
            ref, layer = pick(which, c)
            return ref.at[layer, i]
        return downs[which].at[i - PIECES, :, cols(c)]

    def buf(kind, *lead):
        return (bufr, bufc)[kind].at[lead]

    def own(kind, *lead):
        return (ownr, ownc)[kind].at[lead]

    def part(ref, kind, i):
        return ref.at[i if kind == ROWS else i - PIECES]

    def kind_of(i):
        return ROWS if i < PIECES else COLS

    def pieces(kind):
        return range(PIECES) if kind == ROWS else range(PIECES, kinds)

    def tiles(kind, body):
        if kind == ROWS:
            @pl.loop(0, wide // cstep)
            def _(k):
                body((slice(None), pl.ds(pl.multiple_of(k * cstep, 128), cstep)))
        else:
            @pl.loop(0, tall // rstep)
            def _(k):
                body((pl.ds(pl.multiple_of(k * rstep, 8), rstep), slice(None)))

    def add(kind, dst, *more):
        def body(at):
            total = dst[at].astype(F32)
            for one in more:
                total += one[at].astype(F32)
            dst[at] = total.astype(BF16)

        tiles(kind, body)

    def six(sem):
        got(bufr.at[0, 0, pl.ds(0, kinds // 3), pl.ds(0, 3)], sem)

    last = side - 1
    later = t.x < last, t.x == 0, t.y < last, t.y == 0
    there = tuple(t.along_a(c, 1) for c in COLOURS)
    towards = (0, 2, 1, 3)
    barrier = pltpu.get_barrier_semaphore()
    for c in towards:
        @pl.when(later[c])
        def _():
            tell(barrier, there[c])
    earlier = (t.x + 1) // 2 + (t.y + 1) // 2

    @pl.when(earlier > 0)
    def _():
        pl.semaphore_wait(barrier, earlier)

    for c in towards:
        @pl.when(jnp.logical_not(later[c]))
        def _():
            tell(ready.at[c ^ 1], there[c])

    @pl.when(lax.rem(lax.axis_index("rep"), 2) == LATE_CORE)
    def _():
        pl.delay(LATE_BY)

    def first_hop(q, c):
        for kind in (ROWS, COLS):
            remote(group(TERM, c, kind, t.block(c, 1, q + 1)), buf(kind, 0, c, q), ss.at[0, c, q], rs.at[0, c, q], there[c]).start()

    for c in towards:
        @pl.when(jnp.logical_not(later[c]))
        def _():
            first_hop(0, c)
    for c in towards:
        @pl.when(later[c])
        def _():
            pl.semaphore_wait(ready.at[c], 1)
            first_hop(0, c)

    @pl.loop(1, side)
    def _(q):
        for c in COLOURS:
            first_hop(q, c)

    def own_load(step, c, kind):
        stage, q = 1 + step // side, lax.rem(step, side)
        par = lax.rem(step, 2)
        return local(group(TERM, c, kind, t.block(c, stage + 1, q + 1)), own(kind, par, c), own_sem.at[par, c])

    def start_own(step):
        for kind in (ROWS, COLS):
            for c in COLOURS:
                own_load(step, c, kind).start()

    def mv_load(c, i):
        kind = kind_of(i)
        if kind == ROWS:
            return [local(own_piece(which, c, i), ref.at[c, i % 2], mv_sem.at[c, i % 2]) for which, ref in ((M, mr), (V, vr))]
        return [local(own_group(which, c, COLS), ref.at[c], mv_sem.at[c, 2]) for which, ref in ((M, mc), (V, vc))]

    def mv_wait(c, i):
        if kind_of(i) == ROWS:
            got(mr.at[c], mv_sem.at[c, i % 2])
        else:
            got(mc.at[pl.ds(0, 2)], mv_sem.at[c, 2])

    start_own(0)
    for i in (0, 1, PIECES):
        for c in COLOURS:
            for copy in mv_load(c, i):
                copy.start()

    @pl.loop(0, 2 * side)
    def _(step):
        par, q = step // side, lax.rem(step, side)
        start_own(step + 1)
        for c in COLOURS:
            six(rs.at[par, c, q])
            six(ss.at[par, c, q])

            @pl.when(par == 1)
            def _():
                tell(cred1.at[c], t.along_a(c, -1))

            six(own_sem.at[lax.rem(step, 2), c])
            for kind in (ROWS, COLS):
                here, mine = buf(kind, par, c, q), own(kind, lax.rem(step, 2), c)
                for i in pieces(kind):
                    add(kind, part(here, kind, i), part(mine, kind, i))
        for c in COLOURS:
            @pl.when(par == 1)
            def _():
                pl.semaphore_wait(cred1.at[c], 1)

            for kind in (ROWS, COLS):
                remote(buf(kind, par, c, q), buf(kind, 1 - par, c, q), ss.at[1 - par, c, q], rs.at[1 - par, c, q], t.along_a(c, 1)).start()

    acc[...] = jnp.zeros_like(acc)
    last_own = (3 * side) % 2
    for q in range(side):
        step = 2 * side + q
        if q < side - 1:
            start_own(step + 1)
        else:
            for kind in (ROWS, COLS):
                for c in COLOURS:
                    local(group(WEIGHT, c, kind, me), own(kind, last_own, c), own_sem.at[last_own, c]).start()
        for i in range(kinds):
            kind = kind_of(i)
            for c in COLOURS:
                whole, mine = buf(kind, 0, c, q), own(kind, step % 2, c)
                here = part(whole, kind, i)
                if i == 0:
                    six(rs.at[0, c, q])
                    six(ss.at[0, c, q])
                    six(own_sem.at[step % 2, c])
                more = [part(mine, kind, i)]
                if q:
                    got(here, p2r.at[c, i])
                    more.append(part(buf(kind, 1, c, q - 1), kind, i))
                if q < side - 1:
                    tell(cred2.at[c], t.along_b(c, -1))
                    add(kind, here, *more)
                    continue

                def last(at, here=here, more=more):
                    total = here[at].astype(F32)
                    for one in more:
                        total += one[at].astype(F32)
                    total = total.astype(BF16)
                    here[at] = total
                    square = total.astype(F32)
                    square = square * square
                    rows, columns = square.shape
                    acc[...] += sum(square[a : a + 8, b : b + 128] for a in range(0, rows, 8) for b in range(0, columns, 128))

                tiles(kind, last)
            if q < side - 1:
                for c in COLOURS:
                    pl.semaphore_wait(cred2.at[c], 1)
                    remote(part(buf(kind, 0, c, q), kind, i), part(buf(kind, 1, c, q), kind, i), p2s.at[c, kind], p2r.at[c, i], t.along_b(c, 1)).start()

    sq[me] = jnp.sum(acc[...], axis=0, keepdims=True)
    for k in range(1, n):
        remote(sq.at[me], sq.at[me], sq_sem.at[0], sq_sem.at[1], lax.rem(me + k, n)).start()
    for c in COLOURS:
        for kind in (ROWS, COLS):
            got((bufr, bufc)[kind].at[0, c, pl.ds(0, side - 1)], p2s.at[c, kind])
    got(sq.at[pl.ds(0, n - 1)], sq_sem.at[1])
    total = sum(sq[k] for k in range(n))
    total = jnp.sum(total, axis=(0, 1), keepdims=True)
    factor = jnp.minimum(1.0, 0.5 * lax.rsqrt(total / count + 1e-30))
    factor_ref[...] = jnp.broadcast_to(factor, factor_ref.shape)

    def arrived_b(c, hop):
        return p2r.at[c, hop - 1]

    def arrived_a(c, hop, q):
        return rs.at[hop - 1, c, q]

    def sent(c, kind):
        return p2s.at[c, kind]

    aside = aside_part(wide)

    def send_aside(c, kind, src, dst):
        if c == SPARED and kind == ROWS:
            remote(cut_rows(src, aside), cut_rows(dst, aside), own_sem.at[1, 3], own_sem.at[1, 2], t.along_a(c, -1)).start()

    for i in range(kinds):
        kind = kind_of(i)
        for c in COLOURS:
            if i == 0:
                six(own_sem.at[last_own, c])
            if i <= PIECES:
                mv_wait(c, i)
            w_ref, g_ref = (part(ref, kind, i) for ref in (own(kind, last_own, c), buf(kind, 0, c, side - 1)))
            m_ref, v_ref = (rows.at[c, i % 2] if kind == ROWS else columns.at[c, i - PIECES] for rows, columns in ((mr, mc), (vr, vc)))

            def body(at, w_ref=w_ref, g_ref=g_ref, m_ref=m_ref, v_ref=v_ref):
                g = g_ref[at].astype(F32) * factor
                m, v = moments(m_ref[at], v_ref[at], g)
                w_ref[at] = new_weight(w_ref[at].astype(F32), m, v)

            tiles(kind, body)
            if i + 2 < PIECES:
                for copy in mv_load(c, i + 2):
                    copy.start()
        for c in COLOURS:
            remote(part(own(kind, last_own, c), kind, i), piece(OUT, c, i, me), sent(c, kind), arrived_b(c, 1), t.along_b(c, 1)).start()
    for kind in (ROWS, COLS):
        for c in COLOURS:
            mine, there = own(kind, last_own, c), group(OUT, c, kind, me)
            remote(mine, there, sent(c, kind), arrived_a(c, 1, 0), t.along_a(c, 1)).start()
            send_aside(c, kind, mine, there)
            local(mine, there, loc.at[0, kind]).start()
            local(buf(kind, 0, c, side - 1), own_group(SUM, c, kind), loc.at[1, kind]).start()

    for hop in range(1, side):
        for c in COLOURS:
            six(arrived_b(c, hop))
            for kind in (ROWS, COLS):
                here = group(OUT, c, kind, t.block(c, 0, hop))
                if hop < side - 1:
                    remote(here, here, sent(c, kind), arrived_b(c, hop + 1), t.along_b(c, 1)).start()
                remote(here, here, sent(c, kind), arrived_a(c, 1, hop), t.along_a(c, 1)).start()
                send_aside(c, kind, here, here)

    for hop in range(1, side - 2):
        for q in range(side):
            for c in COLOURS:
                six(arrived_a(c, hop, q))
                a, b = t.back(c, hop, q)
                next_hop = functools.partial(remote, recv=arrived_a(c, hop + 1, q), device=t.along_a(c, 1))
                rows, columns = (group(OUT, c, kind, t.dev(c, a, b)) for kind in (ROWS, COLS))
                if hop < side - 3:
                    next_hop(rows, rows, send=sent(c, ROWS)).start()
                    next_hop(columns, columns, send=sent(c, COLS)).start()
                    continue
                for k, one in enumerate(row_parts(wide, c)):
                    next_hop(cut_rows(rows, one), stay[c * PARTS + k].at[b], send=sent(c, ROWS)).start()
                if c == SPARED:
                    next_hop(cut_rows(rows, aside), cut_rows(rows, aside), send=sent(c, ROWS)).start()
                next_hop(columns, low_stay[c].at[:, b], send=sent(c, COLS)).start()
    for q in range(side):
        for c in COLOURS:
            six(arrived_a(c, side - 2, q))

    ref, layer = pick(OUT, SPARED)
    for k in (2, 3):
        got(cut_rows(ref, aside, (layer, pl.ds(0, side))), own_sem.at[1, k])

    got(sq.at[pl.ds(0, n - 1)], sq_sem.at[0])
    for kind in (ROWS, COLS):
        for k in range(2):
            got((ownr, ownc)[kind].at[last_own], loc.at[k, kind])
    for c in COLOURS:
        ref, layer = pick(OUT, c)
        got(ref.at[layer, pl.ds(0, n - 1 - side)], sent(c, ROWS))
        got(o_down.at[:, pl.ds(0, n - 1 - side), :, cols(c)], sent(c, COLS))


def copy_kernel(side, t_gate, t_up, t_down, g_gate, g_up, g_down, factor_ref, m_gate, m_up, m_down, v_gate, v_up, v_down, *rest):
    stay, low_stay, rest = rest[: 4 * PARTS], rest[4 * PARTS : 4 * PARTS + 4], rest[4 * PARTS + 4 :]
    o_gate, o_up, o_down, nm_gate, nm_up, nm_down, nv_gate, nv_up, nv_down, rowbuf, colbuf, gr, gc, mr, mc, vr, vc, load_sem, store_sem = rest
    layers = o_down.shape[0]
    wide = gr.shape[-1]
    tall = gc.shape[-2]
    quarter = colbuf.shape[-1]
    t = Torus(side)
    factor = factor_ref[0:1, 0:1]

    def at_a(ref, layer, c, a):
        return ref.at[layer, a] if c < 2 else ref.at[layer, :, a]

    def low_at_a(ref, c, a):
        columns = pl.ds(c * quarter, quarter)
        return ref.at[:, a, :, :, columns] if c < 2 else ref.at[:, :, a, :, columns]

    jobs = []
    slots = {"rows": (rowbuf, 0), "cols": (colbuf, 1)}
    made = {"rows": 0, "cols": 0, "mr": 0, "mc": 0}
    depth = {"rows": rowbuf.shape[0], "cols": colbuf.shape[0], "mr": gr.shape[0], "mc": gc.shape[0]}
    base = {"rows": 0, "cols": depth["rows"], "mr": depth["rows"] + depth["cols"], "mc": depth["rows"] + depth["cols"] + depth["mr"]}

    def job(what, loads, stores, work=None):
        slot = made[what] % depth[what]
        made[what] += 1
        jobs.append((what, slot, [f(slot) for f in loads], [f(slot) for f in stores], work and functools.partial(work, slot)))

    def copy_job(what, src, dst):
        ref = slots[what][0]
        job(what, [lambda slot: (src, ref.at[slot])], [lambda slot: (ref.at[slot], dst)])

    def step(gs, ms, vs, parts, where, slot):
        @pl.loop(0, parts)
        def _(k):
            at = (slot, *where(k))
            g = gs[at].astype(F32) * factor
            ms[at], vs[at] = moments(ms[at], vs[at], g)

    def moment_job(what, g, m, v, nm, nv):
        gs, ms, vs = (gr, mr, vr) if what == "mr" else (gc, mc, vc)
        if what == "mr":
            size = divisor(wide, 128, 384)
            parts = gs.shape[1] * (wide // size)
            each = wide // size
            where = lambda k: (k // each, slice(None), pl.ds(pl.multiple_of(lax.rem(k, each) * size, 128), size))
        else:
            size = divisor(tall, 8, 24)
            parts = tall // size
            where = lambda k: (pl.ds(pl.multiple_of(k * size, 8), size), slice(None))
        job(
            what,
            [lambda slot: (g, gs.at[slot]), lambda slot: (m, ms.at[slot]), lambda slot: (v, vs.at[slot])],
            [lambda slot: (ms.at[slot], nm), lambda slot: (vs.at[slot], nv)],
            functools.partial(step, gs, ms, vs, parts, where),
        )

    big = ((t_gate, o_gate), (t_up, o_up))
    small = ((g_gate, m_gate, v_gate, nm_gate, nv_gate), (g_up, m_up, v_up, nm_up, nv_up), (g_down, m_down, v_down, nm_down, nv_down))
    for c in COLOURS:
        layer = c % layers
        src, dst = big[c // layers]
        for back in range(side - 2):
            a, _ = t.back(c, back, 0)
            copy_job("rows", at_a(src, layer, c, a), at_a(dst, layer, c, a))
        moment_job("mr", *(one.at[layer] for one in small[c // layers]))
        a, _ = t.back(c, side - 2, 0)
        ref = rowbuf
        sources = [(stay[c * PARTS + k], one) for k, one in enumerate(row_parts(wide, c))]
        aside = aside_part(wide)
        if c == SPARED:
            sources.append((cut_rows(at_a(src, layer, c, a), aside, (slice(None),)), aside))
        job(
            "rows",
            [lambda slot, src=src, one=one: (src, cut_rows(ref, one, (slot, slice(None)))) for src, one in sources],
            [lambda slot, layer=layer, c=c, a=a, dst=dst: (ref.at[slot], at_a(dst, layer, c, a))],
        )
        if c == SPARED:
            a, _ = t.back(c, side - 1, 0)
            whole = src, dst
            src, dst = (cut_rows(at_a(one, layer, c, a), aside, (slice(None),)) for one in whole)
            job(
                "rows",
                [lambda slot, src=src, aside=aside: (src, cut_rows(ref, aside, (slot, slice(None))))],
                [lambda slot, dst=dst, aside=aside: (cut_rows(ref, aside, (slot, slice(None))), dst)],
            )
        for back in range(side - 2):
            a, _ = t.back(c, back, 0)
            copy_job("cols", low_at_a(t_down, c, a), low_at_a(o_down, c, a))
        a, _ = t.back(c, side - 2, 0)
        copy_job("cols", low_stay[c], low_at_a(o_down, c, a))
        if c // layers == 1:
            moment_job("mc", *(one.at[layer] for one in small[2]))

    def copies(k, which):
        what, slot = jobs[k][:2]
        sem = (load_sem, store_sem)[which]
        return [local(src, dst, sem.at[base[what] + slot, z]) for z, (src, dst) in enumerate(jobs[k][2 + which])]

    ahead, stored = 4, [False] * len(jobs)

    def start_loads(k):
        for one in range(k):
            if jobs[one][:2] == jobs[k][:2] and not stored[one]:
                for copy in copies(one, 1):
                    copy.wait()
                stored[one] = True
        for copy in copies(k, 0):
            copy.start()

    for k in range(ahead):
        start_loads(k)
    for k, (*_, work) in enumerate(jobs):
        for copy in copies(k, 0):
            copy.wait()
        if work is not None:
            work()
        for copy in copies(k, 1):
            copy.start()
        if k + ahead < len(jobs):
            start_loads(k + ahead)
    for k in range(len(jobs)):
        if not stored[k]:
            for copy in copies(k, 1):
                copy.wait()


def place_kernel(side, k, *refs):
    *ins, sem = refs
    wholes = 2 + (k == 0)
    ins, outs = ins[wholes:-wholes], ins[-wholes:]
    t = Torus(side)
    layers = outs[0].shape[0]
    moves = []
    for c in COLOURS:
        a, _ = t.back(c, side - 1, 0)
        dst = outs[c // layers]
        dst = dst.at[c % layers, a] if c < 2 else dst.at[c % layers, :, a]
        part = row_parts(outs[0].shape[-1], c)[k]
        moves.append(local(ins[c], cut_rows(dst, part, (slice(None),)), sem.at[c]))
        if wholes > 2:
            columns = pl.ds(c * ins[4].shape[-1], ins[4].shape[-1])
            dst = outs[2].at[:, a, :, :, columns] if c < 2 else outs[2].at[:, :, a, :, columns]
            moves.append(local(ins[4 + c], dst, sem.at[4 + c]))
    for move in moves:
        move.start()
    for move in moves:
        move.wait()


def solution(mesh):
    n = mesh.shape["dp"]
    side = math.isqrt(n)
    dma = pltpu.SemaphoreType.DMA
    anywhere, in_vmem = pl.BlockSpec(memory_space=pl.ANY), pl.BlockSpec(memory_space=pltpu.VMEM)

    def shape(*dims, dtype=BF16):
        return jax.ShapeDtypeStruct(dims, dtype)

    def in_hbm(*some):
        return [pltpu.with_memory_space_constraint(one, pltpu.HBM) for one in some]

    def permutation(c):
        moved = []
        for i in range(n):
            a, b = (i // side, i % side) if c < 2 else (i % side, i // side)
            a = (a + sign(c)) % side
            moved.append((i, a * side + b if c < 2 else b * side + a))
        return moved

    def step(*arrays):
        terms, weights, m, v = (arrays[i : i + 3] for i in (0, 3, 6, 9))
        layers, rows, wide = m[0].shape
        tall, narrow = m[2].shape[1:]
        assert side == 4 and side * side == n and layers * 2 == len(COLOURS), (n, layers)
        r, quarter = rows // PIECES, narrow // len(COLOURS)
        kinds = PIECES + layers
        block, low_block = (PIECES, r, wide), (tall, narrow)

        def cut(whole, *lead):
            return [one.reshape(layers, *lead, *dims) for one, dims in zip(whole, (block, block, low_block), strict=True)]

        m, v = cut(m), cut(v)
        assert r * wide == tall * quarter and kinds == 6
        stays = [shape(side, one[1], r, one[3]) for c in COLOURS for one in row_parts(wide, c)] + [shape(layers, side, tall, quarter)] * 4
        out = pl.pallas_call(
            functools.partial(main_kernel, n, side, float(n * sum(one.size for one in m))),
            name="sum_step_gather",
            out_shape=(
                *(shape(layers, n, *block),) * 2, shape(layers, n, *low_block),
                *(shape(layers, *block),) * 2, shape(layers, *low_block),
                shape(8, 128, dtype=F32), *stays,
            ),
            in_specs=[anywhere] * 12,
            out_specs=[anywhere] * 6 + [in_vmem] + [anywhere] * len(stays),
            scratch_shapes=[
                pltpu.VMEM((2, 4, side, *block), BF16),
                pltpu.VMEM((2, 4, side, layers, tall, quarter), BF16),
                pltpu.VMEM((2, 4, *block), BF16),
                pltpu.VMEM((2, 4, layers, tall, quarter), BF16),
                pltpu.VMEM((4, 2, r, wide), F32),
                pltpu.VMEM((4, layers, tall, quarter), F32),
                pltpu.VMEM((4, 2, r, wide), F32),
                pltpu.VMEM((4, layers, tall, quarter), F32),
                pltpu.VMEM((8, 128), F32),
                pltpu.VMEM((n, 1, 128), F32),
                dma((2, 4, side)),
                dma((2, 4, side)),
                dma((4, kinds)),
                dma((4, 2)),
                dma((2, 4)),
                dma((4, 3)),
                pltpu.SemaphoreType.REGULAR((4,)),
                pltpu.SemaphoreType.REGULAR((4,)),
                pltpu.SemaphoreType.REGULAR((4,)),
                dma((2,)),
                dma((2, 2)),
            ],
            compiler_params=pltpu.CompilerParams(collective_id=0, has_side_effects=True, vmem_limit_bytes=66_000_000),
        )(*cut([one[0] for one in terms], n), *cut(weights, n), *m, *v)
        gathered, g, factor, stay = out[:3], out[3:6], out[6], out[7:]

        moved = {}
        for k in (0, PARTS, *range(1, PARTS)):
            for c in COLOURS:
                moved[c, k] = lax.ppermute(stay[c * PARTS + k] if k < PARTS else stay[4 * k + c], "dp", permutation(c))

        square = (layers, side, side)
        copied = pl.pallas_call(
            functools.partial(copy_kernel, side),
            name="copy_and_moments",
            out_shape=(
                *(shape(*square, *block),) * 2, shape(*square, *low_block),
                *((shape(layers, *block, dtype=F32),) * 2 + (shape(layers, *low_block, dtype=F32),)) * 2,
            ),
            in_specs=[anywhere] * 6 + [in_vmem] + [anywhere] * (6 + len(stay)),
            out_specs=[anywhere] * 9,
            scratch_shapes=[
                pltpu.VMEM((3, side, *block), BF16),
                pltpu.VMEM((4, layers, side, tall, quarter), BF16),
                pltpu.VMEM((1, *block), BF16),
                pltpu.VMEM((1, *low_block), BF16),
                pltpu.VMEM((1, *block), F32),
                pltpu.VMEM((1, *low_block), F32),
                pltpu.VMEM((1, *block), F32),
                pltpu.VMEM((1, *low_block), F32),
                dma((9, 4)),
                dma((9, 2)),
            ],
            cost_estimate=pl.CostEstimate(flops=10**9, bytes_accessed=200_000_000, transcendentals=0),
            compiler_params=pltpu.CompilerParams(vmem_limit_bytes=32_000_000),
        )(*in_hbm(*(one.reshape(*square, *one.shape[2:]) for one in gathered), *g), factor, *in_hbm(*m, *v, *stay))
        new_w, new_m, new_v = list(copied[:3]), copied[3:6], copied[6:]

        for k in range(PARTS):
            wholes = 3 if k == 0 else 2
            arrived = [moved[c, k] for c in COLOURS] + [moved[c, PARTS] for c in COLOURS if k == 0]
            new_w[:wholes] = pl.pallas_call(
                functools.partial(place_kernel, side, k),
                name=f"place_{k}",
                out_shape=[shape(*old.shape) for old in new_w[:wholes]],
                in_specs=[anywhere] * wholes + [in_vmem] * len(arrived),
                out_specs=[anywhere] * wholes,
                scratch_shapes=[dma((8,))],
                input_output_aliases={i: i for i in range(wholes)},
                compiler_params=pltpu.CompilerParams(vmem_limit_bytes=24_000_000),
            )(*new_w[:wholes], *arrived)
        return tuple(one.reshape(old.shape) for one, old in zip((*new_w, *new_m, *new_v), (*weights, *arrays[6:]), strict=True))

    all_of, part = P(None, None, None), P(None, "dp", None)
    return jax.shard_map(
        step,
        mesh=mesh,
        in_specs=(P(("rep", "dp"), None, None, None),) * 3 + (all_of,) * 3 + (part,) * 6,
        out_specs=(P("rep", None, None),) * 3 + (P("rep", "dp", None),) * 6,
        check_vma=False,
    )
```

```python
import functools
import math

import jax
import jax.numpy as jnp
from jax import lax
from jax.experimental import pallas as pl
from jax.experimental.pallas import tpu as pltpu
from jax.sharding import PartitionSpec as P

MESH = pl.DeviceIdType.MESH
F32, BF16 = jnp.float32, jnp.bfloat16
COLOURS = range(4)
PIECES = 4
PARTS = 3
ROWS, COLS = 0, 1
SPARED = 2
LATE_CORE, LATE_BY = 0, 15_000


def divisor(whole, unit, most):
    return max(d for d in range(unit, most + 1, unit) if whole % d == 0)


def last_columns(wide):
    tiles = wide // 128
    return 128 * max(2, 2 * tiles // 11), 128 * max(1, tiles // 33)


def row_parts(wide, c):
    end, aside = last_columns(wide)
    return [(0, PIECES - 1, 0, wide), (PIECES - 1, 1, 0, wide - end), (PIECES - 1, 1, wide - end, end - aside * (c == SPARED))]


def aside_part(wide):
    _, aside = last_columns(wide)
    return PIECES - 1, 1, wide - aside, aside


def cut_rows(ref, part, lead=()):
    return ref.at[(*lead, pl.ds(*part[:2]), slice(None), pl.ds(*part[2:]))]


def moments(m, v, g):
    m = 0.9 * m + 0.1 * g
    v = 0.95 * v + 0.05 * g * g
    return m, v


def new_weight(w, m, v):
    step = m * lax.rsqrt(v + 1e-8) + 0.1 * w
    return (w - 0.02 * step).astype(BF16)


class Torus:
    def __init__(self, side):
        self.side = side
        self.me = lax.axis_index("dp")
        self.x, self.y = self.me // side, lax.rem(self.me, side)

    def around(self, v):
        return lax.rem(v + 4 * self.side, self.side)

    def ab(self, c):
        return (self.x, self.y) if c < 2 else (self.y, self.x)

    def dev(self, c, a, b):
        return a * self.side + b if c < 2 else b * self.side + a

    def along_a(self, c, k):
        a, b = self.ab(c)
        return self.dev(c, self.around(a + k * sign(c)), b)

    def along_b(self, c, k):
        a, b = self.ab(c)
        return self.dev(c, a, self.around(b + k * sign(c)))

    def back(self, c, back_a, back_b):
        a, b = self.ab(c)
        return self.around(a - back_a * sign(c)), self.around(b - back_b * sign(c))

    def block(self, c, back_a, back_b):
        return self.dev(c, *self.back(c, back_a, back_b))


def sign(c):
    return 1 if c % 2 == 0 else -1


def remote(src, dst, send, recv, device):
    return pltpu.make_async_remote_copy(src, dst, send, recv, device_id={"dp": device}, device_id_type=MESH)


def local(src, dst, sem):
    return pltpu.make_async_copy(src, dst, sem)


def got(ref, sem):
    pltpu.make_async_copy(ref, ref, sem).wait()


def tell(sem, device):
    pl.semaphore_signal(sem, inc=1, device_id={"dp": device}, device_id_type=MESH)


def main_kernel(n, side, count,
                g_gate, g_up, g_down, w_gate, w_up, w_down, m_gate, m_up, m_down, v_gate, v_up, v_down,
                o_gate, o_up, o_down, og_gate, og_up, og_down, factor_ref, *rest):
    stay, low_stay, rest = rest[: PARTS * 4], rest[PARTS * 4 : PARTS * 4 + 4], rest[PARTS * 4 + 4 :]
    bufr, bufc, ownr, ownc, mr, mc, vr, vc, acc, sq, rs, ss, p2r, p2s, own_sem, mv_sem, cred1, cred2, ready, sq_sem, loc = rest
    layers = g_gate.shape[0]
    wide = bufr.shape[-1]
    tall, quarter = bufc.shape[-2:]
    cstep, rstep = divisor(wide, 128, 384), divisor(tall, 8, 24)
    kinds = PIECES + layers
    t = Torus(side)
    me = t.me

    gates = (g_gate, g_up), (w_gate, w_up), (m_gate, m_up), (v_gate, v_up), (o_gate, o_up), (og_gate, og_up)
    downs = g_down, w_down, m_down, v_down, o_down, og_down
    TERM, WEIGHT, M, V, OUT, SUM = range(6)

    def pick(which, c):
        return gates[which][c // layers], c % layers

    def cols(c):
        return pl.ds(c * quarter, quarter)

    def group(which, c, kind, j):
        if kind == ROWS:
            ref, layer = pick(which, c)
            return ref.at[layer, j]
        return downs[which].at[:, j, :, cols(c)]

    def piece(which, c, i, j):
        if i < PIECES:
            ref, layer = pick(which, c)
            return ref.at[layer, j, i]
        return downs[which].at[i - PIECES, j, :, cols(c)]

    def own_group(which, c, kind):
        if kind == ROWS:
            ref, layer = pick(which, c)
            return ref.at[layer]
        return downs[which].at[:, :, cols(c)]

    def own_piece(which, c, i):
        if i < PIECES:
            ref, layer = pick(which, c)
            return ref.at[layer, i]
        return downs[which].at[i - PIECES, :, cols(c)]

    def buf(kind, *lead):
        return (bufr, bufc)[kind].at[lead]

    def own(kind, *lead):
        return (ownr, ownc)[kind].at[lead]

    def part(ref, kind, i):
        return ref.at[i if kind == ROWS else i - PIECES]

    def kind_of(i):
        return ROWS if i < PIECES else COLS

    def pieces(kind):
        return range(PIECES) if kind == ROWS else range(PIECES, kinds)

    def tiles(kind, body):
        if kind == ROWS:
            @pl.loop(0, wide // cstep)
            def _(k):
                body((slice(None), pl.ds(pl.multiple_of(k * cstep, 128), cstep)))
        else:
            @pl.loop(0, tall // rstep)
            def _(k):
                body((pl.ds(pl.multiple_of(k * rstep, 8), rstep), slice(None)))

    def add(kind, dst, *more):
        def body(at):
            total = dst[at].astype(F32)
            for one in more:
                total += one[at].astype(F32)
            dst[at] = total.astype(BF16)

        tiles(kind, body)

    def six(sem):
        got(bufr.at[0, 0, pl.ds(0, kinds // 3), pl.ds(0, 3)], sem)

    last = side - 1
    later = t.x < last, t.x == 0, t.y < last, t.y == 0
    there = tuple(t.along_a(c, 1) for c in COLOURS)
    towards = (0, 2, 1, 3)
    barrier = pltpu.get_barrier_semaphore()
    for c in towards:
        @pl.when(later[c])
        def _():
            tell(barrier, there[c])
    earlier = (t.x + 1) // 2 + (t.y + 1) // 2

    @pl.when(earlier > 0)
    def _():
        pl.semaphore_wait(barrier, earlier)

    for c in towards:
        @pl.when(jnp.logical_not(later[c]))
        def _():
            tell(ready.at[c ^ 1], there[c])

    @pl.when(lax.rem(lax.axis_index("rep"), 2) == LATE_CORE)
    def _():
        pl.delay(LATE_BY)

    def first_hop(q, c):
        for kind in (ROWS, COLS):
            remote(group(TERM, c, kind, t.block(c, 1, q + 1)), buf(kind, 0, c, q), ss.at[0, c, q], rs.at[0, c, q], there[c]).start()

    for c in (2, 0, 1, 3):
        @pl.when(jnp.logical_not(later[c]))
        def _():
            first_hop(0, c)
    for c in towards:
        @pl.when(later[c])
        def _():
            pl.semaphore_wait(ready.at[c], 1)
            first_hop(0, c)

    @pl.loop(1, side)
    def _(q):
        for c in COLOURS:
            first_hop(q, c)

    def own_load(step, c, kind):
        stage, q = 1 + step // side, lax.rem(step, side)
        par = lax.rem(step, 2)
        return local(group(TERM, c, kind, t.block(c, stage + 1, q + 1)), own(kind, par, c), own_sem.at[par, c])

    def start_own(step):
        for kind in (ROWS, COLS):
            for c in COLOURS:
                own_load(step, c, kind).start()

    def mv_load(c, i):
        kind = kind_of(i)
        if kind == ROWS:
            return [local(own_piece(which, c, i), ref.at[c, i % 2], mv_sem.at[c, i % 2]) for which, ref in ((M, mr), (V, vr))]
        return [local(own_group(which, c, COLS), ref.at[c], mv_sem.at[c, 2]) for which, ref in ((M, mc), (V, vc))]

    def mv_wait(c, i):
        if kind_of(i) == ROWS:
            got(mr.at[c], mv_sem.at[c, i % 2])
        else:
            got(mc.at[pl.ds(0, 2)], mv_sem.at[c, 2])

    start_own(0)
    for i in (0, 1, PIECES):
        for c in COLOURS:
            for copy in mv_load(c, i):
                copy.start()

    @pl.loop(0, 2 * side)
    def _(step):
        par, q = step // side, lax.rem(step, side)
        start_own(step + 1)
        for c in COLOURS:
            six(rs.at[par, c, q])
            six(ss.at[par, c, q])

            @pl.when(par == 1)
            def _():
                tell(cred1.at[c], t.along_a(c, -1))

            six(own_sem.at[lax.rem(step, 2), c])
            for kind in (ROWS, COLS):
                here, mine = buf(kind, par, c, q), own(kind, lax.rem(step, 2), c)
                for i in pieces(kind):
                    add(kind, part(here, kind, i), part(mine, kind, i))
        for c in COLOURS:
            @pl.when(par == 1)
            def _():
                pl.semaphore_wait(cred1.at[c], 1)

            for kind in (ROWS, COLS):
                remote(buf(kind, par, c, q), buf(kind, 1 - par, c, q), ss.at[1 - par, c, q], rs.at[1 - par, c, q], t.along_a(c, 1)).start()

    acc[...] = jnp.zeros_like(acc)
    last_own = (3 * side) % 2
    for q in range(side):
        step = 2 * side + q
        if q < side - 1:
            start_own(step + 1)
        else:
            for kind in (ROWS, COLS):
                for c in COLOURS:
                    local(group(WEIGHT, c, kind, me), own(kind, last_own, c), own_sem.at[last_own, c]).start()
        for i in range(kinds):
            kind = kind_of(i)
            for c in COLOURS:
                whole, mine = buf(kind, 0, c, q), own(kind, step % 2, c)
                here = part(whole, kind, i)
                if i == 0:
                    six(rs.at[0, c, q])
                    six(ss.at[0, c, q])
                    six(own_sem.at[step % 2, c])
                more = [part(mine, kind, i)]
                if q:
                    got(here, p2r.at[c, i])
                    more.append(part(buf(kind, 1, c, q - 1), kind, i))
                if q < side - 1:
                    tell(cred2.at[c], t.along_b(c, -1))
                    add(kind, here, *more)
                    continue

                def last(at, here=here, more=more):
                    total = here[at].astype(F32)
                    for one in more:
                        total += one[at].astype(F32)
                    total = total.astype(BF16)
                    here[at] = total
                    square = total.astype(F32)
                    square = square * square
                    rows, columns = square.shape
                    acc[...] += sum(square[a : a + 8, b : b + 128] for a in range(0, rows, 8) for b in range(0, columns, 128))

                tiles(kind, last)
            if q < side - 1:
                for c in COLOURS:
                    pl.semaphore_wait(cred2.at[c], 1)
                    remote(part(buf(kind, 0, c, q), kind, i), part(buf(kind, 1, c, q), kind, i), p2s.at[c, kind], p2r.at[c, i], t.along_b(c, 1)).start()

    sq[me] = jnp.sum(acc[...], axis=0, keepdims=True)
    for k in range(1, n):
        remote(sq.at[me], sq.at[me], sq_sem.at[0], sq_sem.at[1], lax.rem(me + k, n)).start()
    for c in COLOURS:
        for kind in (ROWS, COLS):
            got((bufr, bufc)[kind].at[0, c, pl.ds(0, side - 1)], p2s.at[c, kind])
    got(sq.at[pl.ds(0, n - 1)], sq_sem.at[1])
    total = sum(sq[k] for k in range(n))
    total = jnp.sum(total, axis=(0, 1), keepdims=True)
    factor = jnp.minimum(1.0, 0.5 * lax.rsqrt(total / count + 1e-30))
    factor_ref[...] = jnp.broadcast_to(factor, factor_ref.shape)

    def arrived_b(c, hop):
        return p2r.at[c, hop - 1]

    def arrived_a(c, hop, q):
        return rs.at[hop - 1, c, q]

    def sent(c, kind):
        return p2s.at[c, kind]

    aside = aside_part(wide)

    def send_aside(c, kind, src, dst):
        if c == SPARED and kind == ROWS:
            remote(cut_rows(src, aside), cut_rows(dst, aside), own_sem.at[1, 3], own_sem.at[1, 2], t.along_a(c, -1)).start()

    for i in range(kinds):
        kind = kind_of(i)
        for c in COLOURS:
            if i == 0:
                six(own_sem.at[last_own, c])
            if i <= PIECES:
                mv_wait(c, i)
            w_ref, g_ref = (part(ref, kind, i) for ref in (own(kind, last_own, c), buf(kind, 0, c, side - 1)))
            m_ref, v_ref = (rows.at[c, i % 2] if kind == ROWS else columns.at[c, i - PIECES] for rows, columns in ((mr, mc), (vr, vc)))

            def body(at, w_ref=w_ref, g_ref=g_ref, m_ref=m_ref, v_ref=v_ref):
                g = g_ref[at].astype(F32) * factor
                m, v = moments(m_ref[at], v_ref[at], g)
                w_ref[at] = new_weight(w_ref[at].astype(F32), m, v)

            tiles(kind, body)
            if i + 2 < PIECES:
                for copy in mv_load(c, i + 2):
                    copy.start()
        for c in COLOURS:
            remote(part(own(kind, last_own, c), kind, i), piece(OUT, c, i, me), sent(c, kind), arrived_b(c, 1), t.along_b(c, 1)).start()
    for kind in (ROWS, COLS):
        for c in COLOURS:
            mine, there = own(kind, last_own, c), group(OUT, c, kind, me)
            remote(mine, there, sent(c, kind), arrived_a(c, 1, 0), t.along_a(c, 1)).start()
            send_aside(c, kind, mine, there)
            local(mine, there, loc.at[0, kind]).start()
            local(buf(kind, 0, c, side - 1), own_group(SUM, c, kind), loc.at[1, kind]).start()

    for hop in range(1, side):
        for c in COLOURS:
            six(arrived_b(c, hop))
            for kind in (ROWS, COLS):
                here = group(OUT, c, kind, t.block(c, 0, hop))
                if hop < side - 1:
                    remote(here, here, sent(c, kind), arrived_b(c, hop + 1), t.along_b(c, 1)).start()
                remote(here, here, sent(c, kind), arrived_a(c, 1, hop), t.along_a(c, 1)).start()
                send_aside(c, kind, here, here)

    for hop in range(1, side - 2):
        for q in range(side):
            for c in COLOURS:
                six(arrived_a(c, hop, q))
                a, b = t.back(c, hop, q)
                next_hop = functools.partial(remote, recv=arrived_a(c, hop + 1, q), device=t.along_a(c, 1))
                rows, columns = (group(OUT, c, kind, t.dev(c, a, b)) for kind in (ROWS, COLS))
                if hop < side - 3:
                    next_hop(rows, rows, send=sent(c, ROWS)).start()
                    next_hop(columns, columns, send=sent(c, COLS)).start()
                    continue
                for k, one in enumerate(row_parts(wide, c)):
                    next_hop(cut_rows(rows, one), stay[c * PARTS + k].at[b], send=sent(c, ROWS)).start()
                if c == SPARED:
                    next_hop(cut_rows(rows, aside), cut_rows(rows, aside), send=sent(c, ROWS)).start()
                next_hop(columns, low_stay[c].at[:, b], send=sent(c, COLS)).start()
    for q in range(side):
        for c in COLOURS:
            six(arrived_a(c, side - 2, q))

    ref, layer = pick(OUT, SPARED)
    for k in (2, 3):
        got(cut_rows(ref, aside, (layer, pl.ds(0, side))), own_sem.at[1, k])

    got(sq.at[pl.ds(0, n - 1)], sq_sem.at[0])
    for kind in (ROWS, COLS):
        for k in range(2):
            got((ownr, ownc)[kind].at[last_own], loc.at[k, kind])
    for c in COLOURS:
        ref, layer = pick(OUT, c)
        got(ref.at[layer, pl.ds(0, n - 1 - side)], sent(c, ROWS))
        got(o_down.at[:, pl.ds(0, n - 1 - side), :, cols(c)], sent(c, COLS))


def copy_kernel(side, t_gate, t_up, t_down, g_gate, g_up, g_down, factor_ref, m_gate, m_up, m_down, v_gate, v_up, v_down, *rest):
    stay, low_stay, rest = rest[: 4 * PARTS], rest[4 * PARTS : 4 * PARTS + 4], rest[4 * PARTS + 4 :]
    o_gate, o_up, o_down, nm_gate, nm_up, nm_down, nv_gate, nv_up, nv_down, rowbuf, colbuf, gr, gc, mr, mc, vr, vc, load_sem, store_sem = rest
    layers = o_down.shape[0]
    wide = gr.shape[-1]
    tall = gc.shape[-2]
    quarter = colbuf.shape[-1]
    t = Torus(side)
    factor = factor_ref[0:1, 0:1]

    def at_a(ref, layer, c, a):
        return ref.at[layer, a] if c < 2 else ref.at[layer, :, a]

    def low_at_a(ref, c, a):
        columns = pl.ds(c * quarter, quarter)
        return ref.at[:, a, :, :, columns] if c < 2 else ref.at[:, :, a, :, columns]

    jobs = []
    slots = {"rows": (rowbuf, 0), "cols": (colbuf, 1)}
    made = {"rows": 0, "cols": 0, "mr": 0, "mc": 0}
    depth = {"rows": rowbuf.shape[0], "cols": colbuf.shape[0], "mr": gr.shape[0], "mc": gc.shape[0]}
    base = {"rows": 0, "cols": depth["rows"], "mr": depth["rows"] + depth["cols"], "mc": depth["rows"] + depth["cols"] + depth["mr"]}

    def job(what, loads, stores, work=None):
        slot = made[what] % depth[what]
        made[what] += 1
        jobs.append((what, slot, [f(slot) for f in loads], [f(slot) for f in stores], work and functools.partial(work, slot)))

    def copy_job(what, src, dst):
        ref = slots[what][0]
        job(what, [lambda slot: (src, ref.at[slot])], [lambda slot: (ref.at[slot], dst)])

    def step(gs, ms, vs, parts, where, slot):
        @pl.loop(0, parts)
        def _(k):
            at = (slot, *where(k))
            g = gs[at].astype(F32) * factor
            ms[at], vs[at] = moments(ms[at], vs[at], g)

    def moment_job(what, g, m, v, nm, nv):
        gs, ms, vs = (gr, mr, vr) if what == "mr" else (gc, mc, vc)
        if what == "mr":
            size = divisor(wide, 128, 384)
            parts = gs.shape[1] * (wide // size)
            each = wide // size
            where = lambda k: (k // each, slice(None), pl.ds(pl.multiple_of(lax.rem(k, each) * size, 128), size))
        else:
            size = divisor(tall, 8, 24)
            parts = tall // size
            where = lambda k: (pl.ds(pl.multiple_of(k * size, 8), size), slice(None))
        job(
            what,
            [lambda slot: (g, gs.at[slot]), lambda slot: (m, ms.at[slot]), lambda slot: (v, vs.at[slot])],
            [lambda slot: (ms.at[slot], nm), lambda slot: (vs.at[slot], nv)],
            functools.partial(step, gs, ms, vs, parts, where),
        )

    big = ((t_gate, o_gate), (t_up, o_up))
    small = ((g_gate, m_gate, v_gate, nm_gate, nv_gate), (g_up, m_up, v_up, nm_up, nv_up), (g_down, m_down, v_down, nm_down, nv_down))
    for c in COLOURS:
        layer = c % layers
        src, dst = big[c // layers]
        for back in range(side - 2):
            a, _ = t.back(c, back, 0)
            copy_job("rows", at_a(src, layer, c, a), at_a(dst, layer, c, a))
        moment_job("mr", *(one.at[layer] for one in small[c // layers]))
        a, _ = t.back(c, side - 2, 0)
        ref = rowbuf
        sources = [(stay[c * PARTS + k], one) for k, one in enumerate(row_parts(wide, c))]
        aside = aside_part(wide)
        if c == SPARED:
            sources.append((cut_rows(at_a(src, layer, c, a), aside, (slice(None),)), aside))
        job(
            "rows",
            [lambda slot, src=src, one=one: (src, cut_rows(ref, one, (slot, slice(None)))) for src, one in sources],
            [lambda slot, layer=layer, c=c, a=a, dst=dst: (ref.at[slot], at_a(dst, layer, c, a))],
        )
        if c == SPARED:
            a, _ = t.back(c, side - 1, 0)
            whole = src, dst
            src, dst = (cut_rows(at_a(one, layer, c, a), aside, (slice(None),)) for one in whole)
            job(
                "rows",
                [lambda slot, src=src, aside=aside: (src, cut_rows(ref, aside, (slot, slice(None))))],
                [lambda slot, dst=dst, aside=aside: (cut_rows(ref, aside, (slot, slice(None))), dst)],
            )
        for back in range(side - 2):
            a, _ = t.back(c, back, 0)
            copy_job("cols", low_at_a(t_down, c, a), low_at_a(o_down, c, a))
        a, _ = t.back(c, side - 2, 0)
        copy_job("cols", low_stay[c], low_at_a(o_down, c, a))
        if c // layers == 1:
            moment_job("mc", *(one.at[layer] for one in small[2]))

    def copies(k, which):
        what, slot = jobs[k][:2]
        sem = (load_sem, store_sem)[which]
        return [local(src, dst, sem.at[base[what] + slot, z]) for z, (src, dst) in enumerate(jobs[k][2 + which])]

    ahead, stored = 4, [False] * len(jobs)

    def start_loads(k):
        for one in range(k):
            if jobs[one][:2] == jobs[k][:2] and not stored[one]:
                for copy in copies(one, 1):
                    copy.wait()
                stored[one] = True
        for copy in copies(k, 0):
            copy.start()

    for k in range(ahead):
        start_loads(k)
    for k, (*_, work) in enumerate(jobs):
        for copy in copies(k, 0):
            copy.wait()
        if work is not None:
            work()
        for copy in copies(k, 1):
            copy.start()
        if k + ahead < len(jobs):
            start_loads(k + ahead)
    for k in range(len(jobs)):
        if not stored[k]:
            for copy in copies(k, 1):
                copy.wait()


def place_kernel(side, k, *refs):
    *ins, sem = refs
    wholes = 2 + (k == 0)
    ins, outs = ins[wholes:-wholes], ins[-wholes:]
    t = Torus(side)
    layers = outs[0].shape[0]
    moves = []
    for c in COLOURS:
        a, _ = t.back(c, side - 1, 0)
        dst = outs[c // layers]
        dst = dst.at[c % layers, a] if c < 2 else dst.at[c % layers, :, a]
        part = row_parts(outs[0].shape[-1], c)[k]
        moves.append(local(ins[c], cut_rows(dst, part, (slice(None),)), sem.at[c]))
        if wholes > 2:
            columns = pl.ds(c * ins[4].shape[-1], ins[4].shape[-1])
            dst = outs[2].at[:, a, :, :, columns] if c < 2 else outs[2].at[:, :, a, :, columns]
            moves.append(local(ins[4 + c], dst, sem.at[4 + c]))
    for move in moves:
        move.start()
    for move in moves:
        move.wait()


def solution(mesh):
    n = mesh.shape["dp"]
    side = math.isqrt(n)
    dma = pltpu.SemaphoreType.DMA
    anywhere, in_vmem = pl.BlockSpec(memory_space=pl.ANY), pl.BlockSpec(memory_space=pltpu.VMEM)

    def shape(*dims, dtype=BF16):
        return jax.ShapeDtypeStruct(dims, dtype)

    def in_hbm(*some):
        return [pltpu.with_memory_space_constraint(one, pltpu.HBM) for one in some]

    def permutation(c):
        moved = []
        for i in range(n):
            a, b = (i // side, i % side) if c < 2 else (i % side, i // side)
            a = (a + sign(c)) % side
            moved.append((i, a * side + b if c < 2 else b * side + a))
        return moved

    def step(*arrays):
        terms, weights, m, v = (arrays[i : i + 3] for i in (0, 3, 6, 9))
        layers, rows, wide = m[0].shape
        tall, narrow = m[2].shape[1:]
        assert side == 4 and side * side == n and layers * 2 == len(COLOURS), (n, layers)
        r, quarter = rows // PIECES, narrow // len(COLOURS)
        kinds = PIECES + layers
        block, low_block = (PIECES, r, wide), (tall, narrow)

        def cut(whole, *lead):
            return [one.reshape(layers, *lead, *dims) for one, dims in zip(whole, (block, block, low_block), strict=True)]

        m, v = cut(m), cut(v)
        assert r * wide == tall * quarter and kinds == 6
        stays = [shape(side, one[1], r, one[3]) for c in COLOURS for one in row_parts(wide, c)] + [shape(layers, side, tall, quarter)] * 4
        out = pl.pallas_call(
            functools.partial(main_kernel, n, side, float(n * sum(one.size for one in m))),
            name="sum_step_gather",
            out_shape=(
                *(shape(layers, n, *block),) * 2, shape(layers, n, *low_block),
                *(shape(layers, *block),) * 2, shape(layers, *low_block),
                shape(8, 128, dtype=F32), *stays,
            ),
            in_specs=[anywhere] * 12,
            out_specs=[anywhere] * 6 + [in_vmem] + [anywhere] * len(stays),
            scratch_shapes=[
                pltpu.VMEM((2, 4, side, *block), BF16),
                pltpu.VMEM((2, 4, side, layers, tall, quarter), BF16),
                pltpu.VMEM((2, 4, *block), BF16),
                pltpu.VMEM((2, 4, layers, tall, quarter), BF16),
                pltpu.VMEM((4, 2, r, wide), F32),
                pltpu.VMEM((4, layers, tall, quarter), F32),
                pltpu.VMEM((4, 2, r, wide), F32),
                pltpu.VMEM((4, layers, tall, quarter), F32),
                pltpu.VMEM((8, 128), F32),
                pltpu.VMEM((n, 1, 128), F32),
                dma((2, 4, side)),
                dma((2, 4, side)),
                dma((4, kinds)),
                dma((4, 2)),
                dma((2, 4)),
                dma((4, 3)),
                pltpu.SemaphoreType.REGULAR((4,)),
                pltpu.SemaphoreType.REGULAR((4,)),
                pltpu.SemaphoreType.REGULAR((4,)),
                dma((2,)),
                dma((2, 2)),
            ],
            compiler_params=pltpu.CompilerParams(collective_id=0, has_side_effects=True, vmem_limit_bytes=66_000_000),
        )(*cut([one[0] for one in terms], n), *cut(weights, n), *m, *v)
        gathered, g, factor, stay = out[:3], out[3:6], out[6], out[7:]

        moved = {}
        for k in (0, PARTS, *range(1, PARTS)):
            for c in COLOURS:
                moved[c, k] = lax.ppermute(stay[c * PARTS + k] if k < PARTS else stay[4 * k + c], "dp", permutation(c))

        square = (layers, side, side)
        copied = pl.pallas_call(
            functools.partial(copy_kernel, side),
            name="copy_and_moments",
            out_shape=(
                *(shape(*square, *block),) * 2, shape(*square, *low_block),
                *((shape(layers, *block, dtype=F32),) * 2 + (shape(layers, *low_block, dtype=F32),)) * 2,
            ),
            in_specs=[anywhere] * 6 + [in_vmem] + [anywhere] * (6 + len(stay)),
            out_specs=[anywhere] * 9,
            scratch_shapes=[
                pltpu.VMEM((3, side, *block), BF16),
                pltpu.VMEM((4, layers, side, tall, quarter), BF16),
                pltpu.VMEM((1, *block), BF16),
                pltpu.VMEM((1, *low_block), BF16),
                pltpu.VMEM((1, *block), F32),
                pltpu.VMEM((1, *low_block), F32),
                pltpu.VMEM((1, *block), F32),
                pltpu.VMEM((1, *low_block), F32),
                dma((9, 4)),
                dma((9, 2)),
            ],
            cost_estimate=pl.CostEstimate(flops=10**9, bytes_accessed=200_000_000, transcendentals=0),
            compiler_params=pltpu.CompilerParams(vmem_limit_bytes=32_000_000),
        )(*in_hbm(*(one.reshape(*square, *one.shape[2:]) for one in gathered), *g), factor, *in_hbm(*m, *v, *stay))
        new_w, new_m, new_v = list(copied[:3]), copied[3:6], copied[6:]

        for k in range(PARTS):
            wholes = 3 if k == 0 else 2
            arrived = [moved[c, k] for c in COLOURS] + [moved[c, PARTS] for c in COLOURS if k == 0]
            new_w[:wholes] = pl.pallas_call(
                functools.partial(place_kernel, side, k),
                name=f"place_{k}",
                out_shape=[shape(*old.shape) for old in new_w[:wholes]],
                in_specs=[anywhere] * wholes + [in_vmem] * len(arrived),
                out_specs=[anywhere] * wholes,
                scratch_shapes=[dma((len(arrived),))],
                input_output_aliases={i: i for i in range(wholes)},
                compiler_params=pltpu.CompilerParams(vmem_limit_bytes=24_000_000),
            )(*new_w[:wholes], *arrived)
        return tuple(one.reshape(old.shape) for one, old in zip((*new_w, *new_m, *new_v), (*weights, *arrays[6:]), strict=True))

    all_of, part = P(None, None, None), P(None, "dp", None)
    return jax.shard_map(
        step,
        mesh=mesh,
        in_specs=(P(("rep", "dp"), None, None, None),) * 3 + (all_of,) * 3 + (part,) * 6,
        out_specs=(P("rep", None, None),) * 3 + (P("rep", "dp", None),) * 6,
        check_vma=False,
    )
```
